256 devices in a mesh: gx: 2 (over x_lo), gy: 8 (over x_hi, y), gz: 16 (over z, core).
Axes of the slice: x: 4 (x_hi: 2, x_lo: 2; x = x_hi * 2 + x_lo), y: 4, z: 8, core: 2. Of those that a mesh axis runs over, the one named last changes fastest.
Arguments:
- volume: bfloat16 [32, 64, 64, 256], P(None, 'gx', 'gy', 'gz'), may hold values from -6 to 6
- weight_a: bfloat16 [3, 3, 3, 32, 64], replicated, may hold values from -0.21875 to 0.21875
- bias_a: float32 [64], replicated, may hold values from -3 to 3
- weight_b: bfloat16 [3, 3, 3, 64, 128], replicated, may hold values from -0.15625 to 0.15625
- bias_b: float32 [128], replicated, may hold values from -3 to 3
- cotangent: bfloat16 [128, 32, 32, 128], P(None, ('gx', 'gz'), 'gy'), may hold values from -24 to 24
Outputs:
- features: bfloat16 [128, 32, 32, 128], P(None, ('gx', 'gz'), 'gy')
- grad_input: bfloat16 [32, 64, 64, 256], P(None, 'gx', 'gy', 'gz')
- grad_weight_a: float32 [3, 3, 3, 32, 64], replicated
- grad_bias_a: float32 [64], replicated
- grad_weight_b: float32 [3, 3, 3, 64, 128], replicated
- grad_bias_b: float32 [128], replicated
The draws below stay inside these ranges and needn't reach their ends.
All inputs are finite; a program needn't handle non-finite values.
Results may differ from the reference program's by a relative error of at most 0.012.
Values may be sent and summed in bfloat16 or wider, within the bound.
A program may use at most 128 MiB of HBM per device.

```python
import math
import jax
import jax.numpy as jnp
from jax import lax

C1 = 32
C2 = 64
C3 = 128
NX = 64
NY = 64
NZ = 256


def level_of(key, dims, shards, least, top_value):
    def one(axis_at, blocks):
        steps = jax.random.uniform(jax.random.fold_in(jax.random.fold_in(key, 6), axis_at), (blocks,), jnp.float32, least / len(shards), top_value / len(shards))
        return jnp.repeat(jnp.exp(steps), dims[axis_at] // blocks).reshape((-1,) + (1,) * (len(dims) - axis_at - 1))

    level = one(*shards[0])
    for cut in shards[1:]:
        level = level * one(*cut)
    return level


def centred(own_key, shape, deviation, limit, cuts=(), dtype=jnp.bfloat16):
    entries = deviation * jax.random.normal(own_key, shape, jnp.float32)
    if cuts:
        entries = entries * level_of(own_key, shape, cuts, -0.22, 0.18)
    return jnp.clip(entries, -limit, limit).astype(dtype)


def setup_inputs(seed: int = 0) -> dict:
    seeds = jax.random.split(jax.random.key(seed), 7)
    return {
        "volume": centred(seeds[0], (C1, NX, NY, NZ), 1.0, 6.0, ((1, 2), (2, 8), (3, 16))),
        "weight_a": centred(seeds[1], (3, 3, 3, C1, C2), (27 * C1) ** -0.5, 0.21875),
        "bias_a": centred(seeds[2], (C2,), 0.5, 3.0, (), jnp.float32),
        "weight_b": centred(seeds[3], (3, 3, 3, C2, C3), (27 * C2) ** -0.5, 0.15625),
        "bias_b": centred(seeds[4], (C3,), 0.5, 3.0, (), jnp.float32),
        "cotangent": centred(seeds[5], (C3, NX // 2, NY // 2, NZ // 2), 4.0, 24.0, ((1, 32), (2, 8))),
    }


def activate(value):
    return value * jax.nn.sigmoid(value)

def slope_of(value):
    sigma = jax.nn.sigmoid(value)
    return sigma + value * sigma * (1.0 - sigma)

def conv_valid(padded, weight):
    result = lax.conv_general_dilated(padded[None], weight, (1, 1, 1), 'VALID', dimension_numbers=('NCDHW', 'DHWIO', 'NCDHW'), preferred_element_type=jnp.float32)
    return result[0]

def flipped(weight):
    return jnp.transpose(weight[::-1, ::-1, ::-1], (0, 1, 2, 4, 3))

def pad_all(field):
    return jnp.pad(field, ((0, 0), (1, 1), (1, 1), (1, 1)))

def average_pool(field):
    shape = field.shape
    split = field.reshape(shape[0], shape[1] // 2, 2, shape[2] // 2, 2, shape[3] // 2, 2)
    return lax.optimization_barrier(jnp.sum(split, axis=(2, 4, 6))) * 0.125

def spread_back(field):
    shape = field.shape
    larger = jnp.broadcast_to(field[:, :, None, :, None, :, None], (shape[0], shape[1], 2, shape[2], 2, shape[3], 2))
    return larger.reshape(shape[0], 2 * shape[1], 2 * shape[2], 2 * shape[3])

def weight_terms(padded, grad):
    width_in = padded.shape[0]
    width_out = grad.shape[0]
    extent = grad.shape[1:]
    flattened = grad.reshape(width_out, extent[0] * extent[1] * extent[2])
    products = []
    for first in range(3):
        for second in range(3):
            for third in range(3):
                window = padded[:, first:first + extent[0], second:second + extent[1], third:third + extent[2]]
                window = window.reshape(width_in, extent[0] * extent[1] * extent[2])
                products.append(lax.dot_general(window, flattened, (((1,), (1,)), ((), ())), preferred_element_type=jnp.float32))
    return jnp.stack(products).reshape(3, 3, 3, width_in, width_out)

def reference(volume, weight_a, bias_a, weight_b, bias_b, cotangent):
    scale_a = 1.0 / math.sqrt(NX * NY * NZ)
    scale_b = 1.0 / math.sqrt(NX * NY * NZ // 8)
    padded_a = pad_all(volume)
    before_a = conv_valid(padded_a, weight_a) + bias_a[:, None, None, None]
    pooled = average_pool(activate(before_a)).astype(jnp.bfloat16)
    padded_b = pad_all(pooled)
    before_b = conv_valid(padded_b, weight_b) + bias_b[:, None, None, None]
    features = activate(before_b).astype(jnp.bfloat16)
    grad_b = (cotangent.astype(jnp.float32) * slope_of(before_b)).astype(jnp.bfloat16)
    grad_weight_b = weight_terms(padded_b, grad_b) * scale_b
    grad_bias_b = lax.optimization_barrier(jnp.sum(grad_b.astype(jnp.float32), axis=(1, 2, 3))) * scale_b
    grad_pooled = conv_valid(pad_all(grad_b), flipped(weight_b)).astype(jnp.bfloat16)
    grad_a = (spread_back(grad_pooled.astype(jnp.float32)) * 0.125 * slope_of(before_a)).astype(jnp.bfloat16)
    grad_weight_a = weight_terms(padded_a, grad_a) * scale_a
    grad_bias_a = lax.optimization_barrier(jnp.sum(grad_a.astype(jnp.float32), axis=(1, 2, 3))) * scale_a
    grad_input = conv_valid(pad_all(grad_a), flipped(weight_a)).astype(jnp.bfloat16)
    return (features, grad_input, grad_weight_a, grad_bias_a, grad_weight_b, grad_bias_b)
```

```python
import functools
import math

import jax
import jax.numpy as jnp
from jax import lax
from jax.experimental import pallas as pl
from jax.experimental.pallas import tpu as pltpu
from jax.sharding import PartitionSpec as P

MESH = pl.DeviceIdType.MESH


def slope_of(value):
    sigma = jax.nn.sigmoid(value)
    return sigma + value * sigma * (1.0 - sigma)


def put_windows(wide_ref, windows, planes, rows, depth):
    wide = wide_ref[...]
    width, extent = wide.shape
    place = lax.broadcasted_iota(jnp.int32, (width, extent), 1) % depth
    loose = wide.astype(jnp.float32)
    before = jnp.where(place == 0, 0.0, pltpu.roll(loose, 1, 1)).astype(jnp.bfloat16)
    after = jnp.where(place == depth - 1, 0.0, pltpu.roll(loose, extent - 1, 1)).astype(jnp.bfloat16)
    size = rows * depth
    for third, moved in enumerate((before, wide, after)):
        for first in range(3):
            for second in range(3):
                at = (first * 9 + second * 3 + third) * width
                for plane in range(planes):
                    begin = ((plane + first) * (rows + 2) + second) * depth
                    windows[at : at + width, plane * size : (plane + 1) * size] = moved[
                        :, begin : begin + size
                    ]


def dot_rows(left, right):
    return lax.dot_general(
        left, right, (((1,), (1,)), ((), ())), preferred_element_type=jnp.float32
    )


def forward_a_kernel(dims, wide_ref, weight_ref, bias_ref, pool_ref, before_ref, pooled_ref, windows):
    planes, rows, depth = dims
    put_windows(wide_ref, windows, *dims)
    before = jnp.dot(weight_ref[...], windows[...], preferred_element_type=jnp.float32)
    before = before + bias_ref[...]
    before_ref[...] = before
    active = before * jax.nn.sigmoid(before)
    size = rows * depth
    for row in range(rows // 2):
        parts = [
            active[:, plane * size + (2 * row + j) * depth : plane * size + (2 * row + j + 1) * depth]
            for plane in range(planes)
            for j in range(2)
        ]
        summed = sum(parts[1:], parts[0])
        paired = jnp.dot(
            summed, pool_ref[...], precision=lax.Precision.HIGHEST, preferred_element_type=jnp.float32
        )
        pooled_ref[:, row * depth // 2 : (row + 1) * depth // 2] = (paired * 0.125).astype(jnp.bfloat16)


def middle_kernel(dims, wide_ref, weight_ref, bias_ref, cot_ref, feat_ref, grad_ref, wb_ref, bb_ref, windows):
    put_windows(wide_ref, windows, *dims)
    before = jnp.dot(weight_ref[...], windows[...], preferred_element_type=jnp.float32)
    before = before + bias_ref[...]
    feat_ref[...] = (before * jax.nn.sigmoid(before)).astype(jnp.bfloat16)
    grad = (cot_ref[...].astype(jnp.float32) * slope_of(before)).astype(jnp.bfloat16)
    grad_ref[...] = grad
    wb_ref[...] = dot_rows(windows[...], grad)
    bb_ref[...] = dot_rows(jnp.ones((8, grad.shape[1]), jnp.bfloat16), grad)


def backward_b_kernel(dims, fine, wide_ref, weight_ref, before_ref, spread_ref, grad_ref, windows):
    put_windows(wide_ref, windows, *dims)
    pooled = jnp.dot(weight_ref[...], windows[...], preferred_element_type=jnp.float32)
    pooled = pooled.astype(jnp.bfloat16)
    planes, rows, depth = fine
    size = rows * depth
    for row in range(rows // 2):
        part = pooled[:, row * depth // 2 : (row + 1) * depth // 2]
        spread = jnp.dot(part, spread_ref[...], preferred_element_type=jnp.float32) * 0.125
        for plane in range(planes):
            for j in range(2):
                begin = plane * size + (2 * row + j) * depth
                slope = slope_of(before_ref[:, begin : begin + depth])
                grad_ref[:, begin : begin + depth] = (spread * slope).astype(jnp.bfloat16)


def backward_a_kernel(dims, wide_ref, weight_ref, out_ref, windows):
    put_windows(wide_ref, windows, *dims)
    out = jnp.dot(weight_ref[...], windows[...], preferred_element_type=jnp.float32)
    out_ref[...] = out.astype(jnp.bfloat16)


class Halo:
    def __init__(self, wide, dims, where, sems, at):
        planes, rows, depth = dims
        stride = (rows + 2) * depth
        send, recv = sems
        line, lines, row, cuts, count = where
        self.moves = []
        for up in (-1, 0, 1):
            for side in (-1, 0, 1):
                if up == 0 and side == 0:
                    continue
                to_line, to_row = (line + up + lines) % lines, (row + side + cuts) % cuts
                goes = within(line + up, lines) & within(row + side, cuts)
                comes = within(line - up, lines) & within(row - side, cuts)
                source, target, extent = {
                    -1: (1, rows + 1, 1),
                    0: (1, 1, rows),
                    1: (rows, 0, 1),
                }[side]
                pairs = {
                    -1: [(1, planes + 1)],
                    0: [(p, p) for p in range(1, planes + 1)],
                    1: [(planes, 0)],
                }[up]
                for have, give in pairs:
                    begin, end = have * stride + source * depth, give * stride + target * depth
                    copy = pltpu.make_async_remote_copy(
                        src_ref=wide.at[:, begin : begin + extent * depth],
                        dst_ref=wide.at[:, end : end + extent * depth],
                        send_sem=send.at[at + len(self.moves)],
                        recv_sem=recv.at[at + len(self.moves)],
                        device_id={"gx": to_line // count, "gz": to_line % count, "gy": to_row},
                        device_id_type=MESH,
                    )
                    self.moves.append((copy, goes, comes))

    def start(self):
        for copy, goes, _ in self.moves:
            pl.when(goes)(copy.start)

    def wait(self):
        for copy, goes, comes in self.moves:
            pl.when(goes)(copy.wait_send)
            pl.when(comes)(copy.wait_recv)


def within(at, count):
    return (at >= 0) & (at < count)


class Summing:
    def __init__(self, acc, stage, first, mine, second, whole, sems):
        self.acc, self.stage, self.first = acc, stage, first
        self.mine, self.second, self.whole = mine, second, whole
        self.sems = sems
        gy = lax.axis_size("gy")
        self.count = lax.axis_size("gx") * gy
        self.depth = lax.axis_size("gz")
        self.me = lax.axis_index("gx") * gy + lax.axis_index("gy")
        self.level = lax.axis_index("gz")

    def across(self, phase, k, source, target):
        gy = lax.axis_size("gy")
        to = (self.me + k) % self.count
        return pltpu.make_async_remote_copy(
            src_ref=source(to),
            dst_ref=target,
            send_sem=self.sems.at[phase, 0, k],
            recv_sem=self.sems.at[phase, 1, k],
            device_id={"gx": to // gy, "gy": to % gy},
            device_id_type=MESH,
        )

    def along(self, k):
        return pltpu.make_async_remote_copy(
            src_ref=self.mine,
            dst_ref=self.second.at[self.level],
            send_sem=self.sems.at[1, 0, k],
            recv_sem=self.sems.at[1, 1, k],
            device_id={"gz": (self.level + k) % self.depth},
            device_id_type=MESH,
        )

    def scatters(self):
        return [
            self.across(0, k, lambda to: self.stage.at[to], self.first.at[self.me])
            for k in range(1, self.count)
        ]

    def alongs(self):
        return [self.along(k) for k in range(1, self.depth)]

    def gathers(self):
        here = self.whole.at[self.me]
        return [self.across(2, k, lambda to: here, here) for k in range(1, self.count)]

    def start(self):
        chunk = self.stage.shape[1]
        for i in range(self.count):
            self.stage[i] = self.acc[i * chunk : (i + 1) * chunk].astype(jnp.bfloat16)
        for copy in self.scatters():
            copy.start()
        self.first[self.me] = self.stage[self.me]

    def total(self, parts):
        total = parts[0].astype(jnp.float32)
        for i in range(1, parts.shape[0]):
            total = total + parts[i].astype(jnp.float32)
        return total.astype(jnp.bfloat16)

    def middle(self):
        for copy in self.scatters():
            copy.wait()
        part = self.total(self.first)
        self.mine[...] = part
        for copy in self.alongs():
            copy.start()
        self.second[self.level] = part

    def last(self):
        for copy in self.alongs():
            copy.wait()
        self.whole[self.me] = self.total(self.second)
        for copy in self.gathers():
            copy.start()

    def finish(self):
        for copy in self.gathers():
            copy.wait()


def place(wide, flat, dims):
    planes, rows, depth = dims
    size, stride = rows * depth, (rows + 2) * depth
    for plane in range(planes):
        begin = (plane + 1) * stride + depth
        wide[:, begin : begin + size] = flat[:, plane * size : (plane + 1) * size]


def greet():
    gx, gy, gz = [lax.axis_size(axis) for axis in ("gx", "gy", "gz")]
    me = lax.axis_index("gx") * gy + lax.axis_index("gy")
    level, row = lax.axis_index("gz"), lax.axis_index("gy")
    line = lax.axis_index("gx") * gz + level
    barrier = pltpu.get_barrier_semaphore()
    signal = lambda device: pl.semaphore_signal(barrier, inc=1, device_id=device, device_id_type=MESH)
    for k in range(1, gx * gy):
        to = (me + k) % (gx * gy)
        signal({"gx": to // gy, "gy": to % gy})
    for k in range(1, gz):
        signal({"gz": (level + k) % gz})
    for up in (-1, 0, 1):
        for side in (-1, 0, 1):
            if up or side:
                to, to_row = (line + up + gx * gz) % (gx * gz), (row + side + gy) % gy
                signal({"gx": to // gz, "gz": to % gz, "gy": to_row})
    pl.semaphore_wait(barrier, gx * gy + gz + 6)
    return line, gx * gz, row, gy, gz


def whole_kernel(setting, *refs):
    fine, coarse, scales = setting
    slab, w_a, b_a, pool, w_b, b_b, cot, v_b, spread, v_a = refs[:10]
    features, grad_slab, out_wa, out_ba, out_wb, out_bb = refs[10:16]
    wide_a, wide_b, wide_gb, wide_ga, win_a, win_b, win_gb, win_ga = refs[16:24]
    before_a, pooled, grad_b, grad_a, acc_a, acc_b = refs[24:30]
    parts_a, parts_b, sems = refs[30:35], refs[35:40], refs[40:]
    for wide in (wide_a, wide_b, wide_gb, wide_ga):
        wide[...] = jnp.zeros_like(wide)
    place(wide_a, slab, fine)
    where = greet()
    halos = [
        Halo(wide, dims, where, sems[:2], 10 * i)
        for i, (wide, dims) in enumerate(
            ((wide_a, fine), (wide_b, coarse), (wide_gb, coarse), (wide_ga, fine))
        )
    ]
    sum_a = Summing(acc_a, *parts_a, sems[2])
    sum_b = Summing(acc_b, *parts_b, sems[3])

    halos[0].start()
    halos[0].wait()
    forward_a_kernel(fine, wide_a, w_a, b_a, pool, before_a, pooled, win_a)
    place(wide_b, pooled, coarse)
    halos[1].start()
    halos[1].wait()
    top_b = out_wb.shape[0]
    middle_kernel(
        coarse, wide_b, w_b, b_b, cot, features, grad_b, acc_b.at[:top_b], acc_b.at[top_b : top_b + 8], win_b
    )
    place(wide_gb, grad_b, coarse)
    halos[2].start()
    acc_b[top_b + 8 :] = jnp.zeros((acc_b.shape[0] - top_b - 8, acc_b.shape[1]), jnp.float32)
    sum_b.start()
    halos[2].wait()
    backward_b_kernel(coarse, fine, wide_gb, v_b, before_a, spread, grad_a, win_gb)
    place(wide_ga, grad_a, fine)
    halos[3].start()
    grad = grad_a[...]
    half, width = out_wa.shape[0] // 2, out_wa.shape[1]
    acc_a[:half, :width] = dot_rows(win_a[:half], grad)
    acc_a[:half, width:] = dot_rows(win_a[half:], grad)
    acc_a[half:] = jnp.zeros((acc_a.shape[0] - half, acc_a.shape[1]), jnp.float32)
    acc_a[half : half + 8, :width] = dot_rows(jnp.ones((8, grad.shape[1]), jnp.bfloat16), grad)
    sum_a.start()
    sum_b.middle()
    halos[3].wait()
    backward_a_kernel(fine, wide_ga, v_a, grad_slab, win_ga)
    sum_a.middle()
    sum_b.last()
    sum_a.last()
    sum_b.finish()
    all_a, all_b = parts_a[4], parts_b[4]
    scale_a, scale_b = scales
    flat_b = all_b[...].astype(jnp.float32).reshape(-1, all_b.shape[2]) * scale_b
    out_wb[...] = flat_b[:top_b]
    out_bb[...] = flat_b[top_b : top_b + 1]
    sum_a.finish()
    flat_a = all_a[...].astype(jnp.float32).reshape(-1, all_a.shape[2]) * scale_a
    out_wa[:half] = flat_a[:half, :width]
    out_wa[half:] = flat_a[:half, width:]
    out_ba[...] = flat_a[half : half + 1, :width]


def between_exchanges(fine, coarse, scales, slab, weight_a, bias_a, weight_b, bias_b, cot, pool):
    f32, bf16 = jnp.float32, jnp.bfloat16
    c1, cells = slab.shape
    c2, c3 = weight_b.shape[3:]
    fewer = cells // 8
    members, levels = lax.axis_size("gx") * lax.axis_size("gy"), lax.axis_size("gz")
    rows_a = 27 * c1 // 2 + 16
    rows_a += -rows_a % (16 * members)
    rows_b = 27 * c2 + 16
    rows_b += -rows_b % (16 * members)
    extent = lambda dims: (dims[0] + 2) * (dims[1] + 2) * dims[2]
    setting = (fine, coarse, scales)
    buffers = []
    for rows in (rows_a, rows_b):
        chunk = rows // members
        buffers += [
            pltpu.VMEM((members, chunk, 128), bf16),
            pltpu.VMEM((members, chunk, 128), bf16),
            pltpu.VMEM((chunk, 128), bf16),
            pltpu.VMEM((levels, chunk, 128), bf16),
            pltpu.VMEM((members, chunk, 128), bf16),
        ]
    outs = [
        ((c3, fewer), bf16),
        ((c1, cells), bf16),
        ((27 * c1, c2), f32),
        ((1, c2), f32),
        ((27 * c2, c3), f32),
        ((1, c3), f32),
    ]
    operands = (
        slab,
        outward(weight_a),
        bias_a[:, None],
        pool,
        outward(weight_b),
        bias_b[:, None],
        cot,
        inward(weight_b),
        pool.T.astype(bf16),
        inward(weight_a),
    )
    most = max(members, levels)
    return pl.pallas_call(
        functools.partial(whole_kernel, setting),
        out_shape=[jax.ShapeDtypeStruct(shape, dtype) for shape, dtype in outs],
        in_specs=[pl.BlockSpec(memory_space=pltpu.VMEM)] * len(operands),
        out_specs=[pl.BlockSpec(memory_space=pltpu.VMEM)] * len(outs),
        scratch_shapes=[
            pltpu.VMEM((c1, extent(fine)), bf16),
            pltpu.VMEM((c2, extent(coarse)), bf16),
            pltpu.VMEM((c3, extent(coarse)), bf16),
            pltpu.VMEM((c2, extent(fine)), bf16),
            pltpu.VMEM((27 * c1, cells), bf16),
            pltpu.VMEM((27 * c2, fewer), bf16),
            pltpu.VMEM((27 * c3, fewer), bf16),
            pltpu.VMEM((27 * c2, cells), bf16),
            pltpu.VMEM((c2, cells), f32),
            pltpu.VMEM((c2, fewer), bf16),
            pltpu.VMEM((c3, fewer), bf16),
            pltpu.VMEM((c2, cells), bf16),
            pltpu.VMEM((rows_a, 128), f32),
            pltpu.VMEM((rows_b, 128), f32),
            *buffers,
            pltpu.SemaphoreType.DMA((40,)),
            pltpu.SemaphoreType.DMA((40,)),
            pltpu.SemaphoreType.DMA((3, 2, most)),
            pltpu.SemaphoreType.DMA((3, 2, most)),
        ],
        compiler_params=pltpu.CompilerParams(
            collective_id=1, has_side_effects=True, vmem_limit_bytes=60 * 2**20
        ),
    )(*operands)


def outward(weight):
    return weight.reshape(-1, weight.shape[-1]).T


def inward(weight):
    taps = weight[::-1, ::-1, ::-1].reshape(27, *weight.shape[3:])
    return jnp.transpose(taps, (1, 0, 2)).reshape(weight.shape[3], -1)


def on_device(volume, weight_a, bias_a, weight_b, bias_b, cotangent):
    f32, bf16 = jnp.float32, jnp.bfloat16
    count = lax.axis_size("gz")
    devices_all = lax.axis_size("gx") * lax.axis_size("gy") * count
    c1, nx, rows, nz = volume.shape
    cells = nx * rows * nz
    scale_a = 1.0 / math.sqrt(cells * devices_all)
    scale_b = 1.0 / math.sqrt(cells * devices_all // 8)
    c2, c3 = weight_b.shape[3:]
    planes, depth = nx // count, nz * count
    fine = (planes, rows, depth)
    coarse = (planes // 2, rows // 2, depth // 2)
    fewer = cells // 8
    pool = (jnp.arange(depth)[:, None] // 2 == jnp.arange(depth // 2)[None]).astype(f32)

    slab = lax.all_to_all(volume, "gz", split_axis=1, concat_axis=3, tiled=True).reshape(c1, cells)
    features, grad_slab, sum_wa, sum_ba, sum_wb, sum_bb = between_exchanges(
        fine,
        coarse,
        (scale_a, scale_b),
        slab,
        weight_a,
        bias_a,
        weight_b,
        bias_b,
        cotangent.reshape(c3, fewer),
        pool,
    )
    grad_input = lax.all_to_all(
        grad_slab.reshape(c1, planes, rows, depth), "gz", split_axis=3, concat_axis=1, tiled=True
    )
    return (
        features.reshape(cotangent.shape),
        grad_input,
        sum_wa.reshape(weight_a.shape),
        sum_ba.reshape(c2),
        sum_wb.reshape(weight_b.shape),
        sum_bb.reshape(c3),
    )


def solution(mesh):
    return jax.shard_map(
        on_device,
        mesh=mesh,
        in_specs=(P(None, "gx", "gy", "gz"), P(), P(), P(), P(), P(None, ("gx", "gz"), "gy", None)),
        out_specs=(
            P(None, ("gx", "gz"), "gy", None),
            P(None, "gx", "gy", "gz"),
            P(),
            P(),
            P(),
            P(),
        ),
        check_vma=False,
    )
```

```python
import functools
import math

import jax
import jax.numpy as jnp
from jax import lax
from jax.experimental import pallas as pl
from jax.experimental.pallas import tpu as pltpu
from jax.sharding import PartitionSpec as P

MESH = pl.DeviceIdType.MESH
LANES = 128
BOTH = (0, 1)
NEAR = (-1, 0, 1)


def slope_of(value):
    sigma = jax.nn.sigmoid(value)
    return sigma + value * sigma * (1.0 - sigma)


def dot(left, right):
    return jnp.dot(left, right, preferred_element_type=jnp.float32)


def dot_rows(left, right):
    return lax.dot_general(
        left, right, (((1,), (1,)), ((), ())), preferred_element_type=jnp.float32
    )


def roll(value, by):
    by = by % LANES
    return pltpu.roll(value, by, 1) if by else value


def lanes_at(index, count=1):
    begin = index * LANES
    if not isinstance(begin, int):
        begin = pl.multiple_of(begin, LANES)
    return pl.ds(begin, count * LANES)


def within(at, count):
    return (at >= 0) & (at < count)


class Grid:
    def __init__(self, nx, ny, nz):
        self.ny, self.nz = ny, nz
        self.plane = ny * nz
        self.fold = LANES // self.plane
        self.tiles = nx // self.fold
        self.zpacks = -(-self.tiles // nz)
        self.ypacks = -(-self.tiles // ny)
        self.group = max(ny, min(nz, self.tiles))

    def at(self, rows):
        lane = lax.broadcasted_iota(jnp.int32, (rows, LANES), 1)
        return lane // self.plane, lane // self.nz % self.ny, lane % self.nz

    def corner_groups(self, channels):
        return min(channels // 16, self.nz // self.ypacks)


class Exchange:
    def __init__(self, grid, channels, buffers, sems, at):
        self.grid, self.channels = grid, channels
        self.zs, self.zr, self.ys, self.yr, self.cs, self.cr, self.xs, self.xr = buffers
        self.gx, self.gy, self.gz = [lax.axis_index(axis) for axis in ("gx", "gy", "gz")]
        cuts_y, cuts_z = lax.axis_size("gy"), lax.axis_size("gz")
        moves = []
        step = (1, -1)
        for side in BOTH:
            moves.append((self.ys.at[side], self.yr.at[side], 0, step[side], 0))
        for dy in NEAR:
            for dz in NEAR:
                moves.append((self.xs, self.xr.at[(1 - dy) * 3 + 1 - dz], 1, dy, dz))
        for side in BOTH:
            moves.append((self.zs.at[side], self.zr.at[side], 0, 0, step[side]))
        for sy in BOTH:
            for sz in BOTH:
                i = sy * 2 + sz
                moves.append((self.cs.at[i], self.cr.at[i], 0, step[sy], step[sz]))
        self.moves = []
        for i, (source, target, across, dy, dz) in enumerate(moves):
            copy = pltpu.make_async_remote_copy(
                src_ref=source,
                dst_ref=target,
                send_sem=sems.at[0, at, i],
                recv_sem=sems.at[1, at, i],
                device_id={
                    "gx": (self.gx + across) % 2,
                    "gy": (self.gy + dy + cuts_y) % cuts_y,
                    "gz": (self.gz + dz + cuts_z) % cuts_z,
                },
                device_id_type=MESH,
            )
            goes = within(self.gy + dy, cuts_y) & within(self.gz + dz, cuts_z)
            comes = within(self.gy - dy, cuts_y) & within(self.gz - dz, cuts_z)
            self.moves.append((copy, goes, comes))

    def clear(self):
        for ref in (self.zr, self.yr, self.cr, self.xr):
            ref[...] = jnp.zeros_like(ref)

    def pack(self, field):
        grid, c = self.grid, self.channels
        spot, y, z = grid.at(c)
        last_z, last_y = grid.nz - 1, grid.ny - 1
        ends = [field[:, lanes_at(t)] for t in (grid.tiles - 1, 0)]
        if grid.fold == 1:
            self.xs[...] = jnp.where(spot + self.gx == 0, *ends)
        else:
            part = c // grid.fold
            place = grid.at(part)[0]
            made = []
            for end, i in zip(ends, (grid.fold - 1, 0)):
                out = end[:part]
                out = roll(out, grid.plane * -i)
                for j in range(1, grid.fold):
                    piece = roll(end[j * part : (j + 1) * part], grid.plane * (j - i))
                    out = jnp.where(place == j, piece, out)
                made.append(out)
            self.xs[...] = jnp.where(place * 0 + self.gx == 0, *made)

        def one(q, carry):
            held = [None, None]
            rows = [None, None]
            for k in range(grid.group):
                tile = field[:, lanes_at(q * grid.group + k)]
                j = k % grid.ny
                for side in BOTH:
                    piece = roll(tile, k - last_z if side == 0 else k)
                    held[side] = piece if k == 0 else jnp.where(z == k, piece, held[side])
                    piece = roll(tile, grid.nz * (j - last_y if side == 0 else j))
                    rows[side] = piece if j == 0 else jnp.where(y == j, piece, rows[side])
                    if j == last_y:
                        self.ys[side, :, lanes_at(q * (grid.group // grid.ny) + k // grid.ny)] = rows[side]
            for side in BOTH:
                self.zs[side, :, lanes_at(q)] = held[side]
            return carry

        loops = grid.tiles // grid.group
        if loops == 1:
            one(0, 0)
        else:
            lax.fori_loop(0, loops, one, 0)
        groups, packs = grid.corner_groups(c), grid.ypacks
        part = c // groups
        z = grid.at(part)[2]
        for sy in BOTH:
            for sz in BOTH:
                out = None
                for j in range(groups):
                    for p in range(packs):
                        to = packs * j + p
                        piece = self.ys[sy, j * part : (j + 1) * part, lanes_at(p)]
                        piece = roll(piece, to - (last_z if sz == 0 else 0))
                        out = piece if out is None else jnp.where(z == to, piece, out)
                self.cs[sy * 2 + sz] = out

    def start(self):
        for copy, goes, _ in self.moves:
            pl.when(goes)(copy.start)

    def wait(self):
        for copy, goes, comes in self.moves:
            pl.when(goes)(copy.wait_send)
            pl.when(comes)(copy.wait_recv)

    def shift_z(self, tile, low, high, dz, z):
        if dz == 0:
            return tile
        if dz < 0:
            return jnp.where(z == 0, low, roll(tile, 1))
        return jnp.where(z == self.grid.nz - 1, high, roll(tile, -1))

    def shift_y(self, tile, low, high, dy, y):
        if dy == 0:
            return tile
        if dy < 0:
            return jnp.where(y == 0, low, roll(tile, self.grid.nz))
        return jnp.where(y == self.grid.ny - 1, high, roll(tile, -self.grid.nz))

    def beyond(self):
        grid, c = self.grid, self.channels
        _, y, z = grid.at(c)
        if grid.fold == 1:
            came = [self.xr[i] for i in range(9)]
        else:
            last = grid.fold - 1
            came = [
                jnp.concatenate([roll(self.xr[i], grid.plane * (last - j)) for j in range(grid.fold)], axis=0)
                for i in range(9)
            ]
        along = grid.nz * (grid.ny - 1)
        rows = []
        for dy in range(3):
            low, here, high = came[dy * 3 : dy * 3 + 3]
            low, high = roll(low, 1 - grid.nz), roll(high, grid.nz - 1)
            rows.append([self.shift_z(here, low, high, dz, z) for dz in NEAR])
        return [
            self.shift_y(rows[1][dz], roll(rows[0][dz], -along), roll(rows[2][dz], along), dy, y)
            for dy in NEAR
            for dz in range(3)
        ]

    def strips(self, shifted):
        grid, c = self.grid, self.channels
        groups, packs = grid.corner_groups(c), grid.ypacks
        _, _, z = grid.at(c)
        for side in BOTH:
            for p in range(packs):
                tile = self.yr[side, :, lanes_at(p)]
                ends = []
                for sz in BOTH:
                    to = 0 if sz == 0 else grid.nz - 1
                    corner = self.cr[side * 2 + sz]
                    ends.append(
                        jnp.concatenate([roll(corner, to - packs * j - p) for j in range(groups)], axis=0)
                    )
                for dz in NEAR:
                    shifted[side * 3 + dz + 1, :, lanes_at(p)] = self.shift_z(tile, *ends, dz, z)

    def tile_shifts(self, field, shifted, q, k):
        grid, c = self.grid, self.channels
        _, y, z = grid.at(c)
        last_z, last_y = grid.nz - 1, grid.ny - 1
        tile = field[:, lanes_at(q * grid.group + k)]
        low = roll(self.zr[0, :, lanes_at(q)], -k)
        high = roll(self.zr[1, :, lanes_at(q)], last_z - k)
        moved = [self.shift_z(tile, low, high, dz, z) for dz in NEAR]
        p, j = q * (grid.group // grid.ny) + k // grid.ny, k % grid.ny
        out = []
        for dy in NEAR:
            for dz in range(3):
                low = high = None
                if dy < 0:
                    low = roll(shifted[dz, :, lanes_at(p)], -grid.nz * j)
                if dy > 0:
                    high = roll(shifted[3 + dz, :, lanes_at(p)], grid.nz * (last_y - j))
                out.append(self.shift_y(moved[dz], low, high, dy, y))
        return out

    def only(self, value, side):
        flag = lax.broadcasted_iota(jnp.int32, value.shape, 1) * 0 + self.gx
        return jnp.where(flag == side, value, jnp.zeros_like(value))

    def fine_windows(self, field, shifted, windows):
        grid, c = self.grid, self.channels
        self.strips(shifted)
        for i, value in enumerate(self.beyond()):
            windows[i * c : (i + 1) * c, lanes_at(0)] = self.only(value, 1)
            windows[i * c : (i + 1) * c, lanes_at(grid.tiles + 1)] = self.only(value, 0)

        def one(q, carry):
            for k in range(grid.group):
                for i, value in enumerate(self.tile_shifts(field, shifted, q, k)):
                    windows[i * c : (i + 1) * c, lanes_at(q * grid.group + k + 1)] = value
            return carry

        lax.fori_loop(0, grid.tiles // grid.group, one, 0)

    def coarse_windows(self, field, shifted, windows):
        grid, c = self.grid, self.channels
        spot = grid.at(c)[0]
        self.strips(shifted)
        outer = self.beyond()
        tiles = [self.tile_shifts(field, shifted, 0, k) for k in range(grid.tiles)]
        for i in range(9):
            low = roll(self.only(outer[i], 1), grid.plane)
            high = self.only(outer[i], 0)
            rows = [slice((dx * 9 + i) * c, (dx * 9 + i + 1) * c) for dx in range(3)]
            up = [roll(tile[i], grid.plane) for tile in tiles]
            down = [roll(tile[i], -grid.plane) for tile in tiles]
            for t in range(grid.tiles):
                before = up[t - 1] if t else low
                after = down[t + 1] if t + 1 < grid.tiles else high
                windows[rows[0], lanes_at(t)] = jnp.where(spot == 0, before, up[t])
                windows[rows[1], lanes_at(t)] = tiles[t][i]
                windows[rows[2], lanes_at(t)] = jnp.where(spot == grid.fold - 1, after, down[t])


class Summing:
    def __init__(self, acc, stage, first, mine, second, whole, sems):
        self.acc, self.stage, self.first = acc, stage, first
        self.mine, self.second, self.whole = mine, second, whole
        self.sems = sems
        gy = lax.axis_size("gy")
        self.count = lax.axis_size("gx") * gy
        self.depth = lax.axis_size("gz")
        self.me = lax.axis_index("gx") * gy + lax.axis_index("gy")
        self.level = lax.axis_index("gz")

    def across(self, phase, k, source, target):
        gy = lax.axis_size("gy")
        to = (self.me + k) % self.count
        return pltpu.make_async_remote_copy(
            src_ref=source(to),
            dst_ref=target,
            send_sem=self.sems.at[phase, 0, k],
            recv_sem=self.sems.at[phase, 1, k],
            device_id={"gx": to // gy, "gy": to % gy},
            device_id_type=MESH,
        )

    def along(self, k):
        return pltpu.make_async_remote_copy(
            src_ref=self.mine,
            dst_ref=self.second.at[self.level],
            send_sem=self.sems.at[1, 0, k],
            recv_sem=self.sems.at[1, 1, k],
            device_id={"gz": (self.level + k) % self.depth},
            device_id_type=MESH,
        )

    def scatters(self):
        return [
            self.across(0, k, lambda to: self.stage.at[to], self.first.at[self.me])
            for k in range(1, self.count)
        ]

    def alongs(self):
        return [self.along(k) for k in range(1, self.depth)]

    def gathers(self):
        here = self.whole.at[self.me]
        return [self.across(2, k, lambda to: here, here) for k in range(1, self.count)]

    def start(self):
        chunk = self.stage.shape[1]
        for i in range(self.count):
            self.stage[i] = self.acc[i * chunk : (i + 1) * chunk].astype(jnp.bfloat16)
        for copy in self.scatters():
            copy.start()
        self.first[self.me] = self.stage[self.me]

    def total(self, parts):
        total = parts[0].astype(jnp.float32)
        for i in range(1, parts.shape[0]):
            total = total + parts[i].astype(jnp.float32)
        return total.astype(jnp.bfloat16)

    def middle(self):
        for copy in self.scatters():
            copy.wait()
        part = self.total(self.first)
        self.mine[...] = part
        for copy in self.alongs():
            copy.start()
        self.second[self.level] = part

    def last(self):
        for copy in self.alongs():
            copy.wait()
        self.whole[self.me] = self.total(self.second)
        for copy in self.gathers():
            copy.start()

    def finish(self):
        for copy in self.gathers():
            copy.wait()


class Slabs:
    def __init__(self, sent, came, sems, grid):
        self.sent, self.came, self.sems, self.grid = sent, came, sems, grid
        self.depth, self.level = lax.axis_size("gz"), lax.axis_index("gz")

    def copies(self):
        out = []
        for k in range(1, self.depth):
            to = (self.level + k) % self.depth
            out.append(
                pltpu.make_async_remote_copy(
                    src_ref=self.sent.at[to],
                    dst_ref=self.came.at[self.level],
                    send_sem=self.sems.at[0, k],
                    recv_sem=self.sems.at[1, k],
                    device_id={"gz": to},
                    device_id_type=MESH,
                )
            )
        return out

    def pack(self, field):
        fold, plane = self.grid.fold, self.grid.plane
        part = self.sent.shape[1]
        spot = self.grid.at(part)[0]
        for t in range(self.grid.tiles):
            for i in range(fold):
                out = None
                for j in range(fold):
                    piece = roll(field[j * part : (j + 1) * part, lanes_at(t)], plane * (j - i))
                    out = piece if out is None else jnp.where(spot == j, piece, out)
                self.sent[t * fold + i] = out
        for copy in self.copies():
            copy.start()
        self.came[self.level] = self.sent[self.level]

    def unpack(self, field):
        for copy in self.copies():
            copy.wait()
        fold, plane = self.grid.fold, self.grid.plane
        part = self.came.shape[1]
        spot = self.grid.at(part)[0]
        for t in range(self.grid.tiles):
            for j in range(fold):
                out = None
                for i in range(fold):
                    piece = roll(self.came[t * fold + i], plane * (i - j))
                    out = piece if out is None else jnp.where(spot == i, piece, out)
                field[j * part : (j + 1) * part, lanes_at(t)] = out


def greet():
    gx, gy, gz = [lax.axis_size(axis) for axis in ("gx", "gy", "gz")]
    me = lax.axis_index("gx") * gy + lax.axis_index("gy")
    level, row, half = lax.axis_index("gz"), lax.axis_index("gy"), lax.axis_index("gx")
    barrier = pltpu.get_barrier_semaphore()
    signal = lambda device: pl.semaphore_signal(barrier, inc=1, device_id=device, device_id_type=MESH)
    for k in range(1, gx * gy):
        to = (me + k) % (gx * gy)
        signal({"gx": to // gy, "gy": to % gy})
    for k in range(1, gz):
        signal({"gz": (level + k) % gz})
    extra = 0
    for across in BOTH:
        for dy in NEAR:
            for dz in NEAR:
                if dz and (across or dy):
                    extra += 1
                    signal(
                        {
                            "gx": (half + across) % gx,
                            "gy": (row + dy + gy) % gy,
                            "gz": (level + dz + gz) % gz,
                        }
                    )
    return barrier, gx * gy + gz - 2 + extra


def spread_map(fine, coarse):
    shape = (LANES, coarse.fold * LANES)
    small = lax.broadcasted_iota(jnp.int32, shape, 0)
    large = lax.broadcasted_iota(jnp.int32, shape, 1)
    y, z = large % LANES // fine.nz, large % fine.nz
    match = (
        (small // coarse.plane == large // LANES)
        & (small // coarse.nz % coarse.ny == y // 2)
        & (small % coarse.nz == z // 2)
    )
    ones = match.astype(jnp.float32)
    first = (match & (y % 2 == 0) & (z % 2 == 0)).astype(jnp.float32)
    return ones.astype(jnp.bfloat16), first.astype(jnp.bfloat16)


def order_map(coarse, count):
    shape = (coarse.plane * count,) * 2
    row = lax.broadcasted_iota(jnp.int32, shape, 0)
    column = lax.broadcasted_iota(jnp.int32, shape, 1)
    wide = count * coarse.nz
    match = (
        (row // wide == column // coarse.nz % coarse.ny)
        & (row % wide // coarse.nz == column // coarse.plane)
        & (row % coarse.nz == column % coarse.nz)
    )
    return match.astype(jnp.float32).astype(jnp.bfloat16)


def column_of(row):
    size = row.shape[1]
    across = lax.broadcasted_iota(jnp.int32, (size, size), 0)
    down = lax.broadcasted_iota(jnp.int32, (size, size), 1)
    return jnp.sum(jnp.where(across == down, row, 0.0), axis=1, keepdims=True)


def whole_kernel(setting, *refs):
    fine_size, coarse_size, scales, names = setting
    fine, coarse = Grid(*fine_size), Grid(*coarse_size)
    named = dict(zip(names, refs))
    r = lambda name: named[name]
    fields = ("a", "b", "gb", "ga")
    grids = (fine, coarse, coarse, fine)
    volume, w_a, b_a, w_b, b_b, cot = [r(n) for n in ("volume", "w_a", "b_a", "w_b", "b_b", "cot")]
    features, grad_in, out_wa, out_ba, out_wb, out_bb = [
        r(n) for n in ("features", "grad_in", "out_wa", "out_ba", "out_wb", "out_bb")
    ]
    c1, c2, c3 = volume.shape[0], w_a.shape[1], w_b.shape[1]
    widths = dict(zip(fields, (c1, c2, c3, c2)))
    halos = {
        name: Exchange(
            grid,
            widths[name],
            [r(name + part) for part in ("_zs", "_zr", "_ys", "_yr", "_cs", "_cr", "_xs", "_xr")],
            r("halo_sems"),
            i,
        )
        for i, (name, grid) in enumerate(zip(fields, grids))
    }
    strips = {name: r(name + "_strips") for name in fields}
    win_a, win_b, win_gb, win_ga = [r(name + "_win") for name in fields]
    before_a, pooled, grad_b, grad_a = [r(n) for n in ("before_a", "pooled", "grad_b", "grad_a")]
    acc_a, acc_b, mixed, feat = [r(n) for n in ("acc_a", "acc_b", "mixed", "feat")]
    sum_a = Summing(acc_a, *[r(f"sum_a{i}") for i in range(5)], r("sum_sems").at[0])
    sum_b = Summing(acc_b, *[r(f"sum_b{i}") for i in range(5)], r("sum_sems").at[1])
    cots = Slabs(r("cot_sent"), r("cot_came"), r("slab_sems").at[0], coarse)
    feats = Slabs(r("feat_sent"), r("feat_came"), r("slab_sems").at[1], coarse)
    out_a, in_a, out_b, in_b, spread, thin, order = [
        r(n) for n in ("to_a", "from_a", "to_b", "from_b", "spread", "thin", "order")
    ]
    bf16 = jnp.bfloat16

    for name in fields:
        halos[name].clear()
    barrier, arrivals = greet()
    halos["a"].pack(volume)
    order[...] = order_map(coarse, lax.axis_size("gz"))
    mixed[...] = dot(cot[...], order[...]).astype(bf16)
    pl.semaphore_wait(barrier, arrivals)
    halos["a"].start()
    cots.pack(mixed)

    taps = 9
    for dx in range(3):
        out_a[dx] = w_a[dx * taps * c1 : (dx + 1) * taps * c1].T
        for k in range(taps):
            tap = 26 - dx * taps - k
            in_a[dx, :, k * c2 : (k + 1) * c2] = w_a[tap * c1 : (tap + 1) * c1]
    out_b[...] = w_b[...].T
    for k in range(27):
        in_b[:, k * c3 : (k + 1) * c3] = w_b[(26 - k) * c2 : (27 - k) * c2]
    wide, narrow = spread_map(fine, coarse)
    spread[...] = wide
    thin[...] = narrow
    bias_a, bias_b = column_of(b_a[...]), column_of(b_b[...])
    acc_a[...] = jnp.zeros_like(acc_a)
    acc_b[...] = jnp.zeros_like(acc_b)

    halos["a"].wait()
    halos["a"].fine_windows(volume, strips["a"], win_a)
    many = 2 * coarse.fold

    def forward_a(g, carry):
        before = bias_a
        for dx in range(3):
            before = before + dot(out_a[dx], win_a[:, lanes_at(g * many + dx, many)])
        before_a[:, lanes_at(g * many, many)] = before
        active = before * jax.nn.sigmoid(before)
        pieces = []
        for i in range(coarse.fold):
            first = active[:, 2 * i * LANES : (2 * i + 1) * LANES]
            pair = first + active[:, (2 * i + 1) * LANES : (2 * i + 2) * LANES]
            pair = pair + roll(pair, -1)
            pair = pair + roll(pair, -fine.nz)
            pieces.append((pair * 0.125).astype(bf16))
        pooled[:, lanes_at(g)] = dot_rows(jnp.concatenate(pieces, axis=1), thin[...]).astype(bf16)
        return carry

    lax.fori_loop(0, coarse.tiles, forward_a, 0)
    halos["b"].pack(pooled)
    halos["b"].start()
    cots.unpack(mixed)
    halos["b"].wait()
    halos["b"].coarse_windows(pooled, strips["b"], win_b)
    before = dot(out_b[...], win_b[...]) + bias_b
    grad_b[...] = (mixed[...].astype(jnp.float32) * slope_of(before)).astype(bf16)
    halos["gb"].pack(grad_b)
    halos["gb"].start()
    feat[...] = (before * jax.nn.sigmoid(before)).astype(bf16)
    feats.pack(feat)
    top_b = out_wb.shape[0]
    grad = grad_b[...]
    acc_b[:top_b] = dot_rows(win_b[...], grad)
    acc_b[top_b : top_b + 8] = dot_rows(jnp.ones((8, grad.shape[1]), bf16), grad)
    sum_b.start()
    halos["gb"].wait()
    halos["gb"].coarse_windows(grad_b, strips["gb"], win_gb)
    pooled[...] = dot(in_b[...], win_gb[...]).astype(bf16)

    def backward_b(g, carry):
        wide = dot(pooled[:, lanes_at(g)], spread[...]) * 0.125
        for i in range(coarse.fold):
            for j in BOTH:
                here = lanes_at(g * many + 2 * i + j)
                slope = slope_of(before_a[:, here])
                grad_a[:, here] = (wide[:, i * LANES : (i + 1) * LANES] * slope).astype(bf16)
        return carry

    lax.fori_loop(0, coarse.tiles, backward_b, 0)
    halos["ga"].pack(grad_a)
    halos["ga"].start()
    grad = grad_a[...]
    half, width = out_wa.shape[0] // 2, out_wa.shape[1]
    parts = [dot_rows(win_a[:, lanes_at(dx, fine.tiles)], grad) for dx in range(3)]
    whole = jnp.concatenate(parts, axis=0)
    acc_a[:half, :width] = whole[:half]
    acc_a[:half, width:] = whole[half:]
    acc_a[half : half + 8, :width] = dot_rows(jnp.ones((8, grad.shape[1]), bf16), grad)
    sum_a.start()
    sum_b.middle()
    halos["ga"].wait()
    halos["ga"].fine_windows(grad_a, strips["ga"], win_ga)

    def backward_a(g, carry):
        total = dot(in_a[0], win_ga[:, lanes_at(g * many, many)])
        for dx in (1, 2):
            total = total + dot(in_a[dx], win_ga[:, lanes_at(g * many + dx, many)])
        grad_in[:, lanes_at(g * many, many)] = total.astype(bf16)
        return carry

    lax.fori_loop(0, coarse.tiles, backward_a, 0)
    sum_a.middle()
    feats.unpack(feat)
    features[...] = dot_rows(feat[...], order[...]).astype(bf16)
    sum_b.last()
    sum_a.last()
    sum_b.finish()
    all_a, all_b = r("sum_a4"), r("sum_b4")
    scale_a, scale_b = scales
    flat_b = all_b[...].astype(jnp.float32).reshape(-1, all_b.shape[2]) * scale_b
    out_wb[...] = flat_b[:top_b]
    out_bb[...] = flat_b[top_b : top_b + 1]
    sum_a.finish()
    flat_a = all_a[...].astype(jnp.float32).reshape(-1, all_a.shape[2]) * scale_a
    out_wa[:half] = flat_a[:half, :width]
    out_wa[half:] = flat_a[:half, width:]
    out_ba[...] = flat_a[half : half + 1, :width]


def on_device(volume, weight_a, bias_a, weight_b, bias_b, cotangent):
    f32, bf16 = jnp.float32, jnp.bfloat16
    members, levels = lax.axis_size("gx") * lax.axis_size("gy"), lax.axis_size("gz")
    c1, nx, ny, nz = volume.shape
    c2, c3 = weight_b.shape[3:]
    cells = nx * ny * nz
    fewer = cells // 8
    scale_a = 1.0 / math.sqrt(cells * members * levels)
    scale_b = 1.0 / math.sqrt(cells * members * levels // 8)
    fine_size, coarse_size = (nx, ny, nz), (nx // 2, ny // 2, nz // 2)
    fine, coarse = Grid(*fine_size), Grid(*coarse_size)
    rows_a = 27 * c1 // 2 + 16
    rows_a += -rows_a % (16 * members)
    rows_b = 27 * c2 + 16
    rows_b += -rows_b % (16 * members)
    operands = {
        "volume": volume.reshape(c1, cells),
        "w_a": weight_a.reshape(27 * c1, c2),
        "b_a": bias_a.reshape(1, c2),
        "w_b": weight_b.reshape(27 * c2, c3),
        "b_b": bias_b.reshape(1, c3),
        "cot": cotangent.reshape(c3, fewer),
    }
    outs = {
        "features": ((c3, fewer), bf16),
        "grad_in": ((c1, cells), bf16),
        "out_wa": ((27 * c1, c2), f32),
        "out_ba": ((1, c2), f32),
        "out_wb": ((27 * c2, c3), f32),
        "out_bb": ((1, c3), f32),
    }
    scratch = {}
    for name, grid, c in (("a", fine, c1), ("b", coarse, c2), ("gb", coarse, c3), ("ga", fine, c2)):
        for end in ("s", "r"):
            scratch[f"{name}_z{end}"] = pltpu.VMEM((2, c, grid.zpacks * LANES), bf16)
            scratch[f"{name}_y{end}"] = pltpu.VMEM((2, c, grid.ypacks * LANES), bf16)
            scratch[f"{name}_c{end}"] = pltpu.VMEM((4, c // grid.corner_groups(c), LANES), bf16)
        scratch[f"{name}_xs"] = pltpu.VMEM((c // grid.fold, LANES), bf16)
        scratch[f"{name}_xr"] = pltpu.VMEM((9, c // grid.fold, LANES), bf16)
        scratch[f"{name}_strips"] = pltpu.VMEM((6, c, grid.ypacks * LANES), bf16)
        shape = (9 * c, (grid.tiles + 2) * LANES) if grid is fine else (27 * c, grid.tiles * LANES)
        scratch[f"{name}_win"] = pltpu.VMEM(shape, bf16)
    scratch["before_a"] = pltpu.VMEM((c2, cells), f32)
    scratch["pooled"] = pltpu.VMEM((c2, fewer), bf16)
    scratch["grad_b"] = pltpu.VMEM((c3, fewer), bf16)
    scratch["grad_a"] = pltpu.VMEM((c2, cells), bf16)
    scratch["mixed"] = pltpu.VMEM((c3, fewer), bf16)
    scratch["feat"] = pltpu.VMEM((c3, fewer), bf16)
    for name, rows in (("a", rows_a), ("b", rows_b)):
        chunk = rows // members
        scratch[f"acc_{name}"] = pltpu.VMEM((rows, LANES), f32)
        for i, shape in enumerate(
            ((members, chunk), (members, chunk), (chunk,), (levels, chunk), (members, chunk))
        ):
            scratch[f"sum_{name}{i}"] = pltpu.VMEM((*shape, LANES), bf16)
    for name in ("cot_sent", "cot_came", "feat_sent", "feat_came"):
        scratch[name] = pltpu.VMEM((levels, c3 // coarse.fold, LANES), bf16)
    scratch["to_a"] = pltpu.VMEM((3, c2, 9 * c1), bf16)
    scratch["from_a"] = pltpu.VMEM((3, c1, 9 * c2), bf16)
    scratch["to_b"] = pltpu.VMEM((c3, 27 * c2), bf16)
    scratch["from_b"] = pltpu.VMEM((c2, 27 * c3), bf16)
    scratch["spread"] = pltpu.VMEM((LANES, coarse.fold * LANES), bf16)
    scratch["thin"] = pltpu.VMEM((LANES, coarse.fold * LANES), bf16)
    scratch["order"] = pltpu.VMEM((fewer, fewer), bf16)
    scratch["halo_sems"] = pltpu.SemaphoreType.DMA((2, 4, 17))
    scratch["sum_sems"] = pltpu.SemaphoreType.DMA((2, 3, 2, max(members, levels)))
    scratch["slab_sems"] = pltpu.SemaphoreType.DMA((2, 2, levels))
    names = (*operands, *outs, *scratch)
    got = pl.pallas_call(
        functools.partial(whole_kernel, (fine_size, coarse_size, (scale_a, scale_b), names)),
        out_shape=[jax.ShapeDtypeStruct(shape, dtype) for shape, dtype in outs.values()],
        in_specs=[pl.BlockSpec(memory_space=pltpu.VMEM)] * len(operands),
        out_specs=[pl.BlockSpec(memory_space=pltpu.VMEM)] * len(outs),
        scratch_shapes=list(scratch.values()),
        compiler_params=pltpu.CompilerParams(
            collective_id=1, has_side_effects=True, vmem_limit_bytes=60 * 2**20
        ),
    )(*operands.values())
    features, grad_in, sum_wa, sum_ba, sum_wb, sum_bb = got
    return (
        features.reshape(cotangent.shape),
        grad_in.reshape(volume.shape),
        sum_wa.reshape(weight_a.shape),
        sum_ba.reshape(c2),
        sum_wb.reshape(weight_b.shape),
        sum_bb.reshape(c3),
    )


def solution(mesh):
    return jax.shard_map(
        on_device,
        mesh=mesh,
        in_specs=(P(None, "gx", "gy", "gz"), P(), P(), P(), P(), P(None, ("gx", "gz"), "gy", None)),
        out_specs=(
            P(None, ("gx", "gz"), "gy", None),
            P(None, "gx", "gy", "gz"),
            P(),
            P(),
            P(),
            P(),
        ),
        check_vma=False,
    )
```

```python
import functools
import math

import jax
import jax.numpy as jnp
from jax import lax
from jax.experimental import pallas as pl
from jax.experimental.pallas import tpu as pltpu
from jax.sharding import PartitionSpec as P

MESH = pl.DeviceIdType.MESH
LANES = 128
BOTH = (0, 1)
NEAR = (-1, 0, 1)


def slope_of(value):
    sigma = jax.nn.sigmoid(value)
    return sigma + value * sigma * (1.0 - sigma)


def dot(left, right):
    return jnp.dot(left, right, preferred_element_type=jnp.float32)


def dot_rows(left, right):
    return lax.dot_general(
        left, right, (((1,), (1,)), ((), ())), preferred_element_type=jnp.float32
    )


def roll(value, by):
    by = by % LANES
    return pltpu.roll(value, by, 1) if by else value


def lanes_at(index, count=1):
    begin = index * LANES
    if not isinstance(begin, int):
        begin = pl.multiple_of(begin, LANES)
    return pl.ds(begin, count * LANES)


def within(at, count):
    return (at >= 0) & (at < count)


class Grid:
    def __init__(self, nx, ny, nz):
        self.ny, self.nz = ny, nz
        self.plane = ny * nz
        self.fold = LANES // self.plane
        self.tiles = nx // self.fold
        self.zpacks = -(-self.tiles // nz)
        self.ypacks = -(-self.tiles // ny)
        self.group = max(ny, min(nz, self.tiles))

    def at(self, rows):
        lane = lax.broadcasted_iota(jnp.int32, (rows, LANES), 1)
        return lane // self.plane, lane // self.nz % self.ny, lane % self.nz

    def corner_groups(self, channels):
        return min(channels // 16, self.nz // self.ypacks)


class Exchange:
    def __init__(self, grid, channels, buffers, sems, at):
        self.grid, self.channels = grid, channels
        self.zs, self.zr, self.ys, self.yr, self.cs, self.cr, self.xs, self.xr, self.ds, self.dr = buffers
        self.gx, self.gy, self.gz = [lax.axis_index(axis) for axis in ("gx", "gy", "gz")]
        cuts_y, cuts_z = lax.axis_size("gy"), lax.axis_size("gz")
        moves = []
        step = (1, -1)
        for side in BOTH:
            moves.append((self.ys.at[side], self.yr.at[side], 0, step[side], 0))
        for dy in NEAR:
            for dz in NEAR:
                source = self.ds.at[(1 - dy) // 2] if dy else self.xs
                target = self.dr.at[(1 - dy) // 2, 1 - dz] if dy else self.xr.at[1 - dz]
                moves.append((source, target, 1, dy, dz))
        for side in BOTH:
            moves.append((self.zs.at[side], self.zr.at[side], 0, 0, step[side]))
        for sy in BOTH:
            for sz in BOTH:
                i = sy * 2 + sz
                moves.append((self.cs.at[i], self.cr.at[i], 0, step[sy], step[sz]))
        self.moves = []
        for i, (source, target, across, dy, dz) in enumerate(moves):
            copy = pltpu.make_async_remote_copy(
                src_ref=source,
                dst_ref=target,
                send_sem=sems.at[0, at, i],
                recv_sem=sems.at[1, at, i],
                device_id={
                    "gx": (self.gx + across) % 2,
                    "gy": (self.gy + dy + cuts_y) % cuts_y,
                    "gz": (self.gz + dz + cuts_z) % cuts_z,
                },
                device_id_type=MESH,
            )
            goes = within(self.gy + dy, cuts_y) & within(self.gz + dz, cuts_z)
            comes = within(self.gy - dy, cuts_y) & within(self.gz - dz, cuts_z)
            self.moves.append((copy, goes, comes))

    def clear(self):
        for ref in (self.zr, self.yr, self.cr, self.xr, self.dr):
            ref[...] = jnp.zeros_like(ref)

    def pack(self, field):
        grid, c = self.grid, self.channels
        spot, y, z = grid.at(c)
        last_z, last_y = grid.nz - 1, grid.ny - 1
        ends = [field[:, lanes_at(t)] for t in (grid.tiles - 1, 0)]
        if grid.fold == 1:
            self.xs[...] = jnp.where(spot + self.gx == 0, *ends)
        else:
            part = c // grid.fold
            place = grid.at(part)[0]
            made = []
            for end, i in zip(ends, (grid.fold - 1, 0)):
                out = end[:part]
                out = roll(out, grid.plane * -i)
                for j in range(1, grid.fold):
                    piece = roll(end[j * part : (j + 1) * part], grid.plane * (j - i))
                    out = jnp.where(place == j, piece, out)
                made.append(out)
            self.xs[...] = jnp.where(place * 0 + self.gx == 0, *made)

        groups = c // 16
        block = lax.broadcasted_iota(jnp.int32, (16, LANES), 1) // grid.nz
        for side in BOTH:
            made = []
            for end, i in zip(ends, (grid.fold - 1, 0)):
                here = i * grid.ny + (last_y if side == 0 else 0)
                out = None
                for j in range(groups):
                    piece = roll(end[16 * j : 16 * j + 16], grid.nz * (j - here))
                    out = piece if out is None else jnp.where(block == j, piece, out)
                made.append(out)
            self.ds[side] = jnp.where(block * 0 + self.gx == 0, *made)

        def one(q, carry):
            held = [None, None]
            rows = [None, None]
            for k in range(grid.group):
                tile = field[:, lanes_at(q * grid.group + k)]
                j = k % grid.ny
                for side in BOTH:
                    piece = roll(tile, k - last_z if side == 0 else k)
                    held[side] = piece if k == 0 else jnp.where(z == k, piece, held[side])
                    piece = roll(tile, grid.nz * (j - last_y if side == 0 else j))
                    rows[side] = piece if j == 0 else jnp.where(y == j, piece, rows[side])
                    if j == last_y:
                        self.ys[side, :, lanes_at(q * (grid.group // grid.ny) + k // grid.ny)] = rows[side]
            for side in BOTH:
                self.zs[side, :, lanes_at(q)] = held[side]
            return carry

        loops = grid.tiles // grid.group
        if loops == 1:
            one(0, 0)
        else:
            lax.fori_loop(0, loops, one, 0)
        groups, packs = grid.corner_groups(c), grid.ypacks
        part = c // groups
        z = grid.at(part)[2]
        for sy in BOTH:
            for sz in BOTH:
                out = None
                for j in range(groups):
                    for p in range(packs):
                        to = packs * j + p
                        piece = self.ys[sy, j * part : (j + 1) * part, lanes_at(p)]
                        piece = roll(piece, to - (last_z if sz == 0 else 0))
                        out = piece if out is None else jnp.where(z == to, piece, out)
                self.cs[sy * 2 + sz] = out

    def start(self):
        for copy, goes, _ in self.moves:
            pl.when(goes)(copy.start)

    def wait(self):
        for copy, goes, comes in self.moves:
            pl.when(goes)(copy.wait_send)
            pl.when(comes)(copy.wait_recv)

    def shift_z(self, tile, low, high, dz, z):
        if dz == 0:
            return tile
        if dz < 0:
            return jnp.where(z == 0, low, roll(tile, 1))
        return jnp.where(z == self.grid.nz - 1, high, roll(tile, -1))

    def shift_y(self, tile, low, high, dy, y):
        if dy == 0:
            return tile
        if dy < 0:
            return jnp.where(y == 0, low, roll(tile, self.grid.nz))
        return jnp.where(y == self.grid.ny - 1, high, roll(tile, -self.grid.nz))

    def beyond(self):
        grid, c = self.grid, self.channels
        _, y, z = grid.at(c)
        last = grid.fold - 1
        if grid.fold == 1:
            came = [self.xr[i] for i in range(3)]
        else:
            came = [
                jnp.concatenate([roll(self.xr[i], grid.plane * (last - j)) for j in range(grid.fold)], axis=0)
                for i in range(3)
            ]
        over = []
        for side in BOTH:
            to = last * grid.ny + (0 if side == 0 else grid.ny - 1)
            over.append(
                [
                    jnp.concatenate(
                        [roll(self.dr[side, i], grid.nz * (to - j)) for j in range(c // 16)], axis=0
                    )
                    for i in range(3)
                ]
            )
        rows = []
        for low, here, high in (over[0], came, over[1]):
            low, high = roll(low, 1 - grid.nz), roll(high, grid.nz - 1)
            rows.append([self.shift_z(here, low, high, dz, z) for dz in NEAR])
        return [
            self.shift_y(rows[1][dz], rows[0][dz], rows[2][dz], dy, y) for dy in NEAR for dz in range(3)
        ]

    def strips(self, shifted):
        grid, c = self.grid, self.channels
        groups, packs = grid.corner_groups(c), grid.ypacks
        _, _, z = grid.at(c)
        for side in BOTH:
            for p in range(packs):
                tile = self.yr[side, :, lanes_at(p)]
                ends = []
                for sz in BOTH:
                    to = 0 if sz == 0 else grid.nz - 1
                    corner = self.cr[side * 2 + sz]
                    ends.append(
                        jnp.concatenate([roll(corner, to - packs * j - p) for j in range(groups)], axis=0)
                    )
                for dz in NEAR:
                    shifted[side * 3 + dz + 1, :, lanes_at(p)] = self.shift_z(tile, *ends, dz, z)

    def tile_shifts(self, field, shifted, q, k):
        grid, c = self.grid, self.channels
        _, y, z = grid.at(c)
        last_z, last_y = grid.nz - 1, grid.ny - 1
        tile = field[:, lanes_at(q * grid.group + k)]
        low = roll(self.zr[0, :, lanes_at(q)], -k)
        high = roll(self.zr[1, :, lanes_at(q)], last_z - k)
        moved = [self.shift_z(tile, low, high, dz, z) for dz in NEAR]
        p, j = q * (grid.group // grid.ny) + k // grid.ny, k % grid.ny
        out = []
        for dy in NEAR:
            for dz in range(3):
                low = high = None
                if dy < 0:
                    low = roll(shifted[dz, :, lanes_at(p)], -grid.nz * j)
                if dy > 0:
                    high = roll(shifted[3 + dz, :, lanes_at(p)], grid.nz * (last_y - j))
                out.append(self.shift_y(moved[dz], low, high, dy, y))
        return out

    def only(self, value, side):
        flag = lax.broadcasted_iota(jnp.int32, value.shape, 1) * 0 + self.gx
        return jnp.where(flag == side, value, jnp.zeros_like(value))

    def fine_windows(self, field, shifted, windows):
        grid, c = self.grid, self.channels
        self.strips(shifted)
        for i, value in enumerate(self.beyond()):
            windows[i * c : (i + 1) * c, lanes_at(0)] = self.only(value, 1)
            windows[i * c : (i + 1) * c, lanes_at(grid.tiles + 1)] = self.only(value, 0)

        def one(q, carry):
            for k in range(grid.group):
                for i, value in enumerate(self.tile_shifts(field, shifted, q, k)):
                    windows[i * c : (i + 1) * c, lanes_at(q * grid.group + k + 1)] = value
            return carry

        lax.fori_loop(0, grid.tiles // grid.group, one, 0)

    def coarse_windows(self, field, shifted, windows):
        grid, c = self.grid, self.channels
        spot = grid.at(c)[0]
        self.strips(shifted)
        outer = self.beyond()
        tiles = [self.tile_shifts(field, shifted, 0, k) for k in range(grid.tiles)]
        for i in range(9):
            low = roll(self.only(outer[i], 1), grid.plane)
            high = self.only(outer[i], 0)
            rows = [slice((dx * 9 + i) * c, (dx * 9 + i + 1) * c) for dx in range(3)]
            up = [roll(tile[i], grid.plane) for tile in tiles]
            down = [roll(tile[i], -grid.plane) for tile in tiles]
            for t in range(grid.tiles):
                before = up[t - 1] if t else low
                after = down[t + 1] if t + 1 < grid.tiles else high
                windows[rows[0], lanes_at(t)] = jnp.where(spot == 0, before, up[t])
                windows[rows[1], lanes_at(t)] = tiles[t][i]
                windows[rows[2], lanes_at(t)] = jnp.where(spot == grid.fold - 1, after, down[t])


class Summing:
    def __init__(self, acc, stage, first, mine, second, whole, sems):
        self.acc, self.stage, self.first = acc, stage, first
        self.mine, self.second, self.whole = mine, second, whole
        self.sems = sems
        gy = lax.axis_size("gy")
        self.count = lax.axis_size("gx") * gy
        self.depth = lax.axis_size("gz")
        self.me = lax.axis_index("gx") * gy + lax.axis_index("gy")
        self.level = lax.axis_index("gz")

    def across(self, phase, k, source, target):
        gy = lax.axis_size("gy")
        to = (self.me + k) % self.count
        return pltpu.make_async_remote_copy(
            src_ref=source(to),
            dst_ref=target,
            send_sem=self.sems.at[phase, 0, k],
            recv_sem=self.sems.at[phase, 1, k],
            device_id={"gx": to // gy, "gy": to % gy},
            device_id_type=MESH,
        )

    def along(self, k):
        return pltpu.make_async_remote_copy(
            src_ref=self.mine,
            dst_ref=self.second.at[self.level],
            send_sem=self.sems.at[1, 0, k],
            recv_sem=self.sems.at[1, 1, k],
            device_id={"gz": (self.level + k) % self.depth},
            device_id_type=MESH,
        )

    def scatters(self):
        return [
            self.across(0, k, lambda to: self.stage.at[to], self.first.at[self.me])
            for k in range(1, self.count)
        ]

    def alongs(self):
        return [self.along(k) for k in range(1, self.depth)]

    def gathers(self):
        here = self.whole.at[self.me]
        return [self.across(2, k, lambda to: here, here) for k in range(1, self.count)]

    def start(self):
        chunk = self.stage.shape[1]
        for i in range(self.count):
            self.stage[i] = self.acc[i * chunk : (i + 1) * chunk].astype(jnp.bfloat16)
        for copy in self.scatters():
            copy.start()
        self.first[self.me] = self.stage[self.me]

    def total(self, parts):
        total = parts[0].astype(jnp.float32)
        for i in range(1, parts.shape[0]):
            total = total + parts[i].astype(jnp.float32)
        return total.astype(jnp.bfloat16)

    def middle(self):
        for copy in self.scatters():
            copy.wait()
        part = self.total(self.first)
        self.mine[...] = part
        for copy in self.alongs():
            copy.start()
        self.second[self.level] = part

    def last(self):
        for copy in self.alongs():
            copy.wait()
        self.whole[self.me] = self.total(self.second)
        for copy in self.gathers():
            copy.start()

    def finish(self):
        for copy in self.gathers():
            copy.wait()


class Slabs:
    def __init__(self, sent, came, sems, grid):
        self.sent, self.came, self.sems, self.grid = sent, came, sems, grid
        self.depth, self.level = lax.axis_size("gz"), lax.axis_index("gz")

    def copies(self):
        out = []
        for k in range(1, self.depth):
            to = (self.level + k) % self.depth
            out.append(
                pltpu.make_async_remote_copy(
                    src_ref=self.sent.at[to],
                    dst_ref=self.came.at[self.level],
                    send_sem=self.sems.at[0, k],
                    recv_sem=self.sems.at[1, k],
                    device_id={"gz": to},
                    device_id_type=MESH,
                )
            )
        return out

    def pack(self, field):
        fold, plane = self.grid.fold, self.grid.plane
        part = self.sent.shape[1]
        spot = self.grid.at(part)[0]
        for t in range(self.grid.tiles):
            for i in range(fold):
                out = None
                for j in range(fold):
                    piece = roll(field[j * part : (j + 1) * part, lanes_at(t)], plane * (j - i))
                    out = piece if out is None else jnp.where(spot == j, piece, out)
                self.sent[t * fold + i] = out
        for copy in self.copies():
            copy.start()
        self.came[self.level] = self.sent[self.level]

    def unpack(self, field):
        for copy in self.copies():
            copy.wait()
        fold, plane = self.grid.fold, self.grid.plane
        part = self.came.shape[1]
        spot = self.grid.at(part)[0]
        for t in range(self.grid.tiles):
            for j in range(fold):
                out = None
                for i in range(fold):
                    piece = roll(self.came[t * fold + i], plane * (i - j))
                    out = piece if out is None else jnp.where(spot == i, piece, out)
                field[j * part : (j + 1) * part, lanes_at(t)] = out


def greet():
    gx, gy, gz = [lax.axis_size(axis) for axis in ("gx", "gy", "gz")]
    me = lax.axis_index("gx") * gy + lax.axis_index("gy")
    level, row, half = lax.axis_index("gz"), lax.axis_index("gy"), lax.axis_index("gx")
    barrier = pltpu.get_barrier_semaphore()
    signal = lambda device: pl.semaphore_signal(barrier, inc=1, device_id=device, device_id_type=MESH)
    for k in range(1, gx * gy):
        to = (me + k) % (gx * gy)
        signal({"gx": to // gy, "gy": to % gy})
    for k in range(1, gz):
        signal({"gz": (level + k) % gz})
    extra = 0
    for across in BOTH:
        for dy in NEAR:
            for dz in NEAR:
                if dz and (across or dy):
                    extra += 1
                    signal(
                        {
                            "gx": (half + across) % gx,
                            "gy": (row + dy + gy) % gy,
                            "gz": (level + dz + gz) % gz,
                        }
                    )
    return barrier, gx * gy + gz - 2 + extra


def spread_map(fine, coarse):
    shape = (LANES, coarse.fold * LANES)
    small = lax.broadcasted_iota(jnp.int32, shape, 0)
    large = lax.broadcasted_iota(jnp.int32, shape, 1)
    y, z = large % LANES // fine.nz, large % fine.nz
    match = (
        (small // coarse.plane == large // LANES)
        & (small // coarse.nz % coarse.ny == y // 2)
        & (small % coarse.nz == z // 2)
    )
    ones = match.astype(jnp.float32)
    first = (match & (y % 2 == 0) & (z % 2 == 0)).astype(jnp.float32)
    return ones.astype(jnp.bfloat16), first.astype(jnp.bfloat16)


def order_map(coarse, count):
    shape = (coarse.plane * count,) * 2
    row = lax.broadcasted_iota(jnp.int32, shape, 0)
    column = lax.broadcasted_iota(jnp.int32, shape, 1)
    wide = count * coarse.nz
    match = (
        (row // wide == column // coarse.nz % coarse.ny)
        & (row % wide // coarse.nz == column // coarse.plane)
        & (row % coarse.nz == column % coarse.nz)
    )
    return match.astype(jnp.float32).astype(jnp.bfloat16)


def column_of(row):
    size = row.shape[1]
    across = lax.broadcasted_iota(jnp.int32, (size, size), 0)
    down = lax.broadcasted_iota(jnp.int32, (size, size), 1)
    return jnp.sum(jnp.where(across == down, row, 0.0), axis=1, keepdims=True)


def whole_kernel(setting, *refs):
    names, local = setting[3:]
    pl.run_scoped(lambda **held: stages(setting, dict(zip(names, refs)) | held), **local)


def stages(setting, named):
    fine_size, coarse_size, scales = setting[:3]
    fine, coarse = Grid(*fine_size), Grid(*coarse_size)
    r = lambda name: named[name]
    fields = ("a", "b", "gb", "ga")
    grids = (fine, coarse, coarse, fine)
    volume, w_a, b_a, w_b, b_b, cot = [r(n) for n in ("volume", "w_a", "b_a", "w_b", "b_b", "cot")]
    features, grad_in, out_wa, out_ba, out_wb, out_bb = [
        r(n) for n in ("features", "grad_in", "out_wa", "out_ba", "out_wb", "out_bb")
    ]
    c1, c2, c3 = volume.shape[0], w_a.shape[1], w_b.shape[1]
    widths = dict(zip(fields, (c1, c2, c3, c2)))
    halos = {
        name: Exchange(
            grid,
            widths[name],
            [r(name + part) for part in ("_zs", "_zr", "_ys", "_yr", "_cs", "_cr", "_xs", "_xr", "_ds", "_dr")],
            r("halo_sems"),
            i,
        )
        for i, (name, grid) in enumerate(zip(fields, grids))
    }
    strips = {name: r(name + "_strips") for name in fields}
    win_a, win_b, win_gb, win_ga = [r(name + "_win") for name in fields]
    before_a, pooled, grad_b, grad_a = [r(n) for n in ("before_a", "pooled", "grad_b", "grad_a")]
    acc_a, acc_b, mixed, feat = [r(n) for n in ("acc_a", "acc_b", "mixed", "feat")]
    sum_a = Summing(acc_a, *[r(f"sum_a{i}") for i in range(5)], r("sum_sems").at[0])
    sum_b = Summing(acc_b, *[r(f"sum_b{i}") for i in range(5)], r("sum_sems").at[1])
    cots = Slabs(r("cot_sent"), r("cot_came"), r("slab_sems").at[0], coarse)
    feats = Slabs(r("feat_sent"), r("feat_came"), r("slab_sems").at[1], coarse)
    out_a, in_a, out_b, in_b, spread, thin, order = [
        r(n) for n in ("to_a", "from_a", "to_b", "from_b", "spread", "thin", "order")
    ]
    field = r("field")
    bf16 = jnp.bfloat16

    for name in fields:
        halos[name].clear()
    barrier, arrivals = greet()
    field[...] = volume[...]
    halos["a"].pack(field)
    order[...] = order_map(coarse, lax.axis_size("gz"))
    mixed[...] = dot(cot[...], order[...]).astype(bf16)
    pl.semaphore_wait(barrier, arrivals)
    halos["a"].start()
    cots.pack(mixed)

    taps = 9
    for dx in range(3):
        out_a[dx] = w_a[dx * taps * c1 : (dx + 1) * taps * c1].T
        for k in range(taps):
            tap = 26 - dx * taps - k
            in_a[dx, :, k * c2 : (k + 1) * c2] = w_a[tap * c1 : (tap + 1) * c1]
    out_b[...] = w_b[...].T
    for k in range(27):
        in_b[:, k * c3 : (k + 1) * c3] = w_b[(26 - k) * c2 : (27 - k) * c2]
    wide, narrow = spread_map(fine, coarse)
    spread[...] = wide
    thin[...] = narrow
    bias_a, bias_b = column_of(b_a[...]), column_of(b_b[...])
    acc_a[...] = jnp.zeros_like(acc_a)
    acc_b[...] = jnp.zeros_like(acc_b)

    halos["a"].wait()
    halos["a"].fine_windows(field, strips["a"], win_a)
    many = 2 * coarse.fold

    def forward_a(g, carry):
        before = bias_a
        for dx in range(3):
            before = before + dot(out_a[dx], win_a[:, lanes_at(g * many + dx, many)])
        before_a[:, lanes_at(g * many, many)] = before
        active = before * jax.nn.sigmoid(before)
        pieces = []
        for i in range(coarse.fold):
            first = active[:, 2 * i * LANES : (2 * i + 1) * LANES]
            pair = first + active[:, (2 * i + 1) * LANES : (2 * i + 2) * LANES]
            pair = pair + roll(pair, -1)
            pair = pair + roll(pair, -fine.nz)
            pieces.append((pair * 0.125).astype(bf16))
        pooled[:, lanes_at(g)] = dot_rows(jnp.concatenate(pieces, axis=1), thin[...]).astype(bf16)
        return carry

    lax.fori_loop(0, coarse.tiles, forward_a, 0)
    halos["b"].pack(pooled)
    halos["b"].start()
    cots.unpack(mixed)
    halos["b"].wait()
    halos["b"].coarse_windows(pooled, strips["b"], win_b)
    before = dot(out_b[...], win_b[...]) + bias_b
    grad_b[...] = (mixed[...].astype(jnp.float32) * slope_of(before)).astype(bf16)
    halos["gb"].pack(grad_b)
    halos["gb"].start()
    feat[...] = (before * jax.nn.sigmoid(before)).astype(bf16)
    feats.pack(feat)
    top_b = out_wb.shape[0]
    grad = grad_b[...]
    acc_b[:top_b] = dot_rows(win_b[...], grad)
    acc_b[top_b : top_b + 8] = dot_rows(jnp.ones((8, grad.shape[1]), bf16), grad)
    sum_b.start()
    halos["gb"].wait()
    halos["gb"].coarse_windows(grad_b, strips["gb"], win_gb)
    pooled[...] = dot(in_b[...], win_gb[...]).astype(bf16)

    def backward_b(g, carry):
        wide = dot(pooled[:, lanes_at(g)], spread[...]) * 0.125
        for i in range(coarse.fold):
            for j in BOTH:
                here = lanes_at(g * many + 2 * i + j)
                slope = slope_of(before_a[:, here])
                grad_a[:, here] = (wide[:, i * LANES : (i + 1) * LANES] * slope).astype(bf16)
        return carry

    lax.fori_loop(0, coarse.tiles, backward_b, 0)
    halos["ga"].pack(grad_a)
    halos["ga"].start()
    grad = grad_a[...]
    half, width = out_wa.shape[0] // 2, out_wa.shape[1]
    parts = [dot_rows(win_a[:, lanes_at(dx, fine.tiles)], grad) for dx in range(3)]
    whole = jnp.concatenate(parts, axis=0)
    acc_a[:half, :width] = whole[:half]
    acc_a[:half, width:] = whole[half:]
    acc_a[half : half + 8, :width] = dot_rows(jnp.ones((8, grad.shape[1]), bf16), grad)
    sum_a.start()
    sum_b.middle()
    halos["ga"].wait()
    halos["ga"].fine_windows(grad_a, strips["ga"], win_ga)
    sum_a.middle()

    def backward_a(g, carry):
        total = dot(in_a[0], win_ga[:, lanes_at(g * many, many)])
        for dx in (1, 2):
            total = total + dot(in_a[dx], win_ga[:, lanes_at(g * many + dx, many)])
        grad_in[:, lanes_at(g * many, many)] = total.astype(bf16)
        return carry

    lax.fori_loop(0, coarse.tiles, backward_a, 0)
    sum_b.last()
    feats.unpack(feat)
    features[...] = dot_rows(feat[...], order[...]).astype(bf16)
    sum_a.last()
    sum_b.finish()
    all_a, all_b = r("sum_a4"), r("sum_b4")
    scale_a, scale_b = scales
    flat_b = all_b[...].astype(jnp.float32).reshape(-1, all_b.shape[2]) * scale_b
    out_wb[...] = flat_b[:top_b]
    out_bb[...] = flat_b[top_b : top_b + 1]
    sum_a.finish()
    flat_a = all_a[...].astype(jnp.float32).reshape(-1, all_a.shape[2]) * scale_a
    out_wa[:half] = flat_a[:half, :width]
    out_wa[half:] = flat_a[:half, width:]
    out_ba[...] = flat_a[half : half + 1, :width]


def on_device(volume, weight_a, bias_a, weight_b, bias_b, cotangent):
    f32, bf16 = jnp.float32, jnp.bfloat16
    members, levels = lax.axis_size("gx") * lax.axis_size("gy"), lax.axis_size("gz")
    c1, nx, ny, nz = volume.shape
    c2, c3 = weight_b.shape[3:]
    cells = nx * ny * nz
    fewer = cells // 8
    scale_a = 1.0 / math.sqrt(cells * members * levels)
    scale_b = 1.0 / math.sqrt(cells * members * levels // 8)
    fine_size, coarse_size = (nx, ny, nz), (nx // 2, ny // 2, nz // 2)
    fine, coarse = Grid(*fine_size), Grid(*coarse_size)
    rows_a = 27 * c1 // 2 + 16
    rows_a += -rows_a % (16 * members)
    rows_b = 27 * c2 + 16
    rows_b += -rows_b % (16 * members)
    operands = {
        "volume": volume.reshape(c1, cells),
        "w_a": weight_a.reshape(27 * c1, c2),
        "b_a": bias_a.reshape(1, c2),
        "w_b": weight_b.reshape(27 * c2, c3),
        "b_b": bias_b.reshape(1, c3),
        "cot": cotangent.reshape(c3, fewer),
    }
    outs = {
        "features": ((c3, fewer), bf16),
        "grad_in": ((c1, cells), bf16),
        "out_wa": ((27 * c1, c2), f32),
        "out_ba": ((1, c2), f32),
        "out_wb": ((27 * c2, c3), f32),
        "out_bb": ((1, c3), f32),
    }
    scratch, local = {}, {}
    for name, grid, c in (("a", fine, c1), ("b", coarse, c2), ("gb", coarse, c3), ("ga", fine, c2)):
        for end in ("s", "r"):
            scratch[f"{name}_z{end}"] = pltpu.VMEM((2, c, grid.zpacks * LANES), bf16)
            scratch[f"{name}_y{end}"] = pltpu.VMEM((2, c, grid.ypacks * LANES), bf16)
            scratch[f"{name}_c{end}"] = pltpu.VMEM((4, c // grid.corner_groups(c), LANES), bf16)
        scratch[f"{name}_xs"] = pltpu.VMEM((c // grid.fold, LANES), bf16)
        scratch[f"{name}_xr"] = pltpu.VMEM((3, c // grid.fold, LANES), bf16)
        scratch[f"{name}_ds"] = pltpu.VMEM((2, 16, LANES), bf16)
        scratch[f"{name}_dr"] = pltpu.VMEM((2, 3, 16, LANES), bf16)
        local[f"{name}_strips"] = pltpu.VMEM((6, c, grid.ypacks * LANES), bf16)
        shape = (9 * c, (grid.tiles + 2) * LANES) if grid is fine else (27 * c, grid.tiles * LANES)
        local[f"{name}_win"] = pltpu.VMEM(shape, bf16)
    local["field"] = pltpu.VMEM((c1, cells), bf16)
    local["before_a"] = pltpu.VMEM((c2, cells), f32)
    local["pooled"] = pltpu.VMEM((c2, fewer), bf16)
    local["grad_b"] = pltpu.VMEM((c3, fewer), bf16)
    local["grad_a"] = pltpu.VMEM((c2, cells), bf16)
    local["mixed"] = pltpu.VMEM((c3, fewer), bf16)
    local["feat"] = pltpu.VMEM((c3, fewer), bf16)
    for name, rows in (("a", rows_a), ("b", rows_b)):
        chunk = rows // members
        scratch[f"acc_{name}"] = pltpu.VMEM((rows, LANES), f32)
        for i, shape in enumerate(
            ((members, chunk), (members, chunk), (chunk,), (levels, chunk), (members, chunk))
        ):
            scratch[f"sum_{name}{i}"] = pltpu.VMEM((*shape, LANES), bf16)
    for name in ("cot_sent", "cot_came", "feat_sent", "feat_came"):
        scratch[name] = pltpu.VMEM((levels, c3 // coarse.fold, LANES), bf16)
    local["to_a"] = pltpu.VMEM((3, c2, 9 * c1), bf16)
    local["from_a"] = pltpu.VMEM((3, c1, 9 * c2), bf16)
    local["to_b"] = pltpu.VMEM((c3, 27 * c2), bf16)
    local["from_b"] = pltpu.VMEM((c2, 27 * c3), bf16)
    local["spread"] = pltpu.VMEM((LANES, coarse.fold * LANES), bf16)
    local["thin"] = pltpu.VMEM((LANES, coarse.fold * LANES), bf16)
    local["order"] = pltpu.VMEM((fewer, fewer), bf16)
    scratch["halo_sems"] = pltpu.SemaphoreType.DMA((2, 4, 17))
    scratch["sum_sems"] = pltpu.SemaphoreType.DMA((2, 3, 2, max(members, levels)))
    scratch["slab_sems"] = pltpu.SemaphoreType.DMA((2, 2, levels))
    names = (*operands, *outs, *scratch)
    got = pl.pallas_call(
        functools.partial(whole_kernel, (fine_size, coarse_size, (scale_a, scale_b), names, local)),
        out_shape=[jax.ShapeDtypeStruct(shape, dtype) for shape, dtype in outs.values()],
        in_specs=[pl.BlockSpec(memory_space=pltpu.VMEM)] * len(operands),
        out_specs=[pl.BlockSpec(memory_space=pltpu.VMEM)] * len(outs),
        scratch_shapes=list(scratch.values()),
        compiler_params=pltpu.CompilerParams(
            collective_id=1, has_side_effects=True, vmem_limit_bytes=60 * 2**20
        ),
    )(*operands.values())
    features, grad_in, sum_wa, sum_ba, sum_wb, sum_bb = got
    return (
        features.reshape(cotangent.shape),
        grad_in.reshape(volume.shape),
        sum_wa.reshape(weight_a.shape),
        sum_ba.reshape(c2),
        sum_wb.reshape(weight_b.shape),
        sum_bb.reshape(c3),
    )


def solution(mesh):
    return jax.shard_map(
        on_device,
        mesh=mesh,
        in_specs=(P(None, "gx", "gy", "gz"), P(), P(), P(), P(), P(None, ("gx", "gz"), "gy", None)),
        out_specs=(
            P(None, ("gx", "gz"), "gy", None),
            P(None, "gx", "gy", "gz"),
            P(),
            P(),
            P(),
            P(),
        ),
        check_vma=False,
    )
```

```python
import functools
import math

import jax
import jax.numpy as jnp
from jax import lax
from jax.experimental import pallas as pl
from jax.experimental.pallas import tpu as pltpu
from jax.sharding import PartitionSpec as P

MESH = pl.DeviceIdType.MESH
LANES = 128
PITCH = 40
BOTH = (0, 1)
NEAR = (-1, 0, 1)


def slope_of(value):
    sigma = jax.nn.sigmoid(value)
    return sigma + value * sigma * (1.0 - sigma)


def dot(left, right):
    return jnp.dot(left, right, preferred_element_type=jnp.float32)


def dot_rows(left, right):
    return lax.dot_general(
        left, right, (((1,), (1,)), ((), ())), preferred_element_type=jnp.float32
    )


def roll(value, by):
    by = by % LANES
    return pltpu.roll(value, by, 1) if by else value


def lanes_at(index, count=1):
    begin = index * LANES
    if not isinstance(begin, int):
        begin = pl.multiple_of(begin, LANES)
    return pl.ds(begin, count * LANES)


def within(at, count):
    return (at >= 0) & (at < count)


class Grid:
    def __init__(self, nx, ny, nz):
        self.ny, self.nz = ny, nz
        self.plane = ny * nz
        self.fold = LANES // self.plane
        self.tiles = nx // self.fold
        self.zpacks = -(-self.tiles // nz)
        self.ypacks = -(-self.tiles // ny)
        self.group = max(ny, min(nz, self.tiles))

    def at(self, rows):
        lane = lax.broadcasted_iota(jnp.int32, (rows, LANES), 1)
        return lane // self.plane, lane // self.nz % self.ny, lane % self.nz

    def corner_groups(self, channels):
        return min(channels // 16, self.nz // self.ypacks)


class Exchange:
    def __init__(self, grid, channels, buffers, sems, at):
        self.grid, self.channels = grid, channels
        self.zs, self.zr, self.ys, self.yr, self.cs, self.cr, self.xs, self.xr, self.ds, self.dr = buffers
        self.gx, self.gy, self.gz = [lax.axis_index(axis) for axis in ("gx", "gy", "gz")]
        cuts_y, cuts_z = lax.axis_size("gy"), lax.axis_size("gz")
        moves = []
        step = (1, -1)
        for side in BOTH:
            moves.append((self.ys.at[side], self.yr.at[side], 0, step[side], 0))
        for dy in NEAR:
            for dz in NEAR:
                source = self.ds.at[(1 - dy) // 2] if dy else self.xs
                target = self.dr.at[(1 - dy) // 2, 1 - dz] if dy else self.xr.at[1 - dz]
                moves.append((source, target, 1, dy, dz))
        for side in BOTH:
            moves.append((self.zs.at[side], self.zr.at[side], 0, 0, step[side]))
        for sy in BOTH:
            for sz in BOTH:
                i = sy * 2 + sz
                moves.append((self.cs.at[i], self.cr.at[i], 0, step[sy], step[sz]))
        self.moves = []
        for i, (source, target, across, dy, dz) in enumerate(moves):
            copy = pltpu.make_async_remote_copy(
                src_ref=source,
                dst_ref=target,
                send_sem=sems.at[0, at, i],
                recv_sem=sems.at[1, at, i],
                device_id={
                    "gx": (self.gx + across) % 2,
                    "gy": (self.gy + dy + cuts_y) % cuts_y,
                    "gz": (self.gz + dz + cuts_z) % cuts_z,
                },
                device_id_type=MESH,
            )
            goes = within(self.gy + dy, cuts_y) & within(self.gz + dz, cuts_z)
            comes = within(self.gy - dy, cuts_y) & within(self.gz - dz, cuts_z)
            self.moves.append((copy, goes, comes))

    def clear(self):
        for ref in (self.zr, self.yr, self.cr, self.xr, self.dr):
            ref[...] = jnp.zeros_like(ref)

    def pack(self, field):
        grid, c = self.grid, self.channels
        spot, y, z = grid.at(c)
        last_z, last_y = grid.nz - 1, grid.ny - 1
        ends = [field[:, lanes_at(t)] for t in (grid.tiles - 1, 0)]
        if grid.fold == 1:
            self.xs[...] = jnp.where(spot + self.gx == 0, *ends)
        else:
            part = c // grid.fold
            place = grid.at(part)[0]
            made = []
            for end, i in zip(ends, (grid.fold - 1, 0)):
                out = end[:part]
                out = roll(out, grid.plane * -i)
                for j in range(1, grid.fold):
                    piece = roll(end[j * part : (j + 1) * part], grid.plane * (j - i))
                    out = jnp.where(place == j, piece, out)
                made.append(out)
            self.xs[...] = jnp.where(place * 0 + self.gx == 0, *made)

        groups = c // 16
        block = lax.broadcasted_iota(jnp.int32, (16, LANES), 1) // grid.nz
        for side in BOTH:
            made = []
            for end, i in zip(ends, (grid.fold - 1, 0)):
                here = i * grid.ny + (last_y if side == 0 else 0)
                out = None
                for j in range(groups):
                    piece = roll(end[16 * j : 16 * j + 16], grid.nz * (j - here))
                    out = piece if out is None else jnp.where(block == j, piece, out)
                made.append(out)
            self.ds[side] = jnp.where(block * 0 + self.gx == 0, *made)

        def one(q, carry):
            held = [None, None]
            rows = [None, None]
            for k in range(grid.group):
                tile = field[:, lanes_at(q * grid.group + k)]
                j = k % grid.ny
                for side in BOTH:
                    piece = roll(tile, k - last_z if side == 0 else k)
                    held[side] = piece if k == 0 else jnp.where(z == k, piece, held[side])
                    piece = roll(tile, grid.nz * (j - last_y if side == 0 else j))
                    rows[side] = piece if j == 0 else jnp.where(y == j, piece, rows[side])
                    if j == last_y:
                        self.ys[side, :, lanes_at(q * (grid.group // grid.ny) + k // grid.ny)] = rows[side]
            for side in BOTH:
                self.zs[side, :, lanes_at(q)] = held[side]
            return carry

        loops = grid.tiles // grid.group
        if loops == 1:
            one(0, 0)
        else:
            lax.fori_loop(0, loops, one, 0)
        groups, packs = grid.corner_groups(c), grid.ypacks
        part = c // groups
        z = grid.at(part)[2]
        for sy in BOTH:
            for sz in BOTH:
                out = None
                for j in range(groups):
                    for p in range(packs):
                        to = packs * j + p
                        piece = self.ys[sy, j * part : (j + 1) * part, lanes_at(p)]
                        piece = roll(piece, to - (last_z if sz == 0 else 0))
                        out = piece if out is None else jnp.where(z == to, piece, out)
                self.cs[sy * 2 + sz] = out

    def start(self):
        for copy, goes, _ in self.moves:
            pl.when(goes)(copy.start)

    def wait(self):
        for copy, goes, comes in self.moves:
            pl.when(goes)(copy.wait_send)
            pl.when(comes)(copy.wait_recv)

    def shift_z(self, tile, low, high, dz, z):
        if dz == 0:
            return tile
        if dz < 0:
            return jnp.where(z == 0, low, roll(tile, 1))
        return jnp.where(z == self.grid.nz - 1, high, roll(tile, -1))

    def shift_y(self, tile, low, high, dy, y):
        if dy == 0:
            return tile
        if dy < 0:
            return jnp.where(y == 0, low, roll(tile, self.grid.nz))
        return jnp.where(y == self.grid.ny - 1, high, roll(tile, -self.grid.nz))

    def beyond(self):
        grid, c = self.grid, self.channels
        _, y, z = grid.at(c)
        last = grid.fold - 1
        if grid.fold == 1:
            came = [self.xr[i] for i in range(3)]
        else:
            came = [
                jnp.concatenate([roll(self.xr[i], grid.plane * (last - j)) for j in range(grid.fold)], axis=0)
                for i in range(3)
            ]
        over = []
        for side in BOTH:
            to = last * grid.ny + (0 if side == 0 else grid.ny - 1)
            over.append(
                [
                    jnp.concatenate(
                        [roll(self.dr[side, i], grid.nz * (to - j)) for j in range(c // 16)], axis=0
                    )
                    for i in range(3)
                ]
            )
        rows = []
        for low, here, high in (over[0], came, over[1]):
            low, high = roll(low, 1 - grid.nz), roll(high, grid.nz - 1)
            rows.append([self.shift_z(here, low, high, dz, z) for dz in NEAR])
        return [
            self.shift_y(rows[1][dz], rows[0][dz], rows[2][dz], dy, y) for dy in NEAR for dz in range(3)
        ]

    def strips(self, shifted):
        grid, c = self.grid, self.channels
        groups, packs = grid.corner_groups(c), grid.ypacks
        _, _, z = grid.at(c)
        for side in BOTH:
            for p in range(packs):
                tile = self.yr[side, :, lanes_at(p)]
                ends = []
                for sz in BOTH:
                    to = 0 if sz == 0 else grid.nz - 1
                    corner = self.cr[side * 2 + sz]
                    ends.append(
                        jnp.concatenate([roll(corner, to - packs * j - p) for j in range(groups)], axis=0)
                    )
                for dz in NEAR:
                    shifted[side * 3 + dz + 1, :, lanes_at(p)] = self.shift_z(tile, *ends, dz, z)

    def tile_shifts(self, field, shifted, q, k):
        grid, c = self.grid, self.channels
        _, y, z = grid.at(c)
        last_z, last_y = grid.nz - 1, grid.ny - 1
        tile = field[:, lanes_at(q * grid.group + k)]
        low = roll(self.zr[0, :, lanes_at(q)], -k)
        high = roll(self.zr[1, :, lanes_at(q)], last_z - k)
        moved = [self.shift_z(tile, low, high, dz, z) for dz in NEAR]
        p, j = q * (grid.group // grid.ny) + k // grid.ny, k % grid.ny
        out = []
        for dy in NEAR:
            for dz in range(3):
                low = high = None
                if dy < 0:
                    low = roll(shifted[dz, :, lanes_at(p)], -grid.nz * j)
                if dy > 0:
                    high = roll(shifted[3 + dz, :, lanes_at(p)], grid.nz * (last_y - j))
                out.append(self.shift_y(moved[dz], low, high, dy, y))
        return out

    def only(self, value, side):
        flag = lax.broadcasted_iota(jnp.int32, value.shape, 1) * 0 + self.gx
        return jnp.where(flag == side, value, jnp.zeros_like(value))

    def fine_windows(self, field, shifted, windows):
        grid, c = self.grid, self.channels
        self.strips(shifted)
        for i, value in enumerate(self.beyond()):
            windows[i * c : (i + 1) * c, lanes_at(0)] = self.only(value, 1)
            windows[i * c : (i + 1) * c, lanes_at(grid.tiles + 1)] = self.only(value, 0)

        def one(q, carry):
            for k in range(grid.group):
                for i, value in enumerate(self.tile_shifts(field, shifted, q, k)):
                    windows[i * c : (i + 1) * c, lanes_at(q * grid.group + k + 1)] = value
            return carry

        lax.fori_loop(0, grid.tiles // grid.group, one, 0)

    def coarse_windows(self, field, shifted, windows):
        grid, c = self.grid, self.channels
        spot = grid.at(c)[0]
        self.strips(shifted)
        outer = self.beyond()
        tiles = [self.tile_shifts(field, shifted, 0, k) for k in range(grid.tiles)]
        for i in range(9):
            low = roll(self.only(outer[i], 1), grid.plane)
            high = self.only(outer[i], 0)
            rows = [slice((dx * 9 + i) * c, (dx * 9 + i + 1) * c) for dx in range(3)]
            up = [roll(tile[i], grid.plane) for tile in tiles]
            down = [roll(tile[i], -grid.plane) for tile in tiles]
            for t in range(grid.tiles):
                before = up[t - 1] if t else low
                after = down[t + 1] if t + 1 < grid.tiles else high
                windows[rows[0], lanes_at(t)] = jnp.where(spot == 0, before, up[t])
                windows[rows[1], lanes_at(t)] = tiles[t][i]
                windows[rows[2], lanes_at(t)] = jnp.where(spot == grid.fold - 1, after, down[t])


class Summing:
    def __init__(self, acc, stage, first, mine, second, whole, third, sems):
        self.acc, self.stage, self.first = acc, stage, first
        self.mine, self.second, self.whole, self.third = mine, second, whole, third
        self.sems = sems
        gy = lax.axis_size("gy")
        self.count = lax.axis_size("gx") * gy
        self.depth = lax.axis_size("gz")
        self.me = lax.axis_index("gx") * gy + lax.axis_index("gy")
        self.level = lax.axis_index("gz")

    def copy(self, phase, k, source, target, device):
        return pltpu.make_async_remote_copy(
            src_ref=source,
            dst_ref=target,
            send_sem=self.sems.at[phase, 0, k],
            recv_sem=self.sems.at[phase, 1, k],
            device_id=device,
            device_id_type=MESH,
        )

    def across(self, phase, source, target):
        gy, out = lax.axis_size("gy"), []
        for k in range(1, self.count):
            to = (self.me + k) % self.count
            out.append(self.copy(phase, k, source(to), target, {"gx": to // gy, "gy": to % gy}))
        return out

    def along(self, phase, source, target):
        out = []
        for k in range(1, self.depth):
            to = (self.level + k) % self.depth
            out.append(self.copy(phase, k, source(to), target, {"gz": to}))
        return out

    def scatters(self):
        return self.across(0, lambda to: self.stage.at[to], self.first.at[self.me])

    def alongs(self):
        source = (lambda to: self.mine) if self.third is None else (lambda to: self.mine.at[to])
        return self.along(1, source, self.second.at[self.level])

    def returns(self):
        here = self.third.at[self.level]
        return self.along(3, lambda to: here, here)

    def gathers(self):
        here = self.whole.at[self.me]
        return self.across(2, lambda to: here, here)

    def start(self):
        chunk = self.stage.shape[1]
        for i in range(self.count):
            self.stage[i] = self.acc[i * chunk : (i + 1) * chunk].astype(jnp.bfloat16)
        for copy in self.scatters():
            copy.start()
        self.first[self.me] = self.stage[self.me]

    def total(self, parts):
        total = parts[0].astype(jnp.float32)
        for i in range(1, parts.shape[0]):
            total = total + parts[i].astype(jnp.float32)
        return total

    def middle(self):
        for copy in self.scatters():
            copy.wait()
        self.mine[...] = self.total(self.first).reshape(self.mine.shape).astype(jnp.bfloat16)
        for copy in self.alongs():
            copy.start()
        self.second[self.level] = self.mine[...] if self.third is None else self.mine[self.level]

    def between(self):
        for copy in self.alongs():
            copy.wait()
        self.third[self.level] = self.total(self.second).astype(jnp.bfloat16)
        for copy in self.returns():
            copy.start()

    def last(self):
        if self.third is None:
            for copy in self.alongs():
                copy.wait()
            total = self.total(self.second)
        else:
            for copy in self.returns():
                copy.wait()
            total = self.third[...].astype(jnp.float32).reshape(self.whole.shape[1:])
        self.whole[self.me] = total.astype(jnp.bfloat16)
        for copy in self.gathers():
            copy.start()

    def finish(self):
        for copy in self.gathers():
            copy.wait()


class Slabs:
    def __init__(self, sent, came, sems, grid):
        self.sent, self.came, self.sems, self.grid = sent, came, sems, grid
        self.depth, self.level = lax.axis_size("gz"), lax.axis_index("gz")

    def copies(self):
        out = []
        for k in range(1, self.depth):
            to = (self.level + k) % self.depth
            out.append(
                pltpu.make_async_remote_copy(
                    src_ref=self.sent.at[to],
                    dst_ref=self.came.at[self.level],
                    send_sem=self.sems.at[0, k],
                    recv_sem=self.sems.at[1, k],
                    device_id={"gz": to},
                    device_id_type=MESH,
                )
            )
        return out

    def pack(self, field):
        fold, plane = self.grid.fold, self.grid.plane
        part = self.sent.shape[1]
        spot = self.grid.at(part)[0]
        for t in range(self.grid.tiles):
            for i in range(fold):
                out = None
                for j in range(fold):
                    piece = roll(field[j * part : (j + 1) * part, lanes_at(t)], plane * (j - i))
                    out = piece if out is None else jnp.where(spot == j, piece, out)
                self.sent[t * fold + i] = out
        for copy in self.copies():
            copy.start()
        self.came[self.level] = self.sent[self.level]

    def unpack(self, field):
        for copy in self.copies():
            copy.wait()
        fold, plane = self.grid.fold, self.grid.plane
        part = self.came.shape[1]
        spot = self.grid.at(part)[0]
        for t in range(self.grid.tiles):
            for j in range(fold):
                out = None
                for i in range(fold):
                    piece = roll(self.came[t * fold + i], plane * (i - j))
                    out = piece if out is None else jnp.where(spot == i, piece, out)
                field[j * part : (j + 1) * part, lanes_at(t)] = out


def greet():
    gx, gy, gz = [lax.axis_size(axis) for axis in ("gx", "gy", "gz")]
    me = lax.axis_index("gx") * gy + lax.axis_index("gy")
    level, row, half = lax.axis_index("gz"), lax.axis_index("gy"), lax.axis_index("gx")
    barrier = pltpu.get_barrier_semaphore()
    signal = lambda device: pl.semaphore_signal(barrier, inc=1, device_id=device, device_id_type=MESH)
    for k in range(1, gx * gy):
        to = (me + k) % (gx * gy)
        signal({"gx": to // gy, "gy": to % gy})
    for k in range(1, gz):
        signal({"gz": (level + k) % gz})
    extra = 0
    for across in BOTH:
        for dy in NEAR:
            for dz in NEAR:
                if dz and (across or dy):
                    extra += 1
                    signal(
                        {
                            "gx": (half + across) % gx,
                            "gy": (row + dy + gy) % gy,
                            "gz": (level + dz + gz) % gz,
                        }
                    )
    return barrier, gx * gy + gz - 2 + extra


def spread_map(fine, coarse):
    shape = (LANES, coarse.fold * LANES)
    small = lax.broadcasted_iota(jnp.int32, shape, 0)
    large = lax.broadcasted_iota(jnp.int32, shape, 1)
    y, z = large % LANES // fine.nz, large % fine.nz
    match = (
        (small // coarse.plane == large // LANES)
        & (small // coarse.nz % coarse.ny == y // 2)
        & (small % coarse.nz == z // 2)
    )
    ones = match.astype(jnp.float32)
    first = (match & (y % 2 == 0) & (z % 2 == 0)).astype(jnp.float32)
    return ones.astype(jnp.bfloat16), first.astype(jnp.bfloat16)


def order_map(coarse, count):
    shape = (coarse.plane * count,) * 2
    row = lax.broadcasted_iota(jnp.int32, shape, 0)
    column = lax.broadcasted_iota(jnp.int32, shape, 1)
    wide = count * coarse.nz
    match = (
        (row // wide == column // coarse.nz % coarse.ny)
        & (row % wide // coarse.nz == column // coarse.plane)
        & (row % coarse.nz == column % coarse.nz)
    )
    return match.astype(jnp.float32).astype(jnp.bfloat16)


def column_of(row):
    size = row.shape[1]
    across = lax.broadcasted_iota(jnp.int32, (size, size), 0)
    down = lax.broadcasted_iota(jnp.int32, (size, size), 1)
    return jnp.sum(jnp.where(across == down, row, 0.0), axis=1, keepdims=True)


def turn_in(volume, rows, field):
    channels, _, nx = volume.shape
    fold = LANES // nx
    for q in range(channels // fold):
        wide = jnp.concatenate([volume[q * fold + i] for i in range(fold)], axis=1)
        turned = wide.astype(jnp.float32).T
        for i in range(fold):
            begin = (q * fold + i) * PITCH
            rows[begin : begin + nx] = turned[i * nx : (i + 1) * nx]
    for x in range(nx):
        field[:, lanes_at(x)] = rows[pl.ds(x, channels, stride=PITCH), :].astype(jnp.bfloat16)


def turn_out(rows, out):
    channels, _, nx = out.shape
    fold = LANES // nx
    for q in range(channels // fold):
        begins = [(q * fold + i) * PITCH for i in range(fold)]
        wide = jnp.concatenate([rows[begin : begin + nx] for begin in begins], axis=0)
        turned = wide.T.astype(jnp.bfloat16)
        for i in range(fold):
            out[q * fold + i] = turned[:, i * nx : (i + 1) * nx]


def whole_kernel(setting, *refs):
    names, local = setting[3:]
    pl.run_scoped(lambda **held: stages(setting, dict(zip(names, refs)) | held), **local)


def stages(setting, named):
    fine_size, coarse_size, scales = setting[:3]
    fine, coarse = Grid(*fine_size), Grid(*coarse_size)
    r = lambda name: named[name]
    field = r("field")
    fields = ("a", "b", "gb", "ga")
    grids = (fine, coarse, coarse, fine)
    volume, w_a, b_a, w_b, b_b, cot = [r(n) for n in ("volume", "w_a", "b_a", "w_b", "b_b", "cot")]
    features, grad_in, out_wa, out_ba, out_wb, out_bb = [
        r(n) for n in ("features", "grad_in", "out_wa", "out_ba", "out_wb", "out_bb")
    ]
    c1, c2, c3 = field.shape[0], w_a.shape[1], w_b.shape[1]
    widths = dict(zip(fields, (c1, c2, c3, c2)))
    halos = {
        name: Exchange(
            grid,
            widths[name],
            [r(name + part) for part in ("_zs", "_zr", "_ys", "_yr", "_cs", "_cr", "_xs", "_xr", "_ds", "_dr")],
            r("halo_sems"),
            i,
        )
        for i, (name, grid) in enumerate(zip(fields, grids))
    }
    strips = {name: r(name + "_strips") for name in fields}
    win_a, win_b, win_gb, win_ga = [r(name + "_win") for name in fields]
    before_a, pooled, grad_b, grad_a = [r(n) for n in ("before_a", "pooled", "grad_b", "grad_a")]
    acc_a, acc_b, mixed, feat = [r(n) for n in ("acc_a", "acc_b", "mixed", "feat")]
    sum_a = Summing(acc_a, *[r(f"sum_a{i}") for i in range(5)], None, r("sum_sems").at[0])
    sum_b = Summing(acc_b, *[r(f"sum_b{i}") for i in range(6)], r("sum_sems").at[1])
    cots = Slabs(r("cot_sent"), r("cot_came"), r("slab_sems").at[0], coarse)
    feats = Slabs(r("feat_sent"), r("feat_came"), r("slab_sems").at[1], coarse)
    out_a, in_a, out_b, in_b, spread, thin, order = [
        r(n) for n in ("to_a", "from_a", "to_b", "from_b", "spread", "thin", "order")
    ]
    bf16 = jnp.bfloat16

    for name in fields:
        halos[name].clear()
    barrier, arrivals = greet()
    rows_in, rows_out = r("rows_in"), r("rows_out")
    turn_in(volume, rows_in, field)
    halos["a"].pack(field)
    pl.semaphore_wait(barrier, arrivals)
    halos["a"].start()
    order[...] = order_map(coarse, lax.axis_size("gz"))
    rows_cot = r("rows_cot")
    rows_cot[...] = cot[...].astype(jnp.float32).reshape(rows_cot.shape)
    total = None
    for y in range(coarse.ny):
        row = rows_cot[pl.ds(y, c3, stride=coarse.ny), :].astype(bf16)
        part = dot(row, order[y * LANES : (y + 1) * LANES])
        total = part if total is None else total + part
    mixed[...] = total.astype(bf16)
    cots.pack(mixed)

    taps = 9
    for dx in range(3):
        out_a[dx] = w_a[dx * taps * c1 : (dx + 1) * taps * c1].T
        for k in range(taps):
            tap = 26 - dx * taps - k
            in_a[dx, :, k * c2 : (k + 1) * c2] = w_a[tap * c1 : (tap + 1) * c1]
    out_b[...] = w_b[...].T
    for k in range(27):
        in_b[:, k * c3 : (k + 1) * c3] = w_b[(26 - k) * c2 : (27 - k) * c2]
    wide, narrow = spread_map(fine, coarse)
    spread[...] = wide
    thin[...] = narrow
    bias_a, bias_b = column_of(b_a[...]), column_of(b_b[...])
    acc_a[...] = jnp.zeros_like(acc_a)
    acc_b[...] = jnp.zeros_like(acc_b)

    halos["a"].wait()
    halos["a"].fine_windows(field, strips["a"], win_a)
    many = 2 * coarse.fold

    def forward_a(g, carry):
        before = bias_a
        for dx in range(3):
            before = before + dot(out_a[dx], win_a[:, lanes_at(g * many + dx, many)])
        before_a[:, lanes_at(g * many, many)] = before
        active = before * jax.nn.sigmoid(before)
        pieces = []
        for i in range(coarse.fold):
            first = active[:, 2 * i * LANES : (2 * i + 1) * LANES]
            pair = first + active[:, (2 * i + 1) * LANES : (2 * i + 2) * LANES]
            pair = pair + roll(pair, -1)
            pair = pair + roll(pair, -fine.nz)
            pieces.append((pair * 0.125).astype(bf16))
        pooled[:, lanes_at(g)] = dot_rows(jnp.concatenate(pieces, axis=1), thin[...]).astype(bf16)
        return carry

    lax.fori_loop(0, coarse.tiles, forward_a, 0)
    halos["b"].pack(pooled)
    halos["b"].start()
    cots.unpack(mixed)
    halos["b"].wait()
    halos["b"].coarse_windows(pooled, strips["b"], win_b)
    before = dot(out_b[...], win_b[...]) + bias_b
    grad_b[...] = (mixed[...].astype(jnp.float32) * slope_of(before)).astype(bf16)
    halos["gb"].pack(grad_b)
    halos["gb"].start()
    feat[...] = (before * jax.nn.sigmoid(before)).astype(bf16)
    feats.pack(feat)
    top_b = out_wb.shape[0]
    grad = grad_b[...]
    acc_b[:top_b] = dot_rows(win_b[...], grad)
    acc_b[top_b : top_b + 8] = dot_rows(jnp.ones((8, grad.shape[1]), bf16), grad)
    sum_b.start()
    halos["gb"].wait()
    halos["gb"].coarse_windows(grad_b, strips["gb"], win_gb)
    pooled[...] = dot(in_b[...], win_gb[...]).astype(bf16)

    def backward_b(g, carry):
        wide = dot(pooled[:, lanes_at(g)], spread[...]) * 0.125
        for i in range(coarse.fold):
            for j in BOTH:
                here = lanes_at(g * many + 2 * i + j)
                slope = slope_of(before_a[:, here])
                grad_a[:, here] = (wide[:, i * LANES : (i + 1) * LANES] * slope).astype(bf16)
        return carry

    lax.fori_loop(0, coarse.tiles, backward_b, 0)
    halos["ga"].pack(grad_a)
    halos["ga"].start()
    sum_b.middle()
    grad = grad_a[...]
    half, width = out_wa.shape[0] // 2, out_wa.shape[1]
    parts = [dot_rows(win_a[:, lanes_at(dx, fine.tiles)], grad) for dx in range(3)]
    whole = jnp.concatenate(parts, axis=0)
    acc_a[:half, :width] = whole[:half]
    acc_a[:half, width:] = whole[half:]
    acc_a[half : half + 8, :width] = dot_rows(jnp.ones((8, grad.shape[1]), bf16), grad)
    sum_a.start()
    sum_b.between()
    halos["ga"].wait()
    sum_a.middle()
    halos["ga"].fine_windows(grad_a, strips["ga"], win_ga)
    sum_b.last()

    def backward_a(g, carry):
        total = dot(in_a[0], win_ga[:, lanes_at(g * many, many)])
        for dx in (1, 2):
            total = total + dot(in_a[dx], win_ga[:, lanes_at(g * many + dx, many)])
        for i in range(many):
            tile = total[:, i * LANES : (i + 1) * LANES].astype(bf16).astype(jnp.float32)
            rows_out[pl.ds(g * many + i, c1, stride=PITCH), :] = tile
        return carry

    lax.fori_loop(0, coarse.tiles, backward_a, 0)
    sum_a.last()
    feats.unpack(feat)
    for y in range(coarse.ny):
        rows_cot[pl.ds(y, c3, stride=coarse.ny), :] = dot_rows(feat[...], order[y * LANES : (y + 1) * LANES])
    features[...] = rows_cot[...].reshape(features.shape).astype(bf16)
    turn_out(rows_out, grad_in)
    sum_b.finish()
    all_a, all_b = r("sum_a4"), r("sum_b4")
    scale_a, scale_b = scales
    flat_b = all_b[...].astype(jnp.float32).reshape(-1, all_b.shape[2]) * scale_b
    out_wb[...] = flat_b[:top_b]
    out_bb[...] = flat_b[top_b : top_b + 1]
    sum_a.finish()
    flat_a = all_a[...].astype(jnp.float32).reshape(-1, all_a.shape[2]) * scale_a
    out_wa[:half] = flat_a[:half, :width]
    out_wa[half:] = flat_a[:half, width:]
    out_ba[...] = flat_a[half : half + 1, :width]


def on_device(volume, weight_a, bias_a, weight_b, bias_b, cotangent):
    f32, bf16 = jnp.float32, jnp.bfloat16
    members, levels = lax.axis_size("gx") * lax.axis_size("gy"), lax.axis_size("gz")
    c1, nx, ny, nz = volume.shape
    c2, c3 = weight_b.shape[3:]
    cells = nx * ny * nz
    fewer = cells // 8
    scale_a = 1.0 / math.sqrt(cells * members * levels)
    scale_b = 1.0 / math.sqrt(cells * members * levels // 8)
    fine_size, coarse_size = (nx, ny, nz), (nx // 2, ny // 2, nz // 2)
    fine, coarse = Grid(*fine_size), Grid(*coarse_size)
    rows_a = 27 * c1 // 2 + 16
    rows_a += -rows_a % (16 * members)
    rows_b = 27 * c2 + 16
    rows_b += -rows_b % (8 * members * levels)
    operands = {
        "volume": jnp.transpose(volume, (0, 2, 3, 1)).reshape(c1, ny * nz, nx),
        "w_a": weight_a.reshape(27 * c1, c2),
        "b_a": bias_a.reshape(1, c2),
        "w_b": weight_b.reshape(27 * c2, c3),
        "b_b": bias_b.reshape(1, c3),
        "cot": cotangent.reshape(c3, ny // 2, nz // 2 * levels),
    }
    outs = {
        "features": ((c3, ny // 2, nz // 2 * levels), bf16),
        "grad_in": ((c1, ny * nz, nx), bf16),
        "out_wa": ((27 * c1, c2), f32),
        "out_ba": ((1, c2), f32),
        "out_wb": ((27 * c2, c3), f32),
        "out_bb": ((1, c3), f32),
    }
    scratch, local = {}, {}
    for name, grid, c in (("a", fine, c1), ("b", coarse, c2), ("gb", coarse, c3), ("ga", fine, c2)):
        for end in ("s", "r"):
            scratch[f"{name}_z{end}"] = pltpu.VMEM((2, c, grid.zpacks * LANES), bf16)
            scratch[f"{name}_y{end}"] = pltpu.VMEM((2, c, grid.ypacks * LANES), bf16)
            scratch[f"{name}_c{end}"] = pltpu.VMEM((4, c // grid.corner_groups(c), LANES), bf16)
        scratch[f"{name}_xs"] = pltpu.VMEM((c // grid.fold, LANES), bf16)
        scratch[f"{name}_xr"] = pltpu.VMEM((3, c // grid.fold, LANES), bf16)
        scratch[f"{name}_ds"] = pltpu.VMEM((2, 16, LANES), bf16)
        scratch[f"{name}_dr"] = pltpu.VMEM((2, 3, 16, LANES), bf16)
        local[f"{name}_strips"] = pltpu.VMEM((6, c, grid.ypacks * LANES), bf16)
        shape = (9 * c, (grid.tiles + 2) * LANES) if grid is fine else (27 * c, grid.tiles * LANES)
        local[f"{name}_win"] = pltpu.VMEM(shape, bf16)
    local["field"] = pltpu.VMEM((c1, cells), bf16)
    local["rows_in"] = local["rows_out"] = pltpu.VMEM((c1 * PITCH, ny * nz), f32)
    local["rows_cot"] = pltpu.VMEM((c3 * ny // 2, nz // 2 * levels), f32)
    local["before_a"] = pltpu.VMEM((c2, cells), f32)
    local["pooled"] = pltpu.VMEM((c2, fewer), bf16)
    local["grad_b"] = pltpu.VMEM((c3, fewer), bf16)
    local["grad_a"] = pltpu.VMEM((c2, cells), bf16)
    local["mixed"] = pltpu.VMEM((c3, fewer), bf16)
    local["feat"] = pltpu.VMEM((c3, fewer), bf16)
    for name, rows in (("a", rows_a), ("b", rows_b)):
        chunk = rows // members
        scratch[f"acc_{name}"] = pltpu.VMEM((rows, LANES), f32)
        shapes = [(members, chunk), (members, chunk), (chunk,), (levels, chunk), (members, chunk)]
        if name == "b":
            shapes[2:4] = [(levels, chunk // levels)] * 2
            shapes.append((levels, chunk // levels))
        for i, shape in enumerate(shapes):
            scratch[f"sum_{name}{i}"] = pltpu.VMEM((*shape, LANES), bf16)
    for name in ("cot_sent", "cot_came", "feat_sent", "feat_came"):
        scratch[name] = pltpu.VMEM((levels, c3 // coarse.fold, LANES), bf16)
    local["to_a"] = pltpu.VMEM((3, c2, 9 * c1), bf16)
    local["from_a"] = pltpu.VMEM((3, c1, 9 * c2), bf16)
    local["to_b"] = pltpu.VMEM((c3, 27 * c2), bf16)
    local["from_b"] = pltpu.VMEM((c2, 27 * c3), bf16)
    local["spread"] = pltpu.VMEM((LANES, coarse.fold * LANES), bf16)
    local["thin"] = pltpu.VMEM((LANES, coarse.fold * LANES), bf16)
    local["order"] = pltpu.VMEM((fewer, fewer), bf16)
    scratch["halo_sems"] = pltpu.SemaphoreType.DMA((2, 4, 17))
    scratch["sum_sems"] = pltpu.SemaphoreType.DMA((2, 4, 2, max(members, levels)))
    scratch["slab_sems"] = pltpu.SemaphoreType.DMA((2, 2, levels))
    names = (*operands, *outs, *scratch)
    got = pl.pallas_call(
        functools.partial(whole_kernel, (fine_size, coarse_size, (scale_a, scale_b), names, local)),
        out_shape=[jax.ShapeDtypeStruct(shape, dtype) for shape, dtype in outs.values()],
        in_specs=[pl.BlockSpec(memory_space=pltpu.VMEM)] * len(operands),
        out_specs=[pl.BlockSpec(memory_space=pltpu.VMEM)] * len(outs),
        scratch_shapes=list(scratch.values()),
        compiler_params=pltpu.CompilerParams(
            collective_id=1, has_side_effects=True, vmem_limit_bytes=60 * 2**20
        ),
    )(*operands.values())
    features, grad_in, sum_wa, sum_ba, sum_wb, sum_bb = got
    return (
        features.reshape(cotangent.shape),
        jnp.transpose(grad_in.reshape(c1, ny, nz, nx), (0, 3, 1, 2)),
        sum_wa.reshape(weight_a.shape),
        sum_ba.reshape(c2),
        sum_wb.reshape(weight_b.shape),
        sum_bb.reshape(c3),
    )


def solution(mesh):
    return jax.shard_map(
        on_device,
        mesh=mesh,
        in_specs=(P(None, "gx", "gy", "gz"), P(), P(), P(), P(), P(None, ("gx", "gz"), "gy", None)),
        out_specs=(
            P(None, ("gx", "gz"), "gy", None),
            P(None, "gx", "gy", "gz"),
            P(),
            P(),
            P(),
            P(),
        ),
        check_vma=False,
    )
```

```python
import functools
import math

import jax
import jax.numpy as jnp
from jax import lax
from jax.experimental import pallas as pl
from jax.experimental.pallas import tpu as pltpu
from jax.sharding import PartitionSpec as P

MESH = pl.DeviceIdType.MESH
LANES = 128
PITCH = 40
BOTH = (0, 1)
NEAR = (-1, 0, 1)


def slope_of(value):
    sigma = jax.nn.sigmoid(value)
    return sigma + value * sigma * (1.0 - sigma)


def dot(left, right):
    return jnp.dot(left, right, preferred_element_type=jnp.float32)


def dot_rows(left, right):
    return lax.dot_general(
        left, right, (((1,), (1,)), ((), ())), preferred_element_type=jnp.float32
    )


def roll(value, by):
    by = by % LANES
    return pltpu.roll(value, by, 1) if by else value


def lanes_at(index, count=1):
    begin = index * LANES
    if not isinstance(begin, int):
        begin = pl.multiple_of(begin, LANES)
    return pl.ds(begin, count * LANES)


def within(at, count):
    return (at >= 0) & (at < count)


class Grid:
    def __init__(self, nx, ny, nz):
        self.ny, self.nz = ny, nz
        self.plane = ny * nz
        self.fold = LANES // self.plane
        self.tiles = nx // self.fold
        self.zpacks = -(-self.tiles // nz)
        self.ypacks = -(-self.tiles // ny)
        self.group = max(ny, min(nz, self.tiles))

    def at(self, rows):
        lane = lax.broadcasted_iota(jnp.int32, (rows, LANES), 1)
        return lane // self.plane, lane // self.nz % self.ny, lane % self.nz

    def corner_groups(self, channels):
        return min(channels // 16, self.nz // self.ypacks)


class Exchange:
    def __init__(self, grid, channels, buffers, sems, at):
        self.grid, self.channels = grid, channels
        self.zs, self.zr, self.ys, self.yr, self.cs, self.cr, self.xs, self.xr, self.ds, self.dr = buffers
        self.gx, self.gy, self.gz = [lax.axis_index(axis) for axis in ("gx", "gy", "gz")]
        cuts_y, cuts_z = lax.axis_size("gy"), lax.axis_size("gz")
        moves = []
        step = (1, -1)
        for side in BOTH:
            moves.append((self.ys.at[side], self.yr.at[side], 0, step[side], 0))
        for dy in NEAR:
            for dz in NEAR:
                source = self.ds.at[(1 - dy) // 2] if dy else self.xs
                target = self.dr.at[(1 - dy) // 2, 1 - dz] if dy else self.xr.at[1 - dz]
                moves.append((source, target, 1, dy, dz))
        for side in BOTH:
            moves.append((self.zs.at[side], self.zr.at[side], 0, 0, step[side]))
        for sy in BOTH:
            for sz in BOTH:
                i = sy * 2 + sz
                moves.append((self.cs.at[i], self.cr.at[i], 0, step[sy], step[sz]))
        self.moves, self.targets = [], []
        for i, (source, target, across, dy, dz) in enumerate(moves):
            copy = pltpu.make_async_remote_copy(
                src_ref=source,
                dst_ref=target,
                send_sem=sems.at[0, at, i],
                recv_sem=sems.at[1, at, i],
                device_id={
                    "gx": (self.gx + across) % 2,
                    "gy": (self.gy + dy + cuts_y) % cuts_y,
                    "gz": (self.gz + dz + cuts_z) % cuts_z,
                },
                device_id_type=MESH,
            )
            goes = within(self.gy + dy, cuts_y) & within(self.gz + dz, cuts_z)
            comes = within(self.gy - dy, cuts_y) & within(self.gz - dz, cuts_z)
            self.moves.append((copy, goes, comes))
            if dy or dz:
                self.targets.append((target, comes))

    def clear(self):
        for target, comes in self.targets:

            @pl.when(jnp.logical_not(comes))
            def _(target=target):
                target[...] = jnp.zeros(target.shape, jnp.bfloat16)

    def pack(self, field):
        grid, c = self.grid, self.channels
        spot, y, z = grid.at(c)
        last_z, last_y = grid.nz - 1, grid.ny - 1
        ends = [field[:, lanes_at(t)] for t in (grid.tiles - 1, 0)]
        if grid.fold == 1:
            self.xs[...] = jnp.where(spot + self.gx == 0, *ends)
        else:
            part = c // grid.fold
            place = grid.at(part)[0]
            made = []
            for end, i in zip(ends, (grid.fold - 1, 0)):
                out = end[:part]
                out = roll(out, grid.plane * -i)
                for j in range(1, grid.fold):
                    piece = roll(end[j * part : (j + 1) * part], grid.plane * (j - i))
                    out = jnp.where(place == j, piece, out)
                made.append(out)
            self.xs[...] = jnp.where(place * 0 + self.gx == 0, *made)

        groups = c // 16
        block = lax.broadcasted_iota(jnp.int32, (16, LANES), 1) // grid.nz
        for side in BOTH:
            made = []
            for end, i in zip(ends, (grid.fold - 1, 0)):
                here = i * grid.ny + (last_y if side == 0 else 0)
                out = None
                for j in range(groups):
                    piece = roll(end[16 * j : 16 * j + 16], grid.nz * (j - here))
                    out = piece if out is None else jnp.where(block == j, piece, out)
                made.append(out)
            self.ds[side] = jnp.where(block * 0 + self.gx == 0, *made)

        def one(q, carry):
            held = [None, None]
            rows = [None, None]
            for k in range(grid.group):
                tile = field[:, lanes_at(q * grid.group + k)]
                j = k % grid.ny
                for side in BOTH:
                    piece = roll(tile, k - last_z if side == 0 else k)
                    held[side] = piece if k == 0 else jnp.where(z == k, piece, held[side])
                    piece = roll(tile, grid.nz * (j - last_y if side == 0 else j))
                    rows[side] = piece if j == 0 else jnp.where(y == j, piece, rows[side])
                    if j == last_y:
                        self.ys[side, :, lanes_at(q * (grid.group // grid.ny) + k // grid.ny)] = rows[side]
            for side in BOTH:
                self.zs[side, :, lanes_at(q)] = held[side]
            return carry

        loops = grid.tiles // grid.group
        if loops == 1:
            one(0, 0)
        else:
            lax.fori_loop(0, loops, one, 0)
        groups, packs = grid.corner_groups(c), grid.ypacks
        part = c // groups
        z = grid.at(part)[2]
        for sy in BOTH:
            for sz in BOTH:
                out = None
                for j in range(groups):
                    for p in range(packs):
                        to = packs * j + p
                        piece = self.ys[sy, j * part : (j + 1) * part, lanes_at(p)]
                        piece = roll(piece, to - (last_z if sz == 0 else 0))
                        out = piece if out is None else jnp.where(z == to, piece, out)
                self.cs[sy * 2 + sz] = out

    def start(self):
        for copy, goes, _ in self.moves:
            pl.when(goes)(copy.start)

    def wait(self):
        for copy, goes, comes in self.moves:
            pl.when(goes)(copy.wait_send)
            pl.when(comes)(copy.wait_recv)

    def shift_z(self, tile, low, high, dz, z):
        if dz == 0:
            return tile
        if dz < 0:
            return jnp.where(z == 0, low, roll(tile, 1))
        return jnp.where(z == self.grid.nz - 1, high, roll(tile, -1))

    def shift_y(self, tile, low, high, dy, y):
        if dy == 0:
            return tile
        if dy < 0:
            return jnp.where(y == 0, low, roll(tile, self.grid.nz))
        return jnp.where(y == self.grid.ny - 1, high, roll(tile, -self.grid.nz))

    def beyond(self):
        grid, c = self.grid, self.channels
        _, y, z = grid.at(c)
        last = grid.fold - 1
        if grid.fold == 1:
            came = [self.xr[i] for i in range(3)]
        else:
            came = [
                jnp.concatenate([roll(self.xr[i], grid.plane * (last - j)) for j in range(grid.fold)], axis=0)
                for i in range(3)
            ]
        over = []
        for side in BOTH:
            to = last * grid.ny + (0 if side == 0 else grid.ny - 1)
            over.append(
                [
                    jnp.concatenate(
                        [roll(self.dr[side, i], grid.nz * (to - j)) for j in range(c // 16)], axis=0
                    )
                    for i in range(3)
                ]
            )
        rows = []
        for low, here, high in (over[0], came, over[1]):
            low, high = roll(low, 1 - grid.nz), roll(high, grid.nz - 1)
            rows.append([self.shift_z(here, low, high, dz, z) for dz in NEAR])
        return [
            self.shift_y(rows[1][dz], rows[0][dz], rows[2][dz], dy, y) for dy in NEAR for dz in range(3)
        ]

    def strips(self, shifted):
        grid, c = self.grid, self.channels
        groups, packs = grid.corner_groups(c), grid.ypacks
        _, _, z = grid.at(c)
        for side in BOTH:
            for p in range(packs):
                tile = self.yr[side, :, lanes_at(p)]
                ends = []
                for sz in BOTH:
                    to = 0 if sz == 0 else grid.nz - 1
                    corner = self.cr[side * 2 + sz]
                    ends.append(
                        jnp.concatenate([roll(corner, to - packs * j - p) for j in range(groups)], axis=0)
                    )
                for dz in NEAR:
                    shifted[side * 3 + dz + 1, :, lanes_at(p)] = self.shift_z(tile, *ends, dz, z)

    def tile_shifts(self, field, shifted, q, k):
        grid, c = self.grid, self.channels
        _, y, z = grid.at(c)
        last_z, last_y = grid.nz - 1, grid.ny - 1
        tile = field[:, lanes_at(q * grid.group + k)]
        low = roll(self.zr[0, :, lanes_at(q)], -k)
        high = roll(self.zr[1, :, lanes_at(q)], last_z - k)
        moved = [self.shift_z(tile, low, high, dz, z) for dz in NEAR]
        p, j = q * (grid.group // grid.ny) + k // grid.ny, k % grid.ny
        out = []
        for dy in NEAR:
            for dz in range(3):
                low = high = None
                if dy < 0:
                    low = roll(shifted[dz, :, lanes_at(p)], -grid.nz * j)
                if dy > 0:
                    high = roll(shifted[3 + dz, :, lanes_at(p)], grid.nz * (last_y - j))
                out.append(self.shift_y(moved[dz], low, high, dy, y))
        return out

    def only(self, value, side):
        flag = lax.broadcasted_iota(jnp.int32, value.shape, 1) * 0 + self.gx
        return jnp.where(flag == side, value, jnp.zeros_like(value))

    def fine_windows(self, field, shifted, windows):
        grid, c = self.grid, self.channels
        self.strips(shifted)
        for i, value in enumerate(self.beyond()):
            windows[i * c : (i + 1) * c, lanes_at(0)] = self.only(value, 1)
            windows[i * c : (i + 1) * c, lanes_at(grid.tiles + 1)] = self.only(value, 0)

        def one(q, carry):
            for k in range(grid.group):
                for i, value in enumerate(self.tile_shifts(field, shifted, q, k)):
                    windows[i * c : (i + 1) * c, lanes_at(q * grid.group + k + 1)] = value
            return carry

        lax.fori_loop(0, grid.tiles // grid.group, one, 0)

    def coarse_windows(self, field, shifted, windows):
        grid, c = self.grid, self.channels
        spot = grid.at(c)[0]
        self.strips(shifted)
        outer = self.beyond()
        tiles = [self.tile_shifts(field, shifted, 0, k) for k in range(grid.tiles)]
        for i in range(9):
            low = roll(self.only(outer[i], 1), grid.plane)
            high = self.only(outer[i], 0)
            rows = [slice((dx * 9 + i) * c, (dx * 9 + i + 1) * c) for dx in range(3)]
            up = [roll(tile[i], grid.plane) for tile in tiles]
            down = [roll(tile[i], -grid.plane) for tile in tiles]
            for t in range(grid.tiles):
                before = up[t - 1] if t else low
                after = down[t + 1] if t + 1 < grid.tiles else high
                windows[rows[0], lanes_at(t)] = jnp.where(spot == 0, before, up[t])
                windows[rows[1], lanes_at(t)] = tiles[t][i]
                windows[rows[2], lanes_at(t)] = jnp.where(spot == grid.fold - 1, after, down[t])


def ring(step, count):
    return min(step, count - step)


def far_first(count, hops):
    return sorted(range(1, count), key=hops, reverse=True)


def across_at(k):
    gx, gy = lax.axis_size("gx"), lax.axis_size("gy")
    high, low = gy // 4, 4
    row = lax.axis_index("gy")
    x = (row // low * gx + lax.axis_index("gx") + k // low) % (gx * high)
    return x % gx, x // gx * low + (row + k) % low


class Summing:
    def __init__(self, acc, stage, first, mine, second, whole, third, sems):
        self.acc, self.stage, self.first = acc, stage, first
        self.mine, self.second, self.whole, self.third = mine, second, whole, third
        self.sems = sems
        gy = lax.axis_size("gy")
        self.count = lax.axis_size("gx") * gy
        self.depth = lax.axis_size("gz")
        self.me = lax.axis_index("gx") * gy + lax.axis_index("gy")
        self.level = lax.axis_index("gz")

    def copy(self, phase, k, source, target, device):
        return pltpu.make_async_remote_copy(
            src_ref=source,
            dst_ref=target,
            send_sem=self.sems.at[phase, 0, k],
            recv_sem=self.sems.at[phase, 1, k],
            device_id=device,
            device_id_type=MESH,
        )

    def across(self, phase, source, target):
        gy, out = lax.axis_size("gy"), []
        for k in far_first(self.count, lambda k: ring(k // 4, self.count // 4) + ring(k % 4, 4)):
            gx, row = across_at(k)
            to = gx * gy + row
            out.append(self.copy(phase, k, source(to), target, {"gx": gx, "gy": row}))
        return out

    def along(self, phase, source, target):
        out = []
        for k in far_first(self.depth, lambda k: ring(k, self.depth)):
            to = (self.level + k) % self.depth
            out.append(self.copy(phase, k, source(to), target, {"gz": to}))
        return out

    def scatters(self):
        return self.across(0, lambda to: self.stage.at[to], self.first.at[self.me])

    def alongs(self):
        source = (lambda to: self.mine) if self.third is None else (lambda to: self.mine.at[to])
        return self.along(1, source, self.second.at[self.level])

    def returns(self):
        here = self.third.at[self.level]
        return self.along(3, lambda to: here, here)

    def gathers(self):
        here = self.whole.at[self.me]
        return self.across(2, lambda to: here, here)

    def start(self):
        chunk = self.stage.shape[1]
        for i in range(self.count):
            self.stage[i] = self.acc[i * chunk : (i + 1) * chunk].astype(jnp.bfloat16)
        for copy in self.scatters():
            copy.start()
        self.first[self.me] = self.stage[self.me]

    def total(self, parts):
        total = parts[0].astype(jnp.float32)
        for i in range(1, parts.shape[0]):
            total = total + parts[i].astype(jnp.float32)
        return total

    def middle(self):
        for copy in self.scatters():
            copy.wait()
        self.mine[...] = self.total(self.first).reshape(self.mine.shape).astype(jnp.bfloat16)
        for copy in self.alongs():
            copy.start()
        self.second[self.level] = self.mine[...] if self.third is None else self.mine[self.level]

    def between(self):
        for copy in self.alongs():
            copy.wait()
        self.third[self.level] = self.total(self.second).astype(jnp.bfloat16)
        for copy in self.returns():
            copy.start()

    def last(self):
        if self.third is None:
            for copy in self.alongs():
                copy.wait()
            total = self.total(self.second)
        else:
            for copy in self.returns():
                copy.wait()
            total = self.third[...].astype(jnp.float32).reshape(self.whole.shape[1:])
        self.whole[self.me] = total.astype(jnp.bfloat16)
        for copy in self.gathers():
            copy.start()

    def finish(self):
        for copy in self.gathers():
            copy.wait()


class Slabs:
    def __init__(self, sent, came, sems, grid):
        self.sent, self.came, self.sems, self.grid = sent, came, sems, grid
        self.depth, self.level = lax.axis_size("gz"), lax.axis_index("gz")

    def copies(self):
        out = []
        for k in far_first(self.depth, lambda k: ring(k, self.depth)):
            to = (self.level + k) % self.depth
            out.append(
                pltpu.make_async_remote_copy(
                    src_ref=self.sent.at[to],
                    dst_ref=self.came.at[self.level],
                    send_sem=self.sems.at[0, k],
                    recv_sem=self.sems.at[1, k],
                    device_id={"gz": to},
                    device_id_type=MESH,
                )
            )
        return out

    def pack(self, field):
        fold, plane = self.grid.fold, self.grid.plane
        part = self.sent.shape[1]
        spot = self.grid.at(part)[0]
        for t in range(self.grid.tiles):
            for i in range(fold):
                out = None
                for j in range(fold):
                    piece = roll(field[j * part : (j + 1) * part, lanes_at(t)], plane * (j - i))
                    out = piece if out is None else jnp.where(spot == j, piece, out)
                self.sent[t * fold + i] = out
        for copy in self.copies():
            copy.start()
        self.came[self.level] = self.sent[self.level]

    def unpack(self, field):
        for copy in self.copies():
            copy.wait()
        fold, plane = self.grid.fold, self.grid.plane
        part = self.came.shape[1]
        spot = self.grid.at(part)[0]
        for t in range(self.grid.tiles):
            for j in range(fold):
                out = None
                for i in range(fold):
                    piece = roll(self.came[t * fold + i], plane * (i - j))
                    out = piece if out is None else jnp.where(spot == i, piece, out)
                field[j * part : (j + 1) * part, lanes_at(t)] = out


def greet():
    gx, gy, gz = [lax.axis_size(axis) for axis in ("gx", "gy", "gz")]
    me = lax.axis_index("gx") * gy + lax.axis_index("gy")
    level, row, half = lax.axis_index("gz"), lax.axis_index("gy"), lax.axis_index("gx")
    barrier = pltpu.get_barrier_semaphore()
    signal = lambda device: pl.semaphore_signal(barrier, inc=1, device_id=device, device_id_type=MESH)
    for k in range(1, gx * gy):
        to = (me + k) % (gx * gy)
        signal({"gx": to // gy, "gy": to % gy})
    for k in range(1, gz):
        signal({"gz": (level + k) % gz})
    extra = 0
    for across in BOTH:
        for dy in NEAR:
            for dz in NEAR:
                if dz and (across or dy):
                    extra += 1
                    signal(
                        {
                            "gx": (half + across) % gx,
                            "gy": (row + dy + gy) % gy,
                            "gz": (level + dz + gz) % gz,
                        }
                    )
    return barrier, gx * gy + gz - 2 + extra


def spread_map(fine, coarse):
    shape = (LANES, coarse.fold * LANES)
    small = lax.broadcasted_iota(jnp.int32, shape, 0)
    large = lax.broadcasted_iota(jnp.int32, shape, 1)
    y, z = large % LANES // fine.nz, large % fine.nz
    match = (
        (small // coarse.plane == large // LANES)
        & (small // coarse.nz % coarse.ny == y // 2)
        & (small % coarse.nz == z // 2)
    )
    ones = match.astype(jnp.float32)
    first = (match & (y % 2 == 0) & (z % 2 == 0)).astype(jnp.float32)
    return ones.astype(jnp.bfloat16), first.astype(jnp.bfloat16)


def order_map(coarse, count):
    shape = (coarse.plane * count,) * 2
    row = lax.broadcasted_iota(jnp.int32, shape, 0)
    column = lax.broadcasted_iota(jnp.int32, shape, 1)
    wide = count * coarse.nz
    match = (
        (row // wide == column // coarse.nz % coarse.ny)
        & (row % wide // coarse.nz == column // coarse.plane)
        & (row % coarse.nz == column % coarse.nz)
    )
    return match.astype(jnp.float32).astype(jnp.bfloat16)


def column_of(row):
    size = row.shape[1]
    across = lax.broadcasted_iota(jnp.int32, (size, size), 0)
    down = lax.broadcasted_iota(jnp.int32, (size, size), 1)
    return jnp.sum(jnp.where(across == down, row, 0.0), axis=1, keepdims=True)


def turn_in(volume, rows, field):
    channels, _, nx = volume.shape
    fold = LANES // nx
    for q in range(channels // fold):
        wide = jnp.concatenate([volume[q * fold + i] for i in range(fold)], axis=1)
        turned = wide.astype(jnp.float32).T
        for i in range(fold):
            begin = (q * fold + i) * PITCH
            rows[begin : begin + nx] = turned[i * nx : (i + 1) * nx]
    for x in range(nx):
        field[:, lanes_at(x)] = rows[pl.ds(x, channels, stride=PITCH), :].astype(jnp.bfloat16)


def turn_out(rows, out):
    channels, _, nx = out.shape
    fold = LANES // nx
    for q in range(channels // fold):
        begins = [(q * fold + i) * PITCH for i in range(fold)]
        wide = jnp.concatenate([rows[begin : begin + nx] for begin in begins], axis=0)
        turned = wide.T.astype(jnp.bfloat16)
        for i in range(fold):
            out[q * fold + i] = turned[:, i * nx : (i + 1) * nx]


def whole_kernel(setting, *refs):
    names, local = setting[3:]
    pl.run_scoped(lambda **held: stages(setting, dict(zip(names, refs)) | held), **local)


def stages(setting, named):
    fine_size, coarse_size, scales = setting[:3]
    fine, coarse = Grid(*fine_size), Grid(*coarse_size)
    r = lambda name: named[name]
    field = r("field")
    fields = ("a", "b", "gb", "ga")
    grids = (fine, coarse, coarse, fine)
    volume, w_a, b_a, w_b, b_b, cot = [r(n) for n in ("volume", "w_a", "b_a", "w_b", "b_b", "cot")]
    features, grad_in, out_wa, out_ba, out_wb, out_bb = [
        r(n) for n in ("features", "grad_in", "out_wa", "out_ba", "out_wb", "out_bb")
    ]
    c1, c2, c3 = field.shape[0], w_a.shape[1], w_b.shape[1]
    widths = dict(zip(fields, (c1, c2, c3, c2)))
    halos = {
        name: Exchange(
            grid,
            widths[name],
            [r(name + part) for part in ("_zs", "_zr", "_ys", "_yr", "_cs", "_cr", "_xs", "_xr", "_ds", "_dr")],
            r("halo_sems"),
            i,
        )
        for i, (name, grid) in enumerate(zip(fields, grids))
    }
    strips = {name: r(name + "_strips") for name in fields}
    win_a, win_b, win_gb, win_ga = [r(name + "_win") for name in fields]
    before_a, pooled, grad_b, grad_a = [r(n) for n in ("before_a", "pooled", "grad_b", "grad_a")]
    acc_a, acc_b, mixed, feat = [r(n) for n in ("acc_a", "acc_b", "mixed", "feat")]
    sum_a = Summing(acc_a, *[r(f"sum_a{i}") for i in range(5)], None, r("sum_sems").at[0])
    sum_b = Summing(acc_b, *[r(f"sum_b{i}") for i in range(6)], r("sum_sems").at[1])
    cots = Slabs(r("cot_sent"), r("cot_came"), r("slab_sems").at[0], coarse)
    feats = Slabs(r("feat_sent"), r("feat_came"), r("slab_sems").at[1], coarse)
    out_a, in_a, out_b, in_b, spread, thin, order = [
        r(n) for n in ("to_a", "from_a", "to_b", "from_b", "spread", "thin", "order")
    ]
    bf16 = jnp.bfloat16

    loads = {
        name: pltpu.make_async_copy(r(name + "_hbm"), r(name), r("load_sems").at[i])
        for i, name in enumerate(("volume", "cot", "w_a", "w_b"))
    }
    for load in loads.values():
        load.start()
    barrier, arrivals = greet()
    halos["a"].clear()
    rows_in, rows_out = r("rows_in"), r("rows_out")
    loads["volume"].wait()
    turn_in(volume, rows_in, field)
    halos["a"].pack(field)
    pl.semaphore_wait(barrier, arrivals)
    halos["a"].start()
    order[...] = order_map(coarse, lax.axis_size("gz"))
    rows_cot = r("rows_cot")
    loads["cot"].wait()
    rows_cot[...] = cot[...].astype(jnp.float32).reshape(rows_cot.shape)
    total = None
    for y in range(coarse.ny):
        row = rows_cot[pl.ds(y, c3, stride=coarse.ny), :].astype(bf16)
        part = dot(row, order[y * LANES : (y + 1) * LANES])
        total = part if total is None else total + part
    mixed[...] = total.astype(bf16)
    cots.pack(mixed)

    loads["w_a"].wait()
    loads["w_b"].wait()
    taps = 9
    for dx in range(3):
        out_a[dx] = w_a[dx * taps * c1 : (dx + 1) * taps * c1].T
        for k in range(taps):
            tap = 26 - dx * taps - k
            in_a[dx, :, k * c2 : (k + 1) * c2] = w_a[tap * c1 : (tap + 1) * c1]
    out_b[...] = w_b[...].T
    for k in range(27):
        in_b[:, k * c3 : (k + 1) * c3] = w_b[(26 - k) * c2 : (27 - k) * c2]
    wide, narrow = spread_map(fine, coarse)
    spread[...] = wide
    thin[...] = narrow
    for name in fields[1:]:
        halos[name].clear()
    bias_a, bias_b = column_of(b_a[...]), column_of(b_b[...])
    acc_a[...] = jnp.zeros_like(acc_a)
    acc_b[...] = jnp.zeros_like(acc_b)

    halos["a"].wait()
    halos["a"].fine_windows(field, strips["a"], win_a)
    many = 2 * coarse.fold

    def forward_a(g, carry):
        before = bias_a
        for dx in range(3):
            before = before + dot(out_a[dx], win_a[:, lanes_at(g * many + dx, many)])
        before_a[:, lanes_at(g * many, many)] = before
        active = before * jax.nn.sigmoid(before)
        pieces = []
        for i in range(coarse.fold):
            first = active[:, 2 * i * LANES : (2 * i + 1) * LANES]
            pair = first + active[:, (2 * i + 1) * LANES : (2 * i + 2) * LANES]
            pair = pair + roll(pair, -1)
            pair = pair + roll(pair, -fine.nz)
            pieces.append((pair * 0.125).astype(bf16))
        pooled[:, lanes_at(g)] = dot_rows(jnp.concatenate(pieces, axis=1), thin[...]).astype(bf16)
        return carry

    lax.fori_loop(0, coarse.tiles, forward_a, 0)
    halos["b"].pack(pooled)
    halos["b"].start()
    cots.unpack(mixed)
    halos["b"].wait()
    halos["b"].coarse_windows(pooled, strips["b"], win_b)
    before = dot(out_b[...], win_b[...]) + bias_b
    grad_b[...] = (mixed[...].astype(jnp.float32) * slope_of(before)).astype(bf16)
    halos["gb"].pack(grad_b)
    halos["gb"].start()
    feat[...] = (before * jax.nn.sigmoid(before)).astype(bf16)
    feats.pack(feat)
    top_b = out_wb.shape[0]
    grad = grad_b[...]
    acc_b[:top_b] = dot_rows(win_b[...], grad)
    acc_b[top_b : top_b + 8] = dot_rows(jnp.ones((8, grad.shape[1]), bf16), grad)
    sum_b.start()
    halos["gb"].wait()
    halos["gb"].coarse_windows(grad_b, strips["gb"], win_gb)
    pooled[...] = dot(in_b[...], win_gb[...]).astype(bf16)

    def backward_b(g, carry):
        wide = dot(pooled[:, lanes_at(g)], spread[...]) * 0.125
        for i in range(coarse.fold):
            for j in BOTH:
                here = lanes_at(g * many + 2 * i + j)
                slope = slope_of(before_a[:, here])
                grad_a[:, here] = (wide[:, i * LANES : (i + 1) * LANES] * slope).astype(bf16)
        return carry

    lax.fori_loop(0, coarse.tiles, backward_b, 0)
    halos["ga"].pack(grad_a)
    halos["ga"].start()
    sum_b.middle()
    grad = grad_a[...]
    half, width = out_wa.shape[0] // 2, out_wa.shape[1]
    parts = [dot_rows(win_a[:, lanes_at(dx, fine.tiles)], grad) for dx in range(3)]
    whole = jnp.concatenate(parts, axis=0)
    acc_a[:half, :width] = whole[:half]
    acc_a[:half, width:] = whole[half:]
    acc_a[half : half + 8, :width] = dot_rows(jnp.ones((8, grad.shape[1]), bf16), grad)
    sum_a.start()
    sum_b.between()
    halos["ga"].wait()
    sum_b.last()
    sum_a.middle()
    halos["ga"].fine_windows(grad_a, strips["ga"], win_ga)

    def backward_a(g, carry):
        total = dot(in_a[0], win_ga[:, lanes_at(g * many, many)])
        for dx in (1, 2):
            total = total + dot(in_a[dx], win_ga[:, lanes_at(g * many + dx, many)])
        for i in range(many):
            tile = total[:, i * LANES : (i + 1) * LANES].astype(bf16).astype(jnp.float32)
            rows_out[pl.ds(g * many + i, c1, stride=PITCH), :] = tile
        return carry

    lax.fori_loop(0, coarse.tiles, backward_a, 0)
    sum_a.last()
    feats.unpack(feat)
    for y in range(coarse.ny):
        rows_cot[pl.ds(y, c3, stride=coarse.ny), :] = dot_rows(feat[...], order[y * LANES : (y + 1) * LANES])
    features[...] = rows_cot[...].reshape(features.shape).astype(bf16)
    turn_out(rows_out, grad_in)
    sum_b.finish()
    all_a, all_b = r("sum_a4"), r("sum_b4")
    scale_a, scale_b = scales
    flat_b = all_b[...].astype(jnp.float32).reshape(-1, all_b.shape[2]) * scale_b
    out_wb[...] = flat_b[:top_b]
    out_bb[...] = flat_b[top_b : top_b + 1]
    sum_a.finish()
    flat_a = all_a[...].astype(jnp.float32).reshape(-1, all_a.shape[2]) * scale_a
    out_wa[:half] = flat_a[:half, :width]
    out_wa[half:] = flat_a[:half, width:]
    out_ba[...] = flat_a[half : half + 1, :width]


def on_device(volume, weight_a, bias_a, weight_b, bias_b, cotangent):
    f32, bf16 = jnp.float32, jnp.bfloat16
    members, levels = lax.axis_size("gx") * lax.axis_size("gy"), lax.axis_size("gz")
    c1, nx, ny, nz = volume.shape
    c2, c3 = weight_b.shape[3:]
    cells = nx * ny * nz
    fewer = cells // 8
    scale_a = 1.0 / math.sqrt(cells * members * levels)
    scale_b = 1.0 / math.sqrt(cells * members * levels // 8)
    fine_size, coarse_size = (nx, ny, nz), (nx // 2, ny // 2, nz // 2)
    fine, coarse = Grid(*fine_size), Grid(*coarse_size)
    rows_a = 27 * c1 // 2 + 16
    rows_a += -rows_a % (16 * members)
    rows_b = 27 * c2 + 16
    rows_b += -rows_b % (8 * members * levels)
    operands = {
        "volume_hbm": jnp.transpose(volume, (0, 2, 3, 1)).reshape(c1, ny * nz, nx),
        "w_a_hbm": weight_a.reshape(27 * c1, c2),
        "b_a": bias_a.reshape(1, c2),
        "w_b_hbm": weight_b.reshape(27 * c2, c3),
        "b_b": bias_b.reshape(1, c3),
        "cot_hbm": cotangent.reshape(c3, ny // 2, nz // 2 * levels),
    }
    outs = {
        "features": ((c3, ny // 2, nz // 2 * levels), bf16),
        "grad_in": ((c1, ny * nz, nx), bf16),
        "out_wa": ((27 * c1, c2), f32),
        "out_ba": ((1, c2), f32),
        "out_wb": ((27 * c2, c3), f32),
        "out_bb": ((1, c3), f32),
    }
    scratch, local = {}, {}
    for name, grid, c in (("a", fine, c1), ("b", coarse, c2), ("gb", coarse, c3), ("ga", fine, c2)):
        for end in ("s", "r"):
            scratch[f"{name}_z{end}"] = pltpu.VMEM((2, c, grid.zpacks * LANES), bf16)
            scratch[f"{name}_y{end}"] = pltpu.VMEM((2, c, grid.ypacks * LANES), bf16)
            scratch[f"{name}_c{end}"] = pltpu.VMEM((4, c // grid.corner_groups(c), LANES), bf16)
        scratch[f"{name}_xs"] = pltpu.VMEM((c // grid.fold, LANES), bf16)
        scratch[f"{name}_xr"] = pltpu.VMEM((3, c // grid.fold, LANES), bf16)
        scratch[f"{name}_ds"] = pltpu.VMEM((2, 16, LANES), bf16)
        scratch[f"{name}_dr"] = pltpu.VMEM((2, 3, 16, LANES), bf16)
        local[f"{name}_strips"] = pltpu.VMEM((6, c, grid.ypacks * LANES), bf16)
        shape = (9 * c, (grid.tiles + 2) * LANES) if grid is fine else (27 * c, grid.tiles * LANES)
        local[f"{name}_win"] = pltpu.VMEM(shape, bf16)
    local["field"] = pltpu.VMEM((c1, cells), bf16)
    local["rows_in"] = local["rows_out"] = pltpu.VMEM((c1 * PITCH, ny * nz), f32)
    local["rows_cot"] = pltpu.VMEM((c3 * ny // 2, nz // 2 * levels), f32)
    local["before_a"] = pltpu.VMEM((c2, cells), f32)
    local["pooled"] = pltpu.VMEM((c2, fewer), bf16)
    local["grad_b"] = pltpu.VMEM((c3, fewer), bf16)
    local["grad_a"] = pltpu.VMEM((c2, cells), bf16)
    local["mixed"] = pltpu.VMEM((c3, fewer), bf16)
    local["feat"] = pltpu.VMEM((c3, fewer), bf16)
    for name, rows in (("a", rows_a), ("b", rows_b)):
        chunk = rows // members
        scratch[f"acc_{name}"] = pltpu.VMEM((rows, LANES), f32)
        shapes = [(members, chunk), (members, chunk), (chunk,), (levels, chunk), (members, chunk)]
        if name == "b":
            shapes[2:4] = [(levels, chunk // levels)] * 2
            shapes.append((levels, chunk // levels))
        for i, shape in enumerate(shapes):
            scratch[f"sum_{name}{i}"] = pltpu.VMEM((*shape, LANES), bf16)
    for name in ("cot_sent", "cot_came", "feat_sent", "feat_came"):
        scratch[name] = pltpu.VMEM((levels, c3 // coarse.fold, LANES), bf16)
    local["to_a"] = pltpu.VMEM((3, c2, 9 * c1), bf16)
    local["from_a"] = pltpu.VMEM((3, c1, 9 * c2), bf16)
    local["to_b"] = pltpu.VMEM((c3, 27 * c2), bf16)
    local["from_b"] = pltpu.VMEM((c2, 27 * c3), bf16)
    local["spread"] = pltpu.VMEM((LANES, coarse.fold * LANES), bf16)
    local["thin"] = pltpu.VMEM((LANES, coarse.fold * LANES), bf16)
    local["order"] = pltpu.VMEM((fewer, fewer), bf16)
    for name in ("volume", "cot", "w_a", "w_b"):
        local[name] = pltpu.VMEM(operands[name + "_hbm"].shape, bf16)
    scratch["load_sems"] = pltpu.SemaphoreType.DMA((4,))
    scratch["halo_sems"] = pltpu.SemaphoreType.DMA((2, 4, 17))
    scratch["sum_sems"] = pltpu.SemaphoreType.DMA((2, 4, 2, max(members, levels)))
    scratch["slab_sems"] = pltpu.SemaphoreType.DMA((2, 2, levels))
    names = (*operands, *outs, *scratch)
    got = pl.pallas_call(
        functools.partial(whole_kernel, (fine_size, coarse_size, (scale_a, scale_b), names, local)),
        out_shape=[jax.ShapeDtypeStruct(shape, dtype) for shape, dtype in outs.values()],
        in_specs=[
            pl.BlockSpec(memory_space=pl.ANY if name.endswith("_hbm") else pltpu.VMEM) for name in operands
        ],
        out_specs=[pl.BlockSpec(memory_space=pltpu.VMEM)] * len(outs),
        scratch_shapes=list(scratch.values()),
        compiler_params=pltpu.CompilerParams(
            collective_id=1, has_side_effects=True, vmem_limit_bytes=60 * 2**20
        ),
    )(*operands.values())
    features, grad_in, sum_wa, sum_ba, sum_wb, sum_bb = got
    return (
        features.reshape(cotangent.shape),
        jnp.transpose(grad_in.reshape(c1, ny, nz, nx), (0, 3, 1, 2)),
        sum_wa.reshape(weight_a.shape),
        sum_ba.reshape(c2),
        sum_wb.reshape(weight_b.shape),
        sum_bb.reshape(c3),
    )


def solution(mesh):
    return jax.shard_map(
        on_device,
        mesh=mesh,
        in_specs=(P(None, "gx", "gy", "gz"), P(), P(), P(), P(), P(None, ("gx", "gz"), "gy", None)),
        out_specs=(
            P(None, ("gx", "gz"), "gy", None),
            P(None, "gx", "gy", "gz"),
            P(),
            P(),
            P(),
            P(),
        ),
        check_vma=False,
    )
```

```python
import functools
import math

import jax
import jax.numpy as jnp
from jax import lax
from jax.experimental import pallas as pl
from jax.experimental.pallas import tpu as pltpu
from jax.sharding import PartitionSpec as P

MESH = pl.DeviceIdType.MESH
LANES = 128
PITCH = 40
BOTH = (0, 1)
NEAR = (-1, 0, 1)


def slope_of(value):
    sigma = jax.nn.sigmoid(value)
    return sigma + value * sigma * (1.0 - sigma)


def dot(left, right):
    return jnp.dot(left, right, preferred_element_type=jnp.float32)


def dot_rows(left, right):
    return lax.dot_general(
        left, right, (((1,), (1,)), ((), ())), preferred_element_type=jnp.float32
    )


def roll(value, by):
    by = by % LANES
    return pltpu.roll(value, by, 1) if by else value


def lanes_at(index, count=1):
    begin = index * LANES
    if not isinstance(begin, int):
        begin = pl.multiple_of(begin, LANES)
    return pl.ds(begin, count * LANES)


def within(at, count):
    return (at >= 0) & (at < count)


class Grid:
    def __init__(self, nx, ny, nz):
        self.ny, self.nz = ny, nz
        self.plane = ny * nz
        self.fold = LANES // self.plane
        self.tiles = nx // self.fold
        self.zpacks = -(-self.tiles // nz)
        self.ypacks = -(-self.tiles // ny)
        self.group = max(ny, min(nz, self.tiles))

    def at(self, rows):
        lane = lax.broadcasted_iota(jnp.int32, (rows, LANES), 1)
        return lane // self.plane, lane // self.nz % self.ny, lane % self.nz

    def corner_groups(self, channels):
        return min(channels // 16, self.nz // self.ypacks)


class Exchange:
    def __init__(self, grid, channels, buffers, sems, at):
        self.grid, self.channels = grid, channels
        self.zs, self.zr, self.ys, self.yr, self.cs, self.cr, self.xs, self.xr, self.ds, self.dr = buffers
        self.gx, self.gy, self.gz = [lax.axis_index(axis) for axis in ("gx", "gy", "gz")]
        cuts_y, cuts_z = lax.axis_size("gy"), lax.axis_size("gz")
        moves = []
        step = (1, -1)
        for side in BOTH:
            moves.append((self.ys.at[side], self.yr.at[side], 0, step[side], 0))
        for dy in NEAR:
            for dz in NEAR:
                source = self.ds.at[(1 - dy) // 2] if dy else self.xs
                target = self.dr.at[(1 - dy) // 2, 1 - dz] if dy else self.xr.at[1 - dz]
                moves.append((source, target, 1, dy, dz))
        for side in BOTH:
            moves.append((self.zs.at[side], self.zr.at[side], 0, 0, step[side]))
        for sy in BOTH:
            for sz in BOTH:
                i = sy * 2 + sz
                moves.append((self.cs.at[i], self.cr.at[i], 0, step[sy], step[sz]))
        self.moves, self.targets = [], []
        for i, (source, target, across, dy, dz) in enumerate(moves):
            copy = pltpu.make_async_remote_copy(
                src_ref=source,
                dst_ref=target,
                send_sem=sems.at[0, at, i],
                recv_sem=sems.at[1, at, i],
                device_id={
                    "gx": (self.gx + across) % 2,
                    "gy": (self.gy + dy + cuts_y) % cuts_y,
                    "gz": (self.gz + dz + cuts_z) % cuts_z,
                },
                device_id_type=MESH,
            )
            goes = within(self.gy + dy, cuts_y) & within(self.gz + dz, cuts_z)
            comes = within(self.gy - dy, cuts_y) & within(self.gz - dz, cuts_z)
            self.moves.append((copy, goes, comes))
            if dy or dz:
                self.targets.append((target, comes))

    def clear(self):
        for target, comes in self.targets:

            @pl.when(jnp.logical_not(comes))
            def _(target=target):
                target[...] = jnp.zeros(target.shape, jnp.bfloat16)

    def pack(self, field):
        grid, c = self.grid, self.channels
        spot, y, z = grid.at(c)
        last_z, last_y = grid.nz - 1, grid.ny - 1
        ends = [field[:, lanes_at(t)] for t in (grid.tiles - 1, 0)]
        if grid.fold == 1:
            self.xs[...] = jnp.where(spot + self.gx == 0, *ends)
        else:
            part = c // grid.fold
            place = grid.at(part)[0]
            made = []
            for end, i in zip(ends, (grid.fold - 1, 0)):
                out = end[:part]
                out = roll(out, grid.plane * -i)
                for j in range(1, grid.fold):
                    piece = roll(end[j * part : (j + 1) * part], grid.plane * (j - i))
                    out = jnp.where(place == j, piece, out)
                made.append(out)
            self.xs[...] = jnp.where(place * 0 + self.gx == 0, *made)

        groups = c // 16
        block = lax.broadcasted_iota(jnp.int32, (16, LANES), 1) // grid.nz
        for side in BOTH:
            made = []
            for end, i in zip(ends, (grid.fold - 1, 0)):
                here = i * grid.ny + (last_y if side == 0 else 0)
                out = None
                for j in range(groups):
                    piece = roll(end[16 * j : 16 * j + 16], grid.nz * (j - here))
                    out = piece if out is None else jnp.where(block == j, piece, out)
                made.append(out)
            self.ds[side] = jnp.where(block * 0 + self.gx == 0, *made)

        def one(q, carry):
            held = [None, None]
            rows = [None, None]
            for k in range(grid.group):
                tile = field[:, lanes_at(q * grid.group + k)]
                j = k % grid.ny
                for side in BOTH:
                    piece = roll(tile, k - last_z if side == 0 else k)
                    held[side] = piece if k == 0 else jnp.where(z == k, piece, held[side])
                    piece = roll(tile, grid.nz * (j - last_y if side == 0 else j))
                    rows[side] = piece if j == 0 else jnp.where(y == j, piece, rows[side])
                    if j == last_y:
                        self.ys[side, :, lanes_at(q * (grid.group // grid.ny) + k // grid.ny)] = rows[side]
            for side in BOTH:
                self.zs[side, :, lanes_at(q)] = held[side]
            return carry

        loops = grid.tiles // grid.group
        if loops == 1:
            one(0, 0)
        else:
            lax.fori_loop(0, loops, one, 0)
        groups, packs = grid.corner_groups(c), grid.ypacks
        part = c // groups
        z = grid.at(part)[2]
        for sy in BOTH:
            for sz in BOTH:
                out = None
                for j in range(groups):
                    for p in range(packs):
                        to = packs * j + p
                        piece = self.ys[sy, j * part : (j + 1) * part, lanes_at(p)]
                        piece = roll(piece, to - (last_z if sz == 0 else 0))
                        out = piece if out is None else jnp.where(z == to, piece, out)
                self.cs[sy * 2 + sz] = out

    def start(self):
        for copy, goes, _ in self.moves:
            pl.when(goes)(copy.start)

    def wait(self):
        for copy, goes, comes in self.moves:
            pl.when(goes)(copy.wait_send)
            pl.when(comes)(copy.wait_recv)

    def shift_z(self, tile, low, high, dz, z):
        if dz == 0:
            return tile
        if dz < 0:
            return jnp.where(z == 0, low, roll(tile, 1))
        return jnp.where(z == self.grid.nz - 1, high, roll(tile, -1))

    def shift_y(self, tile, low, high, dy, y):
        if dy == 0:
            return tile
        if dy < 0:
            return jnp.where(y == 0, low, roll(tile, self.grid.nz))
        return jnp.where(y == self.grid.ny - 1, high, roll(tile, -self.grid.nz))

    def beyond(self):
        grid, c = self.grid, self.channels
        _, y, z = grid.at(c)
        last = grid.fold - 1
        if grid.fold == 1:
            came = [self.xr[i] for i in range(3)]
        else:
            came = [
                jnp.concatenate([roll(self.xr[i], grid.plane * (last - j)) for j in range(grid.fold)], axis=0)
                for i in range(3)
            ]
        over = []
        for side in BOTH:
            to = last * grid.ny + (0 if side == 0 else grid.ny - 1)
            over.append(
                [
                    jnp.concatenate(
                        [roll(self.dr[side, i], grid.nz * (to - j)) for j in range(c // 16)], axis=0
                    )
                    for i in range(3)
                ]
            )
        rows = []
        for low, here, high in (over[0], came, over[1]):
            low, high = roll(low, 1 - grid.nz), roll(high, grid.nz - 1)
            rows.append([self.shift_z(here, low, high, dz, z) for dz in NEAR])
        return [
            self.shift_y(rows[1][dz], rows[0][dz], rows[2][dz], dy, y) for dy in NEAR for dz in range(3)
        ]

    def strips(self, shifted):
        grid, c = self.grid, self.channels
        groups, packs = grid.corner_groups(c), grid.ypacks
        _, _, z = grid.at(c)
        for side in BOTH:
            for p in range(packs):
                tile = self.yr[side, :, lanes_at(p)]
                ends = []
                for sz in BOTH:
                    to = 0 if sz == 0 else grid.nz - 1
                    corner = self.cr[side * 2 + sz]
                    ends.append(
                        jnp.concatenate([roll(corner, to - packs * j - p) for j in range(groups)], axis=0)
                    )
                for dz in NEAR:
                    shifted[side * 3 + dz + 1, :, lanes_at(p)] = self.shift_z(tile, *ends, dz, z)

    def tile_shifts(self, field, shifted, q, k):
        grid, c = self.grid, self.channels
        _, y, z = grid.at(c)
        last_z, last_y = grid.nz - 1, grid.ny - 1
        tile = field[:, lanes_at(q * grid.group + k)]
        low = roll(self.zr[0, :, lanes_at(q)], -k)
        high = roll(self.zr[1, :, lanes_at(q)], last_z - k)
        moved = [self.shift_z(tile, low, high, dz, z) for dz in NEAR]
        p, j = q * (grid.group // grid.ny) + k // grid.ny, k % grid.ny
        out = []
        for dy in NEAR:
            for dz in range(3):
                low = high = None
                if dy < 0:
                    low = roll(shifted[dz, :, lanes_at(p)], -grid.nz * j)
                if dy > 0:
                    high = roll(shifted[3 + dz, :, lanes_at(p)], grid.nz * (last_y - j))
                out.append(self.shift_y(moved[dz], low, high, dy, y))
        return out

    def only(self, value, side):
        flag = lax.broadcasted_iota(jnp.int32, value.shape, 1) * 0 + self.gx
        return jnp.where(flag == side, value, jnp.zeros_like(value))

    def fine_windows(self, field, shifted, windows):
        grid, c = self.grid, self.channels
        self.strips(shifted)
        for i, value in enumerate(self.beyond()):
            windows[i * c : (i + 1) * c, lanes_at(0)] = self.only(value, 1)
            windows[i * c : (i + 1) * c, lanes_at(grid.tiles + 1)] = self.only(value, 0)

        def one(q, carry):
            for k in range(grid.group):
                for i, value in enumerate(self.tile_shifts(field, shifted, q, k)):
                    windows[i * c : (i + 1) * c, lanes_at(q * grid.group + k + 1)] = value
            return carry

        lax.fori_loop(0, grid.tiles // grid.group, one, 0)

    def coarse_windows(self, field, shifted, windows):
        grid, c = self.grid, self.channels
        spot = grid.at(c)[0]
        self.strips(shifted)
        outer = self.beyond()
        tiles = [self.tile_shifts(field, shifted, 0, k) for k in range(grid.tiles)]
        for i in range(9):
            low = roll(self.only(outer[i], 1), grid.plane)
            high = self.only(outer[i], 0)
            rows = [slice((dx * 9 + i) * c, (dx * 9 + i + 1) * c) for dx in range(3)]
            up = [roll(tile[i], grid.plane) for tile in tiles]
            down = [roll(tile[i], -grid.plane) for tile in tiles]
            for t in range(grid.tiles):
                before = up[t - 1] if t else low
                after = down[t + 1] if t + 1 < grid.tiles else high
                windows[rows[0], lanes_at(t)] = jnp.where(spot == 0, before, up[t])
                windows[rows[1], lanes_at(t)] = tiles[t][i]
                windows[rows[2], lanes_at(t)] = jnp.where(spot == grid.fold - 1, after, down[t])


def ring(step, count):
    return min(step, count - step)


def far_first(count, hops):
    return sorted(range(1, count), key=hops, reverse=True)


def across_at(k):
    gx, gy = lax.axis_size("gx"), lax.axis_size("gy")
    high, low = gy // 4, 4
    row = lax.axis_index("gy")
    x = (row // low * gx + lax.axis_index("gx") + k // low) % (gx * high)
    return x % gx, x // gx * low + (row + k) % low


class Summing:
    def __init__(self, acc, stage, first, mine, second, whole, third, sems):
        self.acc, self.stage, self.first = acc, stage, first
        self.mine, self.second, self.whole, self.third = mine, second, whole, third
        self.sems = sems
        gy = lax.axis_size("gy")
        self.count = lax.axis_size("gx") * gy
        self.depth = lax.axis_size("gz")
        self.me = lax.axis_index("gx") * gy + lax.axis_index("gy")
        self.level = lax.axis_index("gz")

    def copy(self, phase, k, source, target, device):
        return pltpu.make_async_remote_copy(
            src_ref=source,
            dst_ref=target,
            send_sem=self.sems.at[phase, 0, k],
            recv_sem=self.sems.at[phase, 1, k],
            device_id=device,
            device_id_type=MESH,
        )

    def across(self, phase, source, target):
        gy, out = lax.axis_size("gy"), []
        for k in far_first(self.count, lambda k: ring(k // 4, self.count // 4) + ring(k % 4, 4)):
            gx, row = across_at(k)
            to = gx * gy + row
            out.append(self.copy(phase, k, source(to), target, {"gx": gx, "gy": row}))
        return out

    def along(self, phase, source, target):
        out = []
        for k in far_first(self.depth, lambda k: ring(k, self.depth)):
            to = (self.level + k) % self.depth
            out.append(self.copy(phase, k, source(to), target, {"gz": to}))
        return out

    def scatters(self):
        return self.across(0, lambda to: self.stage.at[to], self.first.at[self.me])

    def alongs(self):
        source = (lambda to: self.mine) if self.third is None else (lambda to: self.mine.at[to])
        return self.along(1, source, self.second.at[self.level])

    def returns(self):
        here = self.third.at[self.level]
        return self.along(3, lambda to: here, here)

    def gathers(self):
        here = self.whole.at[self.me]
        return self.across(2, lambda to: here, here)

    def start(self):
        chunk = self.stage.shape[1]
        for i in range(self.count):
            self.stage[i] = self.acc[i * chunk : (i + 1) * chunk].astype(jnp.bfloat16)
        for copy in self.scatters():
            copy.start()
        self.first[self.me] = self.stage[self.me]

    def total(self, parts):
        total = parts[0].astype(jnp.float32)
        for i in range(1, parts.shape[0]):
            total = total + parts[i].astype(jnp.float32)
        return total

    def middle(self):
        for copy in self.scatters():
            copy.wait()
        self.mine[...] = self.total(self.first).reshape(self.mine.shape).astype(jnp.bfloat16)
        for copy in self.alongs():
            copy.start()
        self.second[self.level] = self.mine[...] if self.third is None else self.mine[self.level]

    def between(self):
        for copy in self.alongs():
            copy.wait()
        self.third[self.level] = self.total(self.second).astype(jnp.bfloat16)
        for copy in self.returns():
            copy.start()

    def last(self):
        if self.third is None:
            for copy in self.alongs():
                copy.wait()
            total = self.total(self.second)
        else:
            for copy in self.returns():
                copy.wait()
            total = self.third[...].astype(jnp.float32).reshape(self.whole.shape[1:])
        self.whole[self.me] = total.astype(jnp.bfloat16)
        for copy in self.gathers():
            copy.start()

    def finish(self):
        for copy in self.gathers():
            copy.wait()


class Slabs:
    def __init__(self, sent, came, sems, grid):
        self.sent, self.came, self.sems, self.grid = sent, came, sems, grid
        self.depth, self.level = lax.axis_size("gz"), lax.axis_index("gz")

    def copies(self):
        out = []
        for k in far_first(self.depth, lambda k: ring(k, self.depth)):
            to = (self.level + k) % self.depth
            out.append(
                pltpu.make_async_remote_copy(
                    src_ref=self.sent.at[to],
                    dst_ref=self.came.at[self.level],
                    send_sem=self.sems.at[0, k],
                    recv_sem=self.sems.at[1, k],
                    device_id={"gz": to},
                    device_id_type=MESH,
                )
            )
        return out

    def pack(self, field):
        fold, plane = self.grid.fold, self.grid.plane
        part = self.sent.shape[1]
        spot = self.grid.at(part)[0]
        for t in range(self.grid.tiles):
            for i in range(fold):
                out = None
                for j in range(fold):
                    piece = roll(field[j * part : (j + 1) * part, lanes_at(t)], plane * (j - i))
                    out = piece if out is None else jnp.where(spot == j, piece, out)
                self.sent[t * fold + i] = out
        for copy in self.copies():
            copy.start()
        self.came[self.level] = self.sent[self.level]

    def unpack(self, field):
        for copy in self.copies():
            copy.wait()
        fold, plane = self.grid.fold, self.grid.plane
        part = self.came.shape[1]
        spot = self.grid.at(part)[0]
        for t in range(self.grid.tiles):
            for j in range(fold):
                out = None
                for i in range(fold):
                    piece = roll(self.came[t * fold + i], plane * (i - j))
                    out = piece if out is None else jnp.where(spot == i, piece, out)
                field[j * part : (j + 1) * part, lanes_at(t)] = out


def greet():
    gx, gy, gz = [lax.axis_size(axis) for axis in ("gx", "gy", "gz")]
    me = lax.axis_index("gx") * gy + lax.axis_index("gy")
    level, row, half = lax.axis_index("gz"), lax.axis_index("gy"), lax.axis_index("gx")
    barrier = pltpu.get_barrier_semaphore()
    signal = lambda device: pl.semaphore_signal(barrier, inc=1, device_id=device, device_id_type=MESH)
    for k in range(1, gx * gy):
        to = (me + k) % (gx * gy)
        signal({"gx": to // gy, "gy": to % gy})
    for k in range(1, gz):
        signal({"gz": (level + k) % gz})
    extra = 0
    for across in BOTH:
        for dy in NEAR:
            for dz in NEAR:
                if dz and (across or dy):
                    extra += 1
                    signal(
                        {
                            "gx": (half + across) % gx,
                            "gy": (row + dy + gy) % gy,
                            "gz": (level + dz + gz) % gz,
                        }
                    )
    return barrier, gx * gy + gz - 2 + extra


def spread_map(fine, coarse):
    shape = (LANES, coarse.fold * LANES)
    small = lax.broadcasted_iota(jnp.int32, shape, 0)
    large = lax.broadcasted_iota(jnp.int32, shape, 1)
    y, z = large % LANES // fine.nz, large % fine.nz
    match = (
        (small // coarse.plane == large // LANES)
        & (small // coarse.nz % coarse.ny == y // 2)
        & (small % coarse.nz == z // 2)
    )
    ones = match.astype(jnp.float32)
    first = (match & (y % 2 == 0) & (z % 2 == 0)).astype(jnp.float32)
    return ones.astype(jnp.bfloat16), first.astype(jnp.bfloat16)


def order_map(coarse, count):
    shape = (coarse.plane * count,) * 2
    row = lax.broadcasted_iota(jnp.int32, shape, 0)
    column = lax.broadcasted_iota(jnp.int32, shape, 1)
    wide = count * coarse.nz
    match = (
        (row // wide == column // coarse.nz % coarse.ny)
        & (row % wide // coarse.nz == column // coarse.plane)
        & (row % coarse.nz == column % coarse.nz)
    )
    return match.astype(jnp.float32).astype(jnp.bfloat16)


def column_of(row):
    size = row.shape[1]
    across = lax.broadcasted_iota(jnp.int32, (size, size), 0)
    down = lax.broadcasted_iota(jnp.int32, (size, size), 1)
    return jnp.sum(jnp.where(across == down, row, 0.0), axis=1, keepdims=True)


def turn_in(volume, rows, field):
    channels, _, nx = volume.shape
    fold = LANES // nx
    for q in range(channels // fold):
        wide = jnp.concatenate([volume[q * fold + i] for i in range(fold)], axis=1)
        turned = wide.astype(jnp.float32).T
        for i in range(fold):
            begin = (q * fold + i) * PITCH
            rows[begin : begin + nx] = turned[i * nx : (i + 1) * nx]
    for x in range(nx):
        field[:, lanes_at(x)] = rows[pl.ds(x, channels, stride=PITCH), :].astype(jnp.bfloat16)


def turn_out(rows, out):
    channels, _, nx = out.shape
    fold = LANES // nx
    for q in range(channels // fold):
        begins = [(q * fold + i) * PITCH for i in range(fold)]
        wide = jnp.concatenate([rows[begin : begin + nx] for begin in begins], axis=0)
        turned = wide.T.astype(jnp.bfloat16)
        for i in range(fold):
            out[q * fold + i] = turned[:, i * nx : (i + 1) * nx]


def whole_kernel(setting, *refs):
    names, local = setting[3:]
    pl.run_scoped(lambda **held: stages(setting, dict(zip(names, refs)) | held), **local)


def stages(setting, named):
    fine_size, coarse_size, scales = setting[:3]
    fine, coarse = Grid(*fine_size), Grid(*coarse_size)
    r = lambda name: named[name]
    field = r("field")
    fields = ("a", "b", "gb", "ga")
    grids = (fine, coarse, coarse, fine)
    volume, w_a, b_a, w_b, b_b, cot = [r(n) for n in ("volume", "w_a", "b_a", "w_b", "b_b", "cot")]
    features, grad_in, out_wa, out_ba, out_wb, out_bb = [
        r(n) for n in ("features", "grad_in", "out_wa", "out_ba", "out_wb", "out_bb")
    ]
    c1, c2, c3 = field.shape[0], w_a.shape[1], w_b.shape[1]
    widths = dict(zip(fields, (c1, c2, c3, c2)))
    halos = {
        name: Exchange(
            grid,
            widths[name],
            [r(name + part) for part in ("_zs", "_zr", "_ys", "_yr", "_cs", "_cr", "_xs", "_xr", "_ds", "_dr")],
            r("halo_sems"),
            i,
        )
        for i, (name, grid) in enumerate(zip(fields, grids))
    }
    strips = {name: r(name + "_strips") for name in fields}
    win_a, win_b, win_gb, win_ga = [r(name + "_win") for name in fields]
    before_a, pooled, grad_b, grad_a = [r(n) for n in ("before_a", "pooled", "grad_b", "grad_a")]
    acc_a, acc_b, mixed, feat = [r(n) for n in ("acc_a", "acc_b", "mixed", "feat")]
    sum_a = Summing(acc_a, *[r(f"sum_a{i}") for i in range(5)], None, r("sum_sems").at[0])
    sum_b = Summing(acc_b, *[r(f"sum_b{i}") for i in range(6)], r("sum_sems").at[1])
    cots = Slabs(r("cot_sent"), r("cot_came"), r("slab_sems").at[0], coarse)
    feats = Slabs(r("feat_sent"), r("feat_came"), r("slab_sems").at[1], coarse)
    out_a, in_a, out_b, in_b, spread, thin, order = [
        r(n) for n in ("to_a", "from_a", "to_b", "from_b", "spread", "thin", "order")
    ]
    bf16 = jnp.bfloat16

    loads = {
        name: pltpu.make_async_copy(r(name + "_hbm"), r(name), r("load_sems").at[i])
        for i, name in enumerate(("volume", "cot", "w_a", "w_b"))
    }
    stores = {
        name: pltpu.make_async_copy(r(name), r(name + "_out"), r("load_sems").at[4 + i])
        for i, name in enumerate(("features", "grad_in"))
    }
    for load in loads.values():
        load.start()
    barrier, arrivals = greet()
    halos["a"].clear()
    rows_in, rows_out = r("rows_in"), r("rows_out")
    loads["volume"].wait()
    turn_in(volume, rows_in, field)
    halos["a"].pack(field)
    pl.semaphore_wait(barrier, arrivals)
    halos["a"].start()
    order[...] = order_map(coarse, lax.axis_size("gz"))
    rows_cot = r("rows_cot")
    loads["cot"].wait()
    rows_cot[...] = cot[...].astype(jnp.float32).reshape(rows_cot.shape)
    total = None
    for y in range(coarse.ny):
        row = rows_cot[pl.ds(y, c3, stride=coarse.ny), :].astype(bf16)
        part = dot(row, order[y * LANES : (y + 1) * LANES])
        total = part if total is None else total + part
    mixed[...] = total.astype(bf16)
    cots.pack(mixed)

    loads["w_a"].wait()
    loads["w_b"].wait()
    taps = 9
    for dx in range(3):
        out_a[dx] = w_a[dx * taps * c1 : (dx + 1) * taps * c1].T
        for k in range(taps):
            tap = 26 - dx * taps - k
            in_a[dx, :, k * c2 : (k + 1) * c2] = w_a[tap * c1 : (tap + 1) * c1]
    out_b[...] = w_b[...].T
    for k in range(27):
        in_b[:, k * c3 : (k + 1) * c3] = w_b[(26 - k) * c2 : (27 - k) * c2]
    wide, narrow = spread_map(fine, coarse)
    spread[...] = wide
    thin[...] = narrow
    for name in fields[1:]:
        halos[name].clear()
    bias_a, bias_b = column_of(b_a[...]), column_of(b_b[...])
    acc_a[...] = jnp.zeros_like(acc_a)
    acc_b[...] = jnp.zeros_like(acc_b)

    halos["a"].wait()
    halos["a"].fine_windows(field, strips["a"], win_a)
    many = 2 * coarse.fold

    def forward_a(g, carry):
        before = bias_a
        for dx in range(3):
            before = before + dot(out_a[dx], win_a[:, lanes_at(g * many + dx, many)])
        before_a[:, lanes_at(g * many, many)] = before
        active = before * jax.nn.sigmoid(before)
        pieces = []
        for i in range(coarse.fold):
            first = active[:, 2 * i * LANES : (2 * i + 1) * LANES]
            pair = first + active[:, (2 * i + 1) * LANES : (2 * i + 2) * LANES]
            pair = pair + roll(pair, -1)
            pair = pair + roll(pair, -fine.nz)
            pieces.append((pair * 0.125).astype(bf16))
        pooled[:, lanes_at(g)] = dot_rows(jnp.concatenate(pieces, axis=1), thin[...]).astype(bf16)
        return carry

    lax.fori_loop(0, coarse.tiles, forward_a, 0)
    halos["b"].pack(pooled)
    halos["b"].start()
    cots.unpack(mixed)
    halos["b"].wait()
    halos["b"].coarse_windows(pooled, strips["b"], win_b)
    before = dot(out_b[...], win_b[...]) + bias_b
    grad_b[...] = (mixed[...].astype(jnp.float32) * slope_of(before)).astype(bf16)
    halos["gb"].pack(grad_b)
    halos["gb"].start()
    feat[...] = (before * jax.nn.sigmoid(before)).astype(bf16)
    feats.pack(feat)
    top_b = out_wb.shape[0]
    grad = grad_b[...]
    acc_b[:top_b] = dot_rows(win_b[...], grad)
    acc_b[top_b : top_b + 8] = dot_rows(jnp.ones((8, grad.shape[1]), bf16), grad)
    sum_b.start()
    halos["gb"].wait()
    halos["gb"].coarse_windows(grad_b, strips["gb"], win_gb)
    pooled[...] = dot(in_b[...], win_gb[...]).astype(bf16)

    def backward_b(g, carry):
        wide = dot(pooled[:, lanes_at(g)], spread[...]) * 0.125
        for i in range(coarse.fold):
            for j in BOTH:
                here = lanes_at(g * many + 2 * i + j)
                slope = slope_of(before_a[:, here])
                grad_a[:, here] = (wide[:, i * LANES : (i + 1) * LANES] * slope).astype(bf16)
        return carry

    lax.fori_loop(0, coarse.tiles, backward_b, 0)
    halos["ga"].pack(grad_a)
    halos["ga"].start()
    sum_b.middle()
    grad = grad_a[...]
    half, width = out_wa.shape[0] // 2, out_wa.shape[1]
    parts = [dot_rows(win_a[:, lanes_at(dx, fine.tiles)], grad) for dx in range(3)]
    whole = jnp.concatenate(parts, axis=0)
    acc_a[:half, :width] = whole[:half]
    acc_a[:half, width:] = whole[half:]
    acc_a[half : half + 8, :width] = dot_rows(jnp.ones((8, grad.shape[1]), bf16), grad)
    sum_a.start()
    sum_b.between()
    halos["ga"].wait()
    sum_b.last()
    sum_a.middle()
    halos["ga"].fine_windows(grad_a, strips["ga"], win_ga)

    def backward_a(g, carry):
        total = dot(in_a[0], win_ga[:, lanes_at(g * many, many)])
        for dx in (1, 2):
            total = total + dot(in_a[dx], win_ga[:, lanes_at(g * many + dx, many)])
        for i in range(many):
            tile = total[:, i * LANES : (i + 1) * LANES].astype(bf16).astype(jnp.float32)
            rows_out[pl.ds(g * many + i, c1, stride=PITCH), :] = tile
        return carry

    lax.fori_loop(0, coarse.tiles, backward_a, 0)
    sum_a.last()
    feats.unpack(feat)
    for y in range(coarse.ny):
        rows_cot[pl.ds(y, c3, stride=coarse.ny), :] = dot_rows(feat[...], order[y * LANES : (y + 1) * LANES])
    features[...] = rows_cot[...].reshape(features.shape).astype(bf16)
    stores["features"].start()
    turn_out(rows_out, grad_in)
    stores["grad_in"].start()
    sum_b.finish()
    all_a, all_b = r("sum_a4"), r("sum_b4")
    scale_a, scale_b = scales
    flat_b = all_b[...].astype(jnp.float32).reshape(-1, all_b.shape[2]) * scale_b
    out_wb[...] = flat_b[:top_b]
    out_bb[...] = flat_b[top_b : top_b + 1]
    sum_a.finish()
    flat_a = all_a[...].astype(jnp.float32).reshape(-1, all_a.shape[2]) * scale_a
    out_wa[:half] = flat_a[:half, :width]
    out_wa[half:] = flat_a[:half, width:]
    out_ba[...] = flat_a[half : half + 1, :width]
    for store in stores.values():
        store.wait()


def landing_kernel(count, *refs):
    arrived, leaving, held = [refs[i * count : (i + 1) * count] for i in range(3)]
    sems = refs[3 * count]
    into = [pltpu.make_async_copy(arrived[i], held[i], sems.at[0, i]) for i in range(count)]
    out = [pltpu.make_async_copy(held[i], leaving[i], sems.at[1, i]) for i in range(count)]
    for copy in into:
        copy.start()
    for first, second in zip(into, out):
        first.wait()
        second.start()
    for copy in out:
        copy.wait()


def landed(arrays):
    count = len(arrays)
    return pl.pallas_call(
        functools.partial(landing_kernel, count),
        out_shape=[jax.ShapeDtypeStruct(array.shape, array.dtype) for array in arrays],
        in_specs=[pl.BlockSpec(memory_space=pl.ANY)] * count,
        out_specs=[pl.BlockSpec(memory_space=pl.ANY)] * count,
        scratch_shapes=[pltpu.VMEM(array.shape, array.dtype) for array in arrays]
        + [pltpu.SemaphoreType.DMA((2, count))],
    )(*arrays)


def on_device(volume, weight_a, bias_a, weight_b, bias_b, cotangent):
    f32, bf16 = jnp.float32, jnp.bfloat16
    members, levels = lax.axis_size("gx") * lax.axis_size("gy"), lax.axis_size("gz")
    c1, nx, ny, nz = volume.shape
    c2, c3 = weight_b.shape[3:]
    cells = nx * ny * nz
    fewer = cells // 8
    scale_a = 1.0 / math.sqrt(cells * members * levels)
    scale_b = 1.0 / math.sqrt(cells * members * levels // 8)
    fine_size, coarse_size = (nx, ny, nz), (nx // 2, ny // 2, nz // 2)
    fine, coarse = Grid(*fine_size), Grid(*coarse_size)
    rows_a = 27 * c1 // 2 + 16
    rows_a += -rows_a % (16 * members)
    rows_b = 27 * c2 + 16
    rows_b += -rows_b % (8 * members * levels)
    operands = {
        "volume_hbm": jnp.transpose(volume, (0, 2, 3, 1)).reshape(c1, ny * nz, nx),
        "w_a_hbm": weight_a.reshape(27 * c1, c2),
        "b_a": bias_a.reshape(1, c2),
        "w_b_hbm": weight_b.reshape(27 * c2, c3),
        "b_b": bias_b.reshape(1, c3),
        "cot_hbm": cotangent.reshape(c3, ny // 2, nz // 2 * levels),
    }
    outs = {
        "features_out": ((c3, ny // 2, nz // 2 * levels), bf16),
        "grad_in_out": ((c1, ny * nz, nx), bf16),
        "out_wa": ((27 * c1, c2), f32),
        "out_ba": ((1, c2), f32),
        "out_wb": ((27 * c2, c3), f32),
        "out_bb": ((1, c3), f32),
    }
    scratch, local = {}, {}
    for name, grid, c in (("a", fine, c1), ("b", coarse, c2), ("gb", coarse, c3), ("ga", fine, c2)):
        for end in ("s", "r"):
            scratch[f"{name}_z{end}"] = pltpu.VMEM((2, c, grid.zpacks * LANES), bf16)
            scratch[f"{name}_y{end}"] = pltpu.VMEM((2, c, grid.ypacks * LANES), bf16)
            scratch[f"{name}_c{end}"] = pltpu.VMEM((4, c // grid.corner_groups(c), LANES), bf16)
        scratch[f"{name}_xs"] = pltpu.VMEM((c // grid.fold, LANES), bf16)
        scratch[f"{name}_xr"] = pltpu.VMEM((3, c // grid.fold, LANES), bf16)
        scratch[f"{name}_ds"] = pltpu.VMEM((2, 16, LANES), bf16)
        scratch[f"{name}_dr"] = pltpu.VMEM((2, 3, 16, LANES), bf16)
        local[f"{name}_strips"] = pltpu.VMEM((6, c, grid.ypacks * LANES), bf16)
        shape = (9 * c, (grid.tiles + 2) * LANES) if grid is fine else (27 * c, grid.tiles * LANES)
        local[f"{name}_win"] = pltpu.VMEM(shape, bf16)
    local["field"] = pltpu.VMEM((c1, cells), bf16)
    local["rows_in"] = local["rows_out"] = pltpu.VMEM((c1 * PITCH, ny * nz), f32)
    local["rows_cot"] = pltpu.VMEM((c3 * ny // 2, nz // 2 * levels), f32)
    local["before_a"] = pltpu.VMEM((c2, cells), f32)
    local["pooled"] = pltpu.VMEM((c2, fewer), bf16)
    local["grad_b"] = pltpu.VMEM((c3, fewer), bf16)
    local["grad_a"] = pltpu.VMEM((c2, cells), bf16)
    local["mixed"] = pltpu.VMEM((c3, fewer), bf16)
    local["feat"] = pltpu.VMEM((c3, fewer), bf16)
    for name, rows in (("a", rows_a), ("b", rows_b)):
        chunk = rows // members
        scratch[f"acc_{name}"] = pltpu.VMEM((rows, LANES), f32)
        shapes = [(members, chunk), (members, chunk), (chunk,), (levels, chunk), (members, chunk)]
        if name == "b":
            shapes[2:4] = [(levels, chunk // levels)] * 2
            shapes.append((levels, chunk // levels))
        for i, shape in enumerate(shapes):
            scratch[f"sum_{name}{i}"] = pltpu.VMEM((*shape, LANES), bf16)
    for name in ("cot_sent", "cot_came", "feat_sent", "feat_came"):
        scratch[name] = pltpu.VMEM((levels, c3 // coarse.fold, LANES), bf16)
    local["to_a"] = pltpu.VMEM((3, c2, 9 * c1), bf16)
    local["from_a"] = pltpu.VMEM((3, c1, 9 * c2), bf16)
    local["to_b"] = pltpu.VMEM((c3, 27 * c2), bf16)
    local["from_b"] = pltpu.VMEM((c2, 27 * c3), bf16)
    local["spread"] = pltpu.VMEM((LANES, coarse.fold * LANES), bf16)
    local["thin"] = pltpu.VMEM((LANES, coarse.fold * LANES), bf16)
    local["order"] = pltpu.VMEM((fewer, fewer), bf16)
    for name in ("volume", "cot", "w_a", "w_b"):
        local[name] = pltpu.VMEM(operands[name + "_hbm"].shape, bf16)
    for name in ("features", "grad_in"):
        local[name] = pltpu.VMEM(*outs[name + "_out"])
    scratch["load_sems"] = pltpu.SemaphoreType.DMA((6,))
    scratch["halo_sems"] = pltpu.SemaphoreType.DMA((2, 4, 17))
    scratch["sum_sems"] = pltpu.SemaphoreType.DMA((2, 4, 2, max(members, levels)))
    scratch["slab_sems"] = pltpu.SemaphoreType.DMA((2, 2, levels))
    names = (*operands, *outs, *scratch)
    got = pl.pallas_call(
        functools.partial(whole_kernel, (fine_size, coarse_size, (scale_a, scale_b), names, local)),
        out_shape=[jax.ShapeDtypeStruct(shape, dtype) for shape, dtype in outs.values()],
        in_specs=[
            pl.BlockSpec(memory_space=pl.ANY if name.endswith("_hbm") else pltpu.VMEM) for name in operands
        ],
        out_specs=[
            pl.BlockSpec(memory_space=pl.ANY if name.endswith("_out") else pltpu.VMEM) for name in outs
        ],
        scratch_shapes=list(scratch.values()),
        compiler_params=pltpu.CompilerParams(
            collective_id=1, has_side_effects=True, vmem_limit_bytes=60 * 2**20
        ),
    )(*operands.values())
    features, grad_in, sum_wa, sum_ba, sum_wb, sum_bb = landed(got)
    return (
        features.reshape(cotangent.shape),
        jnp.transpose(grad_in.reshape(c1, ny, nz, nx), (0, 3, 1, 2)),
        sum_wa.reshape(weight_a.shape),
        sum_ba.reshape(c2),
        sum_wb.reshape(weight_b.shape),
        sum_bb.reshape(c3),
    )


def solution(mesh):
    return jax.shard_map(
        on_device,
        mesh=mesh,
        in_specs=(P(None, "gx", "gy", "gz"), P(), P(), P(), P(), P(None, ("gx", "gz"), "gy", None)),
        out_specs=(
            P(None, ("gx", "gz"), "gy", None),
            P(None, "gx", "gy", "gz"),
            P(),
            P(),
            P(),
            P(),
        ),
        check_vma=False,
    )
```

```python
import functools
import math

import jax
import jax.numpy as jnp
from jax import lax
from jax.experimental import pallas as pl
from jax.experimental.pallas import tpu as pltpu
from jax.sharding import PartitionSpec as P

MESH = pl.DeviceIdType.MESH
LANES = 128
PITCH = 40
BOTH = (0, 1)
NEAR = (-1, 0, 1)


def slope_of(value):
    sigma = jax.nn.sigmoid(value)
    return sigma + value * sigma * (1.0 - sigma)


def dot(left, right):
    return jnp.dot(left, right, preferred_element_type=jnp.float32)


def dot_rows(left, right):
    return lax.dot_general(
        left, right, (((1,), (1,)), ((), ())), preferred_element_type=jnp.float32
    )


def roll(value, by):
    by = by % LANES
    return pltpu.roll(value, by, 1) if by else value


def lanes_at(index, count=1):
    begin = index * LANES
    if not isinstance(begin, int):
        begin = pl.multiple_of(begin, LANES)
    return pl.ds(begin, count * LANES)


def within(at, count):
    return (at >= 0) & (at < count)


class Grid:
    def __init__(self, nx, ny, nz):
        self.ny, self.nz = ny, nz
        self.plane = ny * nz
        self.fold = LANES // self.plane
        self.tiles = nx // self.fold
        self.zpacks = -(-self.tiles // nz)
        self.ypacks = -(-self.tiles // ny)
        self.group = max(ny, min(nz, self.tiles))

    def at(self, rows):
        lane = lax.broadcasted_iota(jnp.int32, (rows, LANES), 1)
        return lane // self.plane, lane // self.nz % self.ny, lane % self.nz

    def corner_groups(self, channels):
        return min(channels // 16, self.nz // self.ypacks)


class Exchange:
    def __init__(self, grid, channels, buffers, sems, at):
        self.grid, self.channels = grid, channels
        self.zs, self.zr, self.ys, self.yr, self.cs, self.cr, self.xs, self.xr, self.ds, self.dr = buffers
        self.gx, self.gy, self.gz = [lax.axis_index(axis) for axis in ("gx", "gy", "gz")]
        cuts_y, cuts_z = lax.axis_size("gy"), lax.axis_size("gz")
        moves = []
        step = (1, -1)
        for side in BOTH:
            moves.append((self.ys.at[side], self.yr.at[side], 0, step[side], 0))
        for dy in NEAR:
            for dz in NEAR:
                source = self.ds.at[(1 - dy) // 2] if dy else self.xs
                target = self.dr.at[(1 - dy) // 2, 1 - dz] if dy else self.xr.at[1 - dz]
                moves.append((source, target, 1, dy, dz))
        for side in BOTH:
            moves.append((self.zs.at[side], self.zr.at[side], 0, 0, step[side]))
        for sy in BOTH:
            for sz in BOTH:
                i = sy * 2 + sz
                moves.append((self.cs.at[i], self.cr.at[i], 0, step[sy], step[sz]))
        self.moves, self.targets = [], []
        for i, (source, target, across, dy, dz) in enumerate(moves):
            copy = pltpu.make_async_remote_copy(
                src_ref=source,
                dst_ref=target,
                send_sem=sems.at[0, at, i],
                recv_sem=sems.at[1, at, i],
                device_id={
                    "gx": (self.gx + across) % 2,
                    "gy": (self.gy + dy + cuts_y) % cuts_y,
                    "gz": (self.gz + dz + cuts_z) % cuts_z,
                },
                device_id_type=MESH,
            )
            goes = within(self.gy + dy, cuts_y) & within(self.gz + dz, cuts_z)
            comes = within(self.gy - dy, cuts_y) & within(self.gz - dz, cuts_z)
            self.moves.append((copy, goes, comes))
            if dy or dz:
                self.targets.append((target, comes))

    def clear(self):
        for target, comes in self.targets:

            @pl.when(jnp.logical_not(comes))
            def _(target=target):
                target[...] = jnp.zeros(target.shape, jnp.bfloat16)

    def pack(self, field):
        grid, c = self.grid, self.channels
        spot, y, z = grid.at(c)
        last_z, last_y = grid.nz - 1, grid.ny - 1
        ends = [field[:, lanes_at(t)] for t in (grid.tiles - 1, 0)]
        if grid.fold == 1:
            self.xs[...] = jnp.where(spot + self.gx == 0, *ends)
        else:
            part = c // grid.fold
            place = grid.at(part)[0]
            made = []
            for end, i in zip(ends, (grid.fold - 1, 0)):
                out = end[:part]
                out = roll(out, grid.plane * -i)
                for j in range(1, grid.fold):
                    piece = roll(end[j * part : (j + 1) * part], grid.plane * (j - i))
                    out = jnp.where(place == j, piece, out)
                made.append(out)
            self.xs[...] = jnp.where(place * 0 + self.gx == 0, *made)

        groups = c // 16
        block = lax.broadcasted_iota(jnp.int32, (16, LANES), 1) // grid.nz
        for side in BOTH:
            made = []
            for end, i in zip(ends, (grid.fold - 1, 0)):
                here = i * grid.ny + (last_y if side == 0 else 0)
                out = None
                for j in range(groups):
                    piece = roll(end[16 * j : 16 * j + 16], grid.nz * (j - here))
                    out = piece if out is None else jnp.where(block == j, piece, out)
                made.append(out)
            self.ds[side] = jnp.where(block * 0 + self.gx == 0, *made)

        def one(q, carry):
            held = [None, None]
            rows = [None, None]
            for k in range(grid.group):
                tile = field[:, lanes_at(q * grid.group + k)]
                j = k % grid.ny
                for side in BOTH:
                    piece = roll(tile, k - last_z if side == 0 else k)
                    held[side] = piece if k == 0 else jnp.where(z == k, piece, held[side])
                    piece = roll(tile, grid.nz * (j - last_y if side == 0 else j))
                    rows[side] = piece if j == 0 else jnp.where(y == j, piece, rows[side])
                    if j == last_y:
                        self.ys[side, :, lanes_at(q * (grid.group // grid.ny) + k // grid.ny)] = rows[side]
            for side in BOTH:
                self.zs[side, :, lanes_at(q)] = held[side]
            return carry

        loops = grid.tiles // grid.group
        if loops == 1:
            one(0, 0)
        else:
            lax.fori_loop(0, loops, one, 0)
        groups, packs = grid.corner_groups(c), grid.ypacks
        part = c // groups
        z = grid.at(part)[2]
        for sy in BOTH:
            for sz in BOTH:
                out = None
                for j in range(groups):
                    for p in range(packs):
                        to = packs * j + p
                        piece = self.ys[sy, j * part : (j + 1) * part, lanes_at(p)]
                        piece = roll(piece, to - (last_z if sz == 0 else 0))
                        out = piece if out is None else jnp.where(z == to, piece, out)
                self.cs[sy * 2 + sz] = out

    def start(self):
        for copy, goes, _ in self.moves:
            pl.when(goes)(copy.start)

    def wait(self):
        for copy, goes, comes in self.moves:
            pl.when(goes)(copy.wait_send)
            pl.when(comes)(copy.wait_recv)

    def shift_z(self, tile, low, high, dz, z):
        if dz == 0:
            return tile
        if dz < 0:
            return jnp.where(z == 0, low, roll(tile, 1))
        return jnp.where(z == self.grid.nz - 1, high, roll(tile, -1))

    def shift_y(self, tile, low, high, dy, y):
        if dy == 0:
            return tile
        if dy < 0:
            return jnp.where(y == 0, low, roll(tile, self.grid.nz))
        return jnp.where(y == self.grid.ny - 1, high, roll(tile, -self.grid.nz))

    def beyond(self):
        grid, c = self.grid, self.channels
        _, y, z = grid.at(c)
        last = grid.fold - 1
        if grid.fold == 1:
            came = [self.xr[i] for i in range(3)]
        else:
            came = [
                jnp.concatenate([roll(self.xr[i], grid.plane * (last - j)) for j in range(grid.fold)], axis=0)
                for i in range(3)
            ]
        over = []
        for side in BOTH:
            to = last * grid.ny + (0 if side == 0 else grid.ny - 1)
            over.append(
                [
                    jnp.concatenate(
                        [roll(self.dr[side, i], grid.nz * (to - j)) for j in range(c // 16)], axis=0
                    )
                    for i in range(3)
                ]
            )
        rows = []
        for low, here, high in (over[0], came, over[1]):
            low, high = roll(low, 1 - grid.nz), roll(high, grid.nz - 1)
            rows.append([self.shift_z(here, low, high, dz, z) for dz in NEAR])
        return [
            self.shift_y(rows[1][dz], rows[0][dz], rows[2][dz], dy, y) for dy in NEAR for dz in range(3)
        ]

    def strips(self, shifted):
        grid, c = self.grid, self.channels
        groups, packs = grid.corner_groups(c), grid.ypacks
        _, _, z = grid.at(c)
        for side in BOTH:
            for p in range(packs):
                tile = self.yr[side, :, lanes_at(p)]
                ends = []
                for sz in BOTH:
                    to = 0 if sz == 0 else grid.nz - 1
                    corner = self.cr[side * 2 + sz]
                    ends.append(
                        jnp.concatenate([roll(corner, to - packs * j - p) for j in range(groups)], axis=0)
                    )
                for dz in NEAR:
                    shifted[side * 3 + dz + 1, :, lanes_at(p)] = self.shift_z(tile, *ends, dz, z)

    def tile_shifts(self, field, shifted, q, k):
        grid, c = self.grid, self.channels
        _, y, z = grid.at(c)
        last_z, last_y = grid.nz - 1, grid.ny - 1
        tile = field[:, lanes_at(q * grid.group + k)]
        low = roll(self.zr[0, :, lanes_at(q)], -k)
        high = roll(self.zr[1, :, lanes_at(q)], last_z - k)
        moved = [self.shift_z(tile, low, high, dz, z) for dz in NEAR]
        p, j = q * (grid.group // grid.ny) + k // grid.ny, k % grid.ny
        out = []
        for dy in NEAR:
            for dz in range(3):
                low = high = None
                if dy < 0:
                    low = roll(shifted[dz, :, lanes_at(p)], -grid.nz * j)
                if dy > 0:
                    high = roll(shifted[3 + dz, :, lanes_at(p)], grid.nz * (last_y - j))
                out.append(self.shift_y(moved[dz], low, high, dy, y))
        return out

    def only(self, value, side):
        flag = lax.broadcasted_iota(jnp.int32, value.shape, 1) * 0 + self.gx
        return jnp.where(flag == side, value, jnp.zeros_like(value))

    def fine_windows(self, field, shifted, windows):
        grid, c = self.grid, self.channels
        self.strips(shifted)
        for i, value in enumerate(self.beyond()):
            windows[i * c : (i + 1) * c, lanes_at(0)] = self.only(value, 1)
            windows[i * c : (i + 1) * c, lanes_at(grid.tiles + 1)] = self.only(value, 0)

        def one(q, carry):
            for k in range(grid.group):
                for i, value in enumerate(self.tile_shifts(field, shifted, q, k)):
                    windows[i * c : (i + 1) * c, lanes_at(q * grid.group + k + 1)] = value
            return carry

        lax.fori_loop(0, grid.tiles // grid.group, one, 0)

    def coarse_windows(self, field, shifted, windows):
        grid, c = self.grid, self.channels
        spot = grid.at(c)[0]
        self.strips(shifted)
        outer = self.beyond()
        tiles = [self.tile_shifts(field, shifted, 0, k) for k in range(grid.tiles)]
        for i in range(9):
            low = roll(self.only(outer[i], 1), grid.plane)
            high = self.only(outer[i], 0)
            rows = [slice((dx * 9 + i) * c, (dx * 9 + i + 1) * c) for dx in range(3)]
            up = [roll(tile[i], grid.plane) for tile in tiles]
            down = [roll(tile[i], -grid.plane) for tile in tiles]
            for t in range(grid.tiles):
                before = up[t - 1] if t else low
                after = down[t + 1] if t + 1 < grid.tiles else high
                windows[rows[0], lanes_at(t)] = jnp.where(spot == 0, before, up[t])
                windows[rows[1], lanes_at(t)] = tiles[t][i]
                windows[rows[2], lanes_at(t)] = jnp.where(spot == grid.fold - 1, after, down[t])


def ring(step, count):
    return min(step, count - step)


def far_first(count, hops):
    return sorted(range(1, count), key=hops, reverse=True)


def across_at(k):
    gx, gy = lax.axis_size("gx"), lax.axis_size("gy")
    high, low = gy // 4, 4
    row = lax.axis_index("gy")
    x = (row // low * gx + lax.axis_index("gx") + k // low) % (gx * high)
    return x % gx, x // gx * low + (row + k) % low


class Summing:
    def __init__(self, acc, stage, first, mine, second, whole, third, sems):
        self.acc, self.stage, self.first = acc, stage, first
        self.mine, self.second, self.whole, self.third = mine, second, whole, third
        self.sems = sems
        gy = lax.axis_size("gy")
        self.count = lax.axis_size("gx") * gy
        self.depth = lax.axis_size("gz")
        self.me = lax.axis_index("gx") * gy + lax.axis_index("gy")
        self.level = lax.axis_index("gz")

    def copy(self, phase, k, source, target, device):
        return pltpu.make_async_remote_copy(
            src_ref=source,
            dst_ref=target,
            send_sem=self.sems.at[phase, 0, k],
            recv_sem=self.sems.at[phase, 1, k],
            device_id=device,
            device_id_type=MESH,
        )

    def across(self, phase, source, target):
        gy, out = lax.axis_size("gy"), []
        for k in far_first(self.count, lambda k: ring(k // 4, self.count // 4) + ring(k % 4, 4)):
            gx, row = across_at(k)
            to = gx * gy + row
            out.append(self.copy(phase, k, source(to), target, {"gx": gx, "gy": row}))
        return out

    def along(self, phase, source, target):
        out = []
        for k in far_first(self.depth, lambda k: ring(k, self.depth)):
            to = (self.level + k) % self.depth
            out.append(self.copy(phase, k, source(to), target, {"gz": to}))
        return out

    def scatters(self):
        return self.across(0, lambda to: self.stage.at[to], self.first.at[self.me])

    def alongs(self):
        source = (lambda to: self.mine) if self.third is None else (lambda to: self.mine.at[to])
        return self.along(1, source, self.second.at[self.level])

    def returns(self):
        here = self.third.at[self.level]
        return self.along(3, lambda to: here, here)

    def gathers(self):
        here = self.whole.at[self.me]
        return self.across(2, lambda to: here, here)

    def start(self):
        chunk = self.stage.shape[1]
        for i in range(self.count):
            self.stage[i] = self.acc[i * chunk : (i + 1) * chunk].astype(jnp.bfloat16)
        for copy in self.scatters():
            copy.start()
        self.first[self.me] = self.stage[self.me]

    def total(self, parts):
        total = parts[0].astype(jnp.float32)
        for i in range(1, parts.shape[0]):
            total = total + parts[i].astype(jnp.float32)
        return total

    def middle(self):
        for copy in self.scatters():
            copy.wait()
        self.mine[...] = self.total(self.first).reshape(self.mine.shape).astype(jnp.bfloat16)
        for copy in self.alongs():
            copy.start()
        self.second[self.level] = self.mine[...] if self.third is None else self.mine[self.level]

    def between(self):
        for copy in self.alongs():
            copy.wait()
        self.third[self.level] = self.total(self.second).astype(jnp.bfloat16)
        for copy in self.returns():
            copy.start()

    def last(self):
        if self.third is None:
            for copy in self.alongs():
                copy.wait()
            total = self.total(self.second)
        else:
            for copy in self.returns():
                copy.wait()
            total = self.third[...].astype(jnp.float32).reshape(self.whole.shape[1:])
        self.whole[self.me] = total.astype(jnp.bfloat16)
        for copy in self.gathers():
            copy.start()

    def finish(self):
        for copy in self.gathers():
            copy.wait()


class Slabs:
    def __init__(self, sent, came, sems, grid):
        self.sent, self.came, self.sems, self.grid = sent, came, sems, grid
        self.depth, self.level = lax.axis_size("gz"), lax.axis_index("gz")

    def copies(self):
        out = []
        for k in far_first(self.depth, lambda k: ring(k, self.depth)):
            to = (self.level + k) % self.depth
            out.append(
                pltpu.make_async_remote_copy(
                    src_ref=self.sent.at[to],
                    dst_ref=self.came.at[self.level],
                    send_sem=self.sems.at[0, k],
                    recv_sem=self.sems.at[1, k],
                    device_id={"gz": to},
                    device_id_type=MESH,
                )
            )
        return out

    def pack(self, field):
        fold, plane = self.grid.fold, self.grid.plane
        part = self.sent.shape[1]
        spot = self.grid.at(part)[0]
        for t in range(self.grid.tiles):
            for i in range(fold):
                out = None
                for j in range(fold):
                    piece = roll(field[j * part : (j + 1) * part, lanes_at(t)], plane * (j - i))
                    out = piece if out is None else jnp.where(spot == j, piece, out)
                self.sent[t * fold + i] = out
        for copy in self.copies():
            copy.start()
        self.came[self.level] = self.sent[self.level]

    def unpack(self, field):
        for copy in self.copies():
            copy.wait()
        fold, plane = self.grid.fold, self.grid.plane
        part = self.came.shape[1]
        spot = self.grid.at(part)[0]
        for t in range(self.grid.tiles):
            for j in range(fold):
                out = None
                for i in range(fold):
                    piece = roll(self.came[t * fold + i], plane * (i - j))
                    out = piece if out is None else jnp.where(spot == i, piece, out)
                field[j * part : (j + 1) * part, lanes_at(t)] = out


def greet():
    gx, gy, gz = [lax.axis_size(axis) for axis in ("gx", "gy", "gz")]
    me = lax.axis_index("gx") * gy + lax.axis_index("gy")
    level, row, half = lax.axis_index("gz"), lax.axis_index("gy"), lax.axis_index("gx")
    barrier = pltpu.get_barrier_semaphore()
    signal = lambda device: pl.semaphore_signal(barrier, inc=1, device_id=device, device_id_type=MESH)
    for k in range(1, gx * gy):
        to = (me + k) % (gx * gy)
        signal({"gx": to // gy, "gy": to % gy})
    for k in range(1, gz):
        signal({"gz": (level + k) % gz})
    extra = 0
    for across in BOTH:
        for dy in NEAR:
            for dz in NEAR:
                if dz and (across or dy):
                    extra += 1
                    signal(
                        {
                            "gx": (half + across) % gx,
                            "gy": (row + dy + gy) % gy,
                            "gz": (level + dz + gz) % gz,
                        }
                    )
    return barrier, gx * gy + gz - 2 + extra


def spread_map(fine, coarse):
    shape = (LANES, coarse.fold * LANES)
    small = lax.broadcasted_iota(jnp.int32, shape, 0)
    large = lax.broadcasted_iota(jnp.int32, shape, 1)
    y, z = large % LANES // fine.nz, large % fine.nz
    match = (
        (small // coarse.plane == large // LANES)
        & (small // coarse.nz % coarse.ny == y // 2)
        & (small % coarse.nz == z // 2)
    )
    ones = match.astype(jnp.float32)
    first = (match & (y % 2 == 0) & (z % 2 == 0)).astype(jnp.float32)
    return ones.astype(jnp.bfloat16), first.astype(jnp.bfloat16)


def order_map(coarse, count):
    shape = (coarse.plane * count,) * 2
    row = lax.broadcasted_iota(jnp.int32, shape, 0)
    column = lax.broadcasted_iota(jnp.int32, shape, 1)
    wide = count * coarse.nz
    match = (
        (row // wide == column // coarse.nz % coarse.ny)
        & (row % wide // coarse.nz == column // coarse.plane)
        & (row % coarse.nz == column % coarse.nz)
    )
    return match.astype(jnp.float32).astype(jnp.bfloat16)


def column_of(row):
    size = row.shape[1]
    across = lax.broadcasted_iota(jnp.int32, (size, size), 0)
    down = lax.broadcasted_iota(jnp.int32, (size, size), 1)
    return jnp.sum(jnp.where(across == down, row, 0.0), axis=1, keepdims=True)


def turn_in(volume, rows, field):
    channels, _, nx = volume.shape
    fold = LANES // nx
    for q in range(channels // fold):
        wide = jnp.concatenate([volume[q * fold + i] for i in range(fold)], axis=1)
        turned = wide.astype(jnp.float32).T
        for i in range(fold):
            begin = (q * fold + i) * PITCH
            rows[begin : begin + nx] = turned[i * nx : (i + 1) * nx]
    for x in range(nx):
        field[:, lanes_at(x)] = rows[pl.ds(x, channels, stride=PITCH), :].astype(jnp.bfloat16)


def turn_out(rows, out):
    channels, _, nx = out.shape
    fold = LANES // nx
    for q in range(channels // fold):
        begins = [(q * fold + i) * PITCH for i in range(fold)]
        wide = jnp.concatenate([rows[begin : begin + nx] for begin in begins], axis=0)
        turned = wide.T.astype(jnp.bfloat16)
        for i in range(fold):
            out[q * fold + i] = turned[:, i * nx : (i + 1) * nx]


def whole_kernel(setting, *refs):
    names, local = setting[3:]
    pl.run_scoped(lambda **held: stages(setting, dict(zip(names, refs)) | held), **local)


def stages(setting, named):
    fine_size, coarse_size, scales = setting[:3]
    fine, coarse = Grid(*fine_size), Grid(*coarse_size)
    r = lambda name: named[name]
    field = r("field")
    fields = ("a", "b", "gb", "ga")
    grids = (fine, coarse, coarse, fine)
    volume, w_a, b_a, w_b, b_b, cot = [r(n) for n in ("volume", "w_a", "b_a", "w_b", "b_b", "cot")]
    features, grad_in, out_wa, out_ba, out_wb, out_bb = [
        r(n) for n in ("features", "grad_in", "out_wa", "out_ba", "out_wb", "out_bb")
    ]
    c1, c2, c3 = field.shape[0], w_a.shape[1], w_b.shape[1]
    widths = dict(zip(fields, (c1, c2, c3, c2)))
    halos = {
        name: Exchange(
            grid,
            widths[name],
            [r(name + part) for part in ("_zs", "_zr", "_ys", "_yr", "_cs", "_cr", "_xs", "_xr", "_ds", "_dr")],
            r("halo_sems"),
            i,
        )
        for i, (name, grid) in enumerate(zip(fields, grids))
    }
    strips = {name: r(name + "_strips") for name in fields}
    win_a, win_b, win_gb, win_ga = [r(name + "_win") for name in fields]
    before_a, pooled, grad_b, grad_a = [r(n) for n in ("before_a", "pooled", "grad_b", "grad_a")]
    acc_a, acc_b, mixed, feat = [r(n) for n in ("acc_a", "acc_b", "mixed", "feat")]
    sum_a = Summing(acc_a, *[r(f"sum_a{i}") for i in range(5)], None, r("sum_sems").at[0])
    sum_b = Summing(acc_b, *[r(f"sum_b{i}") for i in range(6)], r("sum_sems").at[1])
    cots = Slabs(r("cot_sent"), r("cot_came"), r("slab_sems").at[0], coarse)
    feats = Slabs(r("feat_sent"), r("feat_came"), r("slab_sems").at[1], coarse)
    out_a, in_a, out_b, in_b, spread, thin, order = [
        r(n) for n in ("to_a", "from_a", "to_b", "from_b", "spread", "thin", "order")
    ]
    bf16 = jnp.bfloat16

    loads = {
        name: pltpu.make_async_copy(r(name + "_hbm"), r(name), r("load_sems").at[i])
        for i, name in enumerate(("volume", "cot", "w_a", "w_b"))
    }
    stores = {
        name: pltpu.make_async_copy(r(name), r(name + "_out"), r("load_sems").at[4 + i])
        for i, name in enumerate(("features", "grad_in"))
    }
    for load in loads.values():
        load.start()
    barrier, arrivals = greet()
    halos["a"].clear()
    rows_in, rows_out = r("rows_in"), r("rows_out")
    loads["volume"].wait()
    turn_in(volume, rows_in, field)
    halos["a"].pack(field)
    pl.semaphore_wait(barrier, arrivals)
    halos["a"].start()
    order[...] = order_map(coarse, lax.axis_size("gz"))
    rows_cot = r("rows_cot")
    loads["cot"].wait()
    rows_cot[...] = cot[...].astype(jnp.float32).reshape(rows_cot.shape)
    total = None
    for y in range(coarse.ny):
        row = rows_cot[pl.ds(y, c3, stride=coarse.ny), :].astype(bf16)
        part = dot(row, order[y * LANES : (y + 1) * LANES])
        total = part if total is None else total + part
    mixed[...] = total.astype(bf16)
    cots.pack(mixed)

    loads["w_a"].wait()
    loads["w_b"].wait()
    out_a[...] = w_a[...].T
    for k in range(27):
        in_a[:, k * c2 : (k + 1) * c2] = w_a[(26 - k) * c1 : (27 - k) * c1]
    out_b[...] = w_b[...].T
    for k in range(27):
        in_b[:, k * c3 : (k + 1) * c3] = w_b[(26 - k) * c2 : (27 - k) * c2]
    wide, narrow = spread_map(fine, coarse)
    spread[...] = wide
    thin[...] = narrow
    for name in fields[1:]:
        halos[name].clear()
    bias_a, bias_b = column_of(b_a[...]), column_of(b_b[...])
    acc_a[...] = jnp.zeros_like(acc_a)
    acc_b[...] = jnp.zeros_like(acc_b)

    halos["a"].wait()
    halos["a"].fine_windows(field, strips["a"], win_a)
    many = 2 * coarse.fold

    def forward_a(g, carry):
        near = [win_a[:, lanes_at(g * many + dx, many)] for dx in range(3)]
        before = dot(out_a[...], jnp.concatenate(near, axis=0)) + bias_a
        before_a[:, lanes_at(g * many, many)] = before
        active = before * jax.nn.sigmoid(before)
        pieces = []
        for i in range(coarse.fold):
            first = active[:, 2 * i * LANES : (2 * i + 1) * LANES]
            pair = first + active[:, (2 * i + 1) * LANES : (2 * i + 2) * LANES]
            pair = pair + roll(pair, -1)
            pair = pair + roll(pair, -fine.nz)
            pieces.append((pair * 0.125).astype(bf16))
        pooled[:, lanes_at(g)] = dot_rows(jnp.concatenate(pieces, axis=1), thin[...]).astype(bf16)
        return carry

    lax.fori_loop(0, coarse.tiles, forward_a, 0)
    halos["b"].pack(pooled)
    halos["b"].start()
    cots.unpack(mixed)
    halos["b"].wait()
    halos["b"].coarse_windows(pooled, strips["b"], win_b)
    before = dot(out_b[...], win_b[...]) + bias_b
    grad_b[...] = (mixed[...].astype(jnp.float32) * slope_of(before)).astype(bf16)
    halos["gb"].pack(grad_b)
    halos["gb"].start()
    top_b = out_wb.shape[0]
    grad = grad_b[...]
    acc_b[:top_b] = dot_rows(win_b[...], grad)
    acc_b[top_b : top_b + 8] = dot_rows(jnp.ones((8, grad.shape[1]), bf16), grad)
    sum_b.start()
    feat[...] = (before * jax.nn.sigmoid(before)).astype(bf16)
    feats.pack(feat)
    halos["gb"].wait()
    halos["gb"].coarse_windows(grad_b, strips["gb"], win_gb)
    pooled[...] = dot(in_b[...], win_gb[...]).astype(bf16)

    def backward_b(g, carry):
        wide = dot(pooled[:, lanes_at(g)], spread[...]) * 0.125
        for i in range(coarse.fold):
            for j in BOTH:
                here = lanes_at(g * many + 2 * i + j)
                slope = slope_of(before_a[:, here])
                grad_a[:, here] = (wide[:, i * LANES : (i + 1) * LANES] * slope).astype(bf16)
        return carry

    lax.fori_loop(0, coarse.tiles, backward_b, 0)
    halos["ga"].pack(grad_a)
    sum_b.middle()
    grad = grad_a[...]
    half, width = out_wa.shape[0] // 2, out_wa.shape[1]
    parts = [dot_rows(win_a[:, lanes_at(dx, fine.tiles)], grad) for dx in range(3)]
    whole = jnp.concatenate(parts, axis=0)
    acc_a[:half, :width] = whole[:half]
    acc_a[:half, width:] = whole[half:]
    acc_a[half : half + 8, :width] = dot_rows(jnp.ones((8, grad.shape[1]), bf16), grad)
    sum_a.start()
    halos["ga"].start()
    sum_b.between()
    halos["ga"].wait()
    sum_b.last()
    sum_a.middle()
    halos["ga"].fine_windows(grad_a, strips["ga"], win_ga)

    def backward_a(g, carry):
        near = [win_ga[:, lanes_at(g * many + dx, many)] for dx in range(3)]
        total = dot(in_a[...], jnp.concatenate(near, axis=0))
        for i in range(many):
            tile = total[:, i * LANES : (i + 1) * LANES].astype(bf16).astype(jnp.float32)
            rows_out[pl.ds(g * many + i, c1, stride=PITCH), :] = tile
        return carry

    lax.fori_loop(0, coarse.tiles, backward_a, 0)
    sum_a.last()
    feats.unpack(feat)
    for y in range(coarse.ny):
        rows_cot[pl.ds(y, c3, stride=coarse.ny), :] = dot_rows(feat[...], order[y * LANES : (y + 1) * LANES])
    features[...] = rows_cot[...].reshape(features.shape).astype(bf16)
    stores["features"].start()
    turn_out(rows_out, grad_in)
    stores["grad_in"].start()
    sum_b.finish()
    all_a, all_b = r("sum_a4"), r("sum_b4")
    scale_a, scale_b = scales
    flat_b = all_b[...].astype(jnp.float32).reshape(-1, all_b.shape[2]) * scale_b
    out_wb[...] = flat_b[:top_b]
    out_bb[...] = flat_b[top_b : top_b + 1]
    sum_a.finish()
    flat_a = all_a[...].astype(jnp.float32).reshape(-1, all_a.shape[2]) * scale_a
    out_wa[:half] = flat_a[:half, :width]
    out_wa[half:] = flat_a[:half, width:]
    out_ba[...] = flat_a[half : half + 1, :width]
    for store in stores.values():
        store.wait()


def landing_kernel(count, *refs):
    arrived, leaving, held = [refs[i * count : (i + 1) * count] for i in range(3)]
    sems = refs[3 * count]
    into = [pltpu.make_async_copy(arrived[i], held[i], sems.at[0, i]) for i in range(count)]
    out = [pltpu.make_async_copy(held[i], leaving[i], sems.at[1, i]) for i in range(count)]
    for copy in into:
        copy.start()
    for first, second in zip(into, out):
        first.wait()
        second.start()
    for copy in out:
        copy.wait()


def landed(arrays):
    count = len(arrays)
    return pl.pallas_call(
        functools.partial(landing_kernel, count),
        out_shape=[jax.ShapeDtypeStruct(array.shape, array.dtype) for array in arrays],
        in_specs=[pl.BlockSpec(memory_space=pl.ANY)] * count,
        out_specs=[pl.BlockSpec(memory_space=pl.ANY)] * count,
        scratch_shapes=[pltpu.VMEM(array.shape, array.dtype) for array in arrays]
        + [pltpu.SemaphoreType.DMA((2, count))],
    )(*arrays)


def on_device(volume, weight_a, bias_a, weight_b, bias_b, cotangent):
    f32, bf16 = jnp.float32, jnp.bfloat16
    members, levels = lax.axis_size("gx") * lax.axis_size("gy"), lax.axis_size("gz")
    c1, nx, ny, nz = volume.shape
    c2, c3 = weight_b.shape[3:]
    cells = nx * ny * nz
    fewer = cells // 8
    scale_a = 1.0 / math.sqrt(cells * members * levels)
    scale_b = 1.0 / math.sqrt(cells * members * levels // 8)
    fine_size, coarse_size = (nx, ny, nz), (nx // 2, ny // 2, nz // 2)
    fine, coarse = Grid(*fine_size), Grid(*coarse_size)
    rows_a = 27 * c1 // 2 + 16
    rows_a += -rows_a % (16 * members)
    rows_b = 27 * c2 + 16
    rows_b += -rows_b % (8 * members * levels)
    operands = {
        "volume_hbm": jnp.transpose(volume, (0, 2, 3, 1)).reshape(c1, ny * nz, nx),
        "w_a_hbm": weight_a.reshape(27 * c1, c2),
        "b_a": bias_a.reshape(1, c2),
        "w_b_hbm": weight_b.reshape(27 * c2, c3),
        "b_b": bias_b.reshape(1, c3),
        "cot_hbm": cotangent.reshape(c3, ny // 2, nz // 2 * levels),
    }
    outs = {
        "features_out": ((c3, ny // 2, nz // 2 * levels), bf16),
        "grad_in_out": ((c1, ny * nz, nx), bf16),
        "out_wa": ((27 * c1, c2), f32),
        "out_ba": ((1, c2), f32),
        "out_wb": ((27 * c2, c3), f32),
        "out_bb": ((1, c3), f32),
    }
    scratch, local = {}, {}
    for name, grid, c in (("a", fine, c1), ("b", coarse, c2), ("gb", coarse, c3), ("ga", fine, c2)):
        for end in ("s", "r"):
            scratch[f"{name}_z{end}"] = pltpu.VMEM((2, c, grid.zpacks * LANES), bf16)
            scratch[f"{name}_y{end}"] = pltpu.VMEM((2, c, grid.ypacks * LANES), bf16)
            scratch[f"{name}_c{end}"] = pltpu.VMEM((4, c // grid.corner_groups(c), LANES), bf16)
        scratch[f"{name}_xs"] = pltpu.VMEM((c // grid.fold, LANES), bf16)
        scratch[f"{name}_xr"] = pltpu.VMEM((3, c // grid.fold, LANES), bf16)
        scratch[f"{name}_ds"] = pltpu.VMEM((2, 16, LANES), bf16)
        scratch[f"{name}_dr"] = pltpu.VMEM((2, 3, 16, LANES), bf16)
        local[f"{name}_strips"] = pltpu.VMEM((6, c, grid.ypacks * LANES), bf16)
        shape = (9 * c, (grid.tiles + 2) * LANES) if grid is fine else (27 * c, grid.tiles * LANES)
        local[f"{name}_win"] = pltpu.VMEM(shape, bf16)
    local["field"] = pltpu.VMEM((c1, cells), bf16)
    local["rows_in"] = local["rows_out"] = pltpu.VMEM((c1 * PITCH, ny * nz), f32)
    local["rows_cot"] = pltpu.VMEM((c3 * ny // 2, nz // 2 * levels), f32)
    local["before_a"] = pltpu.VMEM((c2, cells), f32)
    local["pooled"] = pltpu.VMEM((c2, fewer), bf16)
    local["grad_b"] = pltpu.VMEM((c3, fewer), bf16)
    local["grad_a"] = pltpu.VMEM((c2, cells), bf16)
    local["mixed"] = pltpu.VMEM((c3, fewer), bf16)
    local["feat"] = pltpu.VMEM((c3, fewer), bf16)
    for name, rows in (("a", rows_a), ("b", rows_b)):
        chunk = rows // members
        scratch[f"acc_{name}"] = pltpu.VMEM((rows, LANES), f32)
        shapes = [(members, chunk), (members, chunk), (chunk,), (levels, chunk), (members, chunk)]
        if name == "b":
            shapes[2:4] = [(levels, chunk // levels)] * 2
            shapes.append((levels, chunk // levels))
        for i, shape in enumerate(shapes):
            scratch[f"sum_{name}{i}"] = pltpu.VMEM((*shape, LANES), bf16)
    for name in ("cot_sent", "cot_came", "feat_sent", "feat_came"):
        scratch[name] = pltpu.VMEM((levels, c3 // coarse.fold, LANES), bf16)
    local["to_a"] = pltpu.VMEM((c2, 27 * c1), bf16)
    local["from_a"] = pltpu.VMEM((c1, 27 * c2), bf16)
    local["to_b"] = pltpu.VMEM((c3, 27 * c2), bf16)
    local["from_b"] = pltpu.VMEM((c2, 27 * c3), bf16)
    local["spread"] = pltpu.VMEM((LANES, coarse.fold * LANES), bf16)
    local["thin"] = pltpu.VMEM((LANES, coarse.fold * LANES), bf16)
    local["order"] = pltpu.VMEM((fewer, fewer), bf16)
    for name in ("volume", "cot", "w_a", "w_b"):
        local[name] = pltpu.VMEM(operands[name + "_hbm"].shape, bf16)
    for name in ("features", "grad_in"):
        local[name] = pltpu.VMEM(*outs[name + "_out"])
    scratch["load_sems"] = pltpu.SemaphoreType.DMA((6,))
    scratch["halo_sems"] = pltpu.SemaphoreType.DMA((2, 4, 17))
    scratch["sum_sems"] = pltpu.SemaphoreType.DMA((2, 4, 2, max(members, levels)))
    scratch["slab_sems"] = pltpu.SemaphoreType.DMA((2, 2, levels))
    names = (*operands, *outs, *scratch)
    got = pl.pallas_call(
        functools.partial(whole_kernel, (fine_size, coarse_size, (scale_a, scale_b), names, local)),
        out_shape=[jax.ShapeDtypeStruct(shape, dtype) for shape, dtype in outs.values()],
        in_specs=[
            pl.BlockSpec(memory_space=pl.ANY if name.endswith("_hbm") else pltpu.VMEM) for name in operands
        ],
        out_specs=[
            pl.BlockSpec(memory_space=pl.ANY if name.endswith("_out") else pltpu.VMEM) for name in outs
        ],
        scratch_shapes=list(scratch.values()),
        compiler_params=pltpu.CompilerParams(
            collective_id=1, has_side_effects=True, vmem_limit_bytes=60 * 2**20
        ),
    )(*operands.values())
    features, grad_in, sum_wa, sum_ba, sum_wb, sum_bb = landed(got)
    return (
        features.reshape(cotangent.shape),
        jnp.transpose(grad_in.reshape(c1, ny, nz, nx), (0, 3, 1, 2)),
        sum_wa.reshape(weight_a.shape),
        sum_ba.reshape(c2),
        sum_wb.reshape(weight_b.shape),
        sum_bb.reshape(c3),
    )


def solution(mesh):
    return jax.shard_map(
        on_device,
        mesh=mesh,
        in_specs=(P(None, "gx", "gy", "gz"), P(), P(), P(), P(), P(None, ("gx", "gz"), "gy", None)),
        out_specs=(
            P(None, ("gx", "gz"), "gy", None),
            P(None, "gx", "gy", "gz"),
            P(),
            P(),
            P(),
            P(),
        ),
        check_vma=False,
    )
```
